256 devices in a mesh: lev: 8 (over x, core), lon: 32 (over y, z).
Axes of the slice: x: 4, y: 4, z: 8, core: 2. Of those that a mesh axis runs over, the one named last changes fastest.
Arguments:
- previous: float32 [72, 64, 16384], P('lev', None, 'lon'), may hold values from -4 to 4
- loss_matrix: float32 [72, 64, 64], P('lev'), may hold values from -3 to 10, as said below
- pair_matrix: float32 [72, 64, 64], P('lev'), may hold values from -0.1875 to 0.1875
- diffusivity: float32 [72], P('lev'), may hold values from 200 to 2000
- mixing: float32 [72], P('lev'), may hold values from 0.1 to 1
Outputs:
- concentration: float32 [72, 64, 16384], P('lev', None, 'lon')
- level_variance: float32 [72, 64], P('lev')
The draws below stay inside these ranges and needn't reach their ends.
Inputs may be any that keep to these rules, and one draw needn't show every extreme that they name: `loss_matrix`: each of the 72 blocks is symmetric and at least 0.05 times the identity in the positive definite order.
All inputs are finite; a program needn't handle non-finite values.
Results may differ from the reference program's by a relative error of at most 0.00045.
Values sent between devices are 32-bit elements; how exact they have to be, the bound alone decides.
A program may use at most 64 MiB of HBM per device.

```python
import math
import jax
import jax.numpy as jnp
from jax import lax

S = 64
ITERS = 2
L = 72
NCOL = 16384


def draw_loss_matrix(key, part):
    first_key, second_key = jax.random.split(jax.random.fold_in(key, 17))
    base = jax.random.normal(first_key, (L, S, S), jnp.float32)
    level_scale = jax.random.uniform(second_key, (L,), jnp.float32, 0.2, 2.0)
    gram = jnp.einsum('lst,lut->lsu', base, base, precision=lax.Precision.HIGHEST) / S
    gram = 0.5 * (gram + jnp.swapaxes(gram, 1, 2))
    identity = jnp.eye(S, dtype=jnp.float32)
    return level_scale[:, None, None] * (0.25 * identity + gram)


def block_scale(own_key, dims, shards, least, high):
    def one(position, parts):
        steps = jax.random.uniform(jax.random.fold_in(jax.random.fold_in(own_key, 6), position), (parts,), jnp.float32, least / len(shards), high / len(shards))
        return jnp.repeat(jnp.exp(steps), dims[position] // parts).reshape((-1,) + (1,) * (len(dims) - position - 1))

    level = one(*shards[0])
    for cut in shards[1:]:
        level = level * one(*cut)
    return level


def normal_values(own_key, dims, scale, most, cuts=(), held_as=jnp.bfloat16):
    gain = block_scale(own_key, dims, cuts, -0.22, 0.18) if cuts else 1.0
    drawn = jax.random.normal(own_key, dims, jnp.float32) * scale * gain
    return jnp.minimum(jnp.maximum(drawn, -most), most).astype(held_as)


def setup_inputs(seed: int = 0) -> dict:
    key_of = jax.random.split(jax.random.key(seed), 6)
    return {
        "previous": normal_values(key_of[0], (L, S, NCOL), 1.0, 4.0, ((0, 8), (2, 32)), jnp.float32),
        "loss_matrix": draw_loss_matrix(jax.random.fold_in(key_of[5], 71), 0),
        "pair_matrix": normal_values(key_of[2], (L, S, S), (16 * S) ** -0.5, 0.1875, ((0, 8),), jnp.float32),
        "diffusivity": jnp.clip(jnp.exp(math.log(2000.0) - 2.3025851 * jax.random.uniform(key_of[3], (L,), jnp.float32) ** block_scale(key_of[3], (L,), ((0, 8),), -0.2, 0.2)), 200.0, 2000.0),
        "mixing": jnp.clip(jnp.exp(math.log(1.0) - 2.3025851 * jax.random.uniform(key_of[4], (L,), jnp.float32) ** block_scale(key_of[4], (L,), ((0, 8),), -0.2, 0.2)), 0.1, 1.0),
    }


HIGHEST_PRECISION = lax.Precision.HIGHEST

def residual_of(current, previous, loss_matrix, pair_matrix, diffusivity, mixing):
    above_links = jnp.concatenate([jnp.zeros((1,), current.dtype), diffusivity[:-1]])
    zero_level = jnp.zeros_like(current[:1])
    level_above = jnp.concatenate([zero_level, current[:-1]], axis=0)
    level_below = jnp.concatenate([current[1:], zero_level], axis=0)
    across = mixing[:, None, None] * (jnp.roll(current, 1, axis=2) + jnp.roll(current, -1, axis=2) - 2.0 * current)
    own_chem = jnp.einsum('lst,ltc->lsc', loss_matrix, current, precision=HIGHEST_PRECISION)
    pair_chem = jnp.einsum('lst,ltc->lsc', pair_matrix, current * current, precision=HIGHEST_PRECISION)
    vertical = diffusivity[:, None, None] * (current - level_below) + above_links[:, None, None] * (current - level_above)
    return current + own_chem + pair_chem + vertical - across - previous

def newton_solve(forcing, loss_matrix, diffusivity):
    species = loss_matrix.shape[1]
    identity = jnp.eye(species, dtype=loss_matrix.dtype)
    above_links = jnp.concatenate([jnp.zeros((1,), diffusivity.dtype), diffusivity[:-1]])
    diagonal = (1.0 + above_links + diffusivity)[:, None, None] * identity + loss_matrix

    def factor_step(prev_inverse, pieces):
        block, link_above = pieces
        inverse = jnp.linalg.inv(block - link_above * link_above * prev_inverse)
        return (inverse, inverse)
    _, inverses = lax.scan(factor_step, jnp.zeros_like(identity), (diagonal, above_links))

    def forward(prev_lifted, pieces):
        inverse, link_above, right_side = pieces
        lifted = jnp.dot(inverse, right_side + link_above * prev_lifted, precision=HIGHEST_PRECISION)
        return (lifted, lifted)
    _, lifted_all = lax.scan(forward, jnp.zeros_like(forcing[0]), (inverses, above_links, forcing))

    def backward(next_value, pieces):
        inverse, link_below, lifted_level = pieces
        value = lifted_level + link_below * jnp.dot(inverse, next_value, precision=HIGHEST_PRECISION)
        return (value, value)
    _, solution = lax.scan(backward, jnp.zeros_like(forcing[0]), (inverses, diffusivity, lifted_all), reverse=True)
    return solution

def reference(previous, loss_matrix, pair_matrix, diffusivity, mixing):
    current = previous
    for newton_step in range(ITERS):
        forcing = residual_of(current, previous, loss_matrix, pair_matrix, diffusivity, mixing)
        current = current - newton_solve(forcing, loss_matrix, diffusivity)
    variance = jnp.mean(current * current, axis=2)
    return (current, variance)
```

```python
import functools

import jax
import jax.numpy as jnp
from jax import lax
from jax.experimental import pallas as pl
from jax.experimental.pallas import tpu as pltpu
from jax.sharding import PartitionSpec as P

ITERS = 2
F32 = jnp.float32
BF16 = jnp.bfloat16
MESH = pl.DeviceIdType.MESH
HIGHEST = lax.Precision.HIGHEST

S = 64
ORDER = (1, 2, 3, 4, 6, 8, 7, 5)
NN = (((1,), (0,)), ((), ()))
NT = (((1,), (1,)), ((), ()))
TN = (((0,), (0,)), ((), ()))


def split(x):
    high = x.astype(BF16)
    return high, (x - high.astype(F32)).astype(BF16)


def dot3(a, b, dims=NN):
    one = lambda x, y: lax.dot_general(x, y, dims, preferred_element_type=F32)
    return one(a[0], b[0]) + (one(a[0], b[1]) + one(a[1], b[0]))


def mm(a, b, dims=NN):
    return dot3(split(a), split(b), dims)


def mm_full(a, b, dims=NN):
    return lax.dot_general(a, b, dims, precision=HIGHEST, preferred_element_type=F32)


def eye(n):
    rows = lax.broadcasted_iota(jnp.int32, (n, n), 0)
    return (rows == lax.broadcasted_iota(jnp.int32, (n, n), 1)).astype(F32)


def spd_inverses(blocks, low, high, doublings):
    centre, radius = 0.5 * (high + low), 0.5 * (high - low)
    units = [eye(block.shape[0]) for block in blocks]
    inverses = [unit * (1.0 / centre) for unit in units]
    residuals = [unit - block * (1.0 / centre) for unit, block in zip(units, blocks)]
    term = centre / radius
    for step in range(doublings):
        twice = 2.0 * term * term - 1.0
        gain, shift = 2.0 * term * term / twice, 1.0 / twice
        last = step == doublings - 1
        for i, unit in enumerate(units):
            n = unit.shape[0]
            rest = split(residuals[i])
            if step == 0:
                inverses[i] = (inverses[i] + residuals[i] * (1.0 / centre)) * gain
                if not last:
                    residuals[i] = gain * dot3(rest, rest) - shift * unit
                continue
            known = split(inverses[i])
            if last:
                inverses[i] = gain * (inverses[i] + dot3(known, rest))
                continue
            both = dot3(tuple(jnp.concatenate(p, axis=0) for p in zip(known, rest)), rest)
            inverses[i] = gain * (inverses[i] + both[:n])
            residuals[i] = gain * both[n:] - shift * unit
        term = twice
    exact = [unit - mm_full(block, inverse) for unit, block, inverse in zip(units, blocks, inverses)]
    return [inverse + mm(inverse, rest) for inverse, rest in zip(inverses, exact)]


def wide(grid):
    return jnp.concatenate([jnp.concatenate(row, axis=1) if len(row) > 1 else row[0] for row in grid], axis=0)


def interior(shunt, links):
    one = eye(S)
    zero = jnp.zeros((S, S), F32)
    diag = [shunt[i] + (links[i] + links[i + 1]) * one for i in range(8)]
    tie = [-links[i + 1] * one for i in range(7)]
    upper = wide([
        [diag[0], tie[0], zero, zero],
        [tie[0], diag[1], tie[1], zero],
        [zero, tie[1], diag[2], tie[2]],
        [zero, zero, tie[2], diag[3]],
    ])
    lower = wide([[diag[5], zero, tie[5]], [zero, diag[7], tie[6]], [tie[5], tie[6], diag[6]]])
    upper_inverse, = spd_inverses([upper], 77.0, 8700.0, 6)
    lower_inverse, = spd_inverses([lower], 117.0, 8700.0, 6)
    upper_t = links[4] * upper_inverse[192:256, :]
    lower_t = links[5] * lower_inverse[0:64, :]
    ground_up = jnp.concatenate([shunt[0] + links[0] * one, shunt[1], shunt[2], shunt[3]], axis=0)
    ground_low = jnp.concatenate([shunt[5], shunt[7] + links[8] * one, shunt[6]], axis=0)
    middle = shunt[4] + mm_full(upper_t, ground_up) + mm_full(lower_t, ground_low)
    middle_inverse, = spd_inverses([middle], 90.0, 4700.0, 5)
    spread = jnp.concatenate([upper_t, lower_t, one], axis=1)
    lifted = mm(middle_inverse, spread)
    return upper_inverse, lower_inverse, spread, lifted


def setup_kernel(link_ref, mix_ref, loss_ref, pair_ref, prev_ref, g_hi, g_lo, hc_hi, hc_lo, hr_hi, hr_lo, pack_ref,
                 pw_hi, pw_lo, pn_hi, pn_lo, field_ref, mixrow_ref, full):
    one = eye(S)
    links = [link_ref[i] for i in range(9)]
    shunt = [loss_ref[i] + one for i in range(9)]
    upper_inverse, lower_inverse, spread, lifted = interior(shunt[1:], links)
    inverse = mm(spread, lifted, TN)
    full[...] = inverse
    full[0:256, 0:256] += upper_inverse
    full[256:448, 256:448] += lower_inverse
    lane = lax.broadcasted_iota(jnp.int32, (512, 128), 1)
    columns = jnp.where(lane < S, links[0] * full[:, 0:128], links[8] * full[:, 256:384])
    hc_hi[...], hc_lo[...] = split(columns)
    rows = jnp.concatenate([links[0] * full[0:64, :], links[8] * full[320:384, :]], axis=0)
    hr_hi[...], hr_lo[...] = split(rows)
    g_hi[...], g_lo[...] = split(full[...])
    stack = jnp.concatenate([shunt[level] for level in ORDER], axis=0)
    ends = mm_full(rows, stack)
    across = links[8] * rows[0:64, 320:384]
    pack_ref[0:64, :] = jnp.concatenate([shunt[0] + ends[0:64], ends[64:128]], axis=1)
    pack_ref[64:96, :] = jnp.concatenate([across[0:32], across[32:64]], axis=1)
    for half in range(2):
        row = lax.broadcasted_iota(jnp.int32, (256, 256), 0) // S
        column = lax.broadcasted_iota(jnp.int32, (256, 256), 1) // S
        tall = jnp.concatenate([pair_ref[level] for level in ORDER[4 * half : 4 * half + 4]], axis=0)
        tall = jnp.concatenate([tall, tall], axis=1)
        tall = jnp.where(row == column, jnp.concatenate([tall, tall], axis=1), 0.0)
        pw_hi[half], pw_lo[half] = split(tall)
    pn_hi[...], pn_lo[...] = split(pair_ref[0])
    for j in range(4):
        both = jnp.concatenate([prev_ref[ORDER[2 * j]], prev_ref[ORDER[2 * j + 1]]], axis=0)
        field_ref[:, 128 * j : 128 * j + 128] = both.T
    last = jnp.concatenate([prev_ref[0], jnp.zeros_like(prev_ref[0])], axis=0)
    field_ref[:, 512:640] = last.T
    lane = lax.broadcasted_iota(jnp.int32, (8, 640), 1) // S
    row = jnp.zeros((8, 640), F32)
    for j, level in enumerate(ORDER + (0,)):
        row = jnp.where(lane == j, mix_ref[level], row)
    mixrow_ref[...] = row


def unpack(packs, q):
    both, folded = packs(q)
    across = jnp.concatenate([folded[:, 0:S], folded[:, S:]], axis=0)
    return both[:, 0:S], both[:, S:], across


def interface_kernel(pack_ref, own_hi, own_lo, msg_hi, msg_lo, rlo_hi, rlo_lo, rhi_hi, rhi_lo, full, wp, wc, rs, rc, own):
    chip = lax.axis_index("lev") // 2
    one = eye(S)
    zero = jnp.zeros((S, S), F32)
    here, below, across = zip(*[
        unpack(lambda q: (pack_ref[q, 0:64, :], pack_ref[q, 64:96, :]), q) for q in range(8)
    ])
    back = [a.T for a in across]
    ground = [here[q] + (below[q - 1] if q else 0.0) for q in range(8)]
    diag = [ground[q] + across[q] + (back[q - 1] if q else 0.0) for q in range(8)]
    upper = wide([
        [diag[0], -across[0], zero, zero],
        [-back[0], diag[1], -across[1], zero],
        [zero, -back[1], diag[2], -across[2]],
        [zero, zero, -back[2], diag[3]],
    ])
    lower = wide([
        [diag[5], -across[5], zero],
        [-back[5], diag[6], -across[6]],
        [zero, -back[6], diag[7]],
    ])
    first = chip < 2
    small = jnp.where(
        first, upper[0:128, 0:128], wide([[1000.0 * one, zero], [zero, diag[7]]])
    )
    upper_inverse, lower_inverse, small_inverse = spd_inverses([upper, lower, small], 9.0, 4700.0, 7)
    upper_t = mm(back[3], upper_inverse[192:256, :])
    lower_t = mm(across[4], lower_inverse[0:64, :])
    middle = (
        ground[4]
        + mm_full(upper_t, jnp.concatenate(ground[0:4], axis=0))
        + mm_full(lower_t, jnp.concatenate([ground[5], ground[6], ground[7] + across[7]], axis=0))
    )
    middle_inverse, = spd_inverses([middle], 9.0, 4700.0, 7)
    spread = jnp.concatenate([upper_t, lower_t, one], axis=1)
    lifted = mm(middle_inverse, spread)
    full[...] = mm(spread, lifted, TN)
    full[0:256, 0:256] += upper_inverse
    full[256:448, 256:448] += lower_inverse
    place = {0: 0, 1: 1, 2: 2, 3: 3, 4: 7, 5: 4, 6: 5, 7: 6}
    link = jnp.where(first, back[1], across[6])
    away = mm(link, small_inverse[64:128, :])

    def block(r, c):
        if r > 7 or c > 7:
            return zero
        r, c = place[r], place[c]
        return full[S * r : S * r + S, S * c : S * c + S]

    def blocks(rows, columns):
        return wide([[block(r, c) for c in columns] for r in rows])

    for c in range(4):
        nodes = (2 * c, 2 * c + 1, 2 * c + 1, 2 * c + 2)

        @pl.when(chip == c)
        def _(c=c, nodes=nodes):
            own[...] = blocks(nodes, nodes)
            wc[...] = blocks(nodes, (4,))
            if c in (0, 3):
                far = [away[:, 0:64], away[:, 64:128]]
                if c == 0:
                    rs[...] = jnp.concatenate([far[0], far[1], far[1], one], axis=1)
                    wp[...] = jnp.concatenate([far[0].T, far[1].T, far[1].T, one], axis=0)
                else:
                    rs[...] = jnp.concatenate([one, far[1], far[1], zero], axis=1)
                    wp[...] = jnp.concatenate([one, far[1].T, far[1].T, zero], axis=0)
            else:
                gate = 2 if c == 1 else 6
                rs[...] = blocks((gate,), nodes)
                wp[...] = blocks(nodes, (gate,))

            def seen(n):
                if n > 7:
                    return zero
                n = place[n]
                return spread[:, S * n : S * n + S]

            rc[...] = jnp.concatenate([seen(n) for n in nodes], axis=1)

    own_hi[...], own_lo[...] = split(own[...])
    none = jnp.zeros((256, S), F32)
    msg = wide([[wp[...], none, wc[...], none], [none, wp[...], none, wc[...]]])
    msg_hi[...], msg_lo[...] = split(msg)
    none = jnp.zeros((S, 256), F32)
    rlo_hi[...], rlo_lo[...] = split(jnp.concatenate([rs[...], none, rc[...], none], axis=0))
    rhi_hi[...], rhi_lo[...] = split(jnp.concatenate([none, rs[...], none, rc[...]], axis=0))


def gather_kernel(pack_ref, all_ref, send_sem, recv_sem, own_sem):
    lev = lax.axis_index("lev")
    barrier = pltpu.get_barrier_semaphore()
    for d in range(1, 8):
        pl.semaphore_signal(barrier, inc=1, device_id={"lev": lax.rem(lev + d, 8)}, device_id_type=MESH)
    keep = pltpu.make_async_copy(pack_ref, all_ref.at[lev], own_sem)
    keep.start()
    pl.semaphore_wait(barrier, 7)
    copies = []
    for d in range(1, 8):
        copy = pltpu.make_async_remote_copy(
            src_ref=pack_ref, dst_ref=all_ref.at[lev], send_sem=send_sem.at[d - 1], recv_sem=recv_sem.at[d - 1],
            device_id={"lev": lax.rem(lev + d, 8)}, device_id_type=MESH,
        )
        copy.start()
        copies.append(copy)
    keep.wait()
    for copy in copies:
        copy.wait()


def solve_kernel(count, field_ref, mixrow_ref, pw_hi, pw_lo, pn_hi, pn_lo, g_hi, g_lo, hc_hi, hc_lo, hr_hi, hr_lo,
                 own_hi, own_lo, msg_hi, msg_lo, rlo_hi, rlo_lo, rhi_hi, rhi_lo,
                 out_ref, var_ref,
                 state, gs_hi, gs_lo, gnode, injs, outgo, incoming, nodes, nodebuf, halo, sums, mysum, sumbuf,
                 halo_send, halo_recv, part_send, part_recv, msg_send, msg_recv, sum_send, sum_recv):
    lev = lax.axis_index("lev")
    lon = lax.axis_index("lon")
    core = lax.rem(lev, 2)
    chip = lev // 2
    partner = lev + 1 - 2 * core
    sibling_chip = chip + 1 - 2 * lax.rem(chip, 2)
    across_base = 2 - 2 * (chip // 2)
    sibling = 2 * sibling_chip + core
    across = [2 * (across_base + i) + core for i in range(2)]
    west, east = lax.rem(lon + count - 1, count), lax.rem(lon + 1, count)

    barrier = pltpu.get_barrier_semaphore()
    for other in [partner, sibling] + across:
        pl.semaphore_signal(barrier, inc=1, device_id={"lev": other}, device_id_type=MESH)

    def greet(d, carry):
        pl.semaphore_signal(barrier, inc=1, device_id={"lon": lax.rem(lon + d, count)}, device_id_type=MESH)
        return carry

    lax.fori_loop(1, count, greet, 0)

    def remote(src, dst, send, recv, where):
        return pltpu.make_async_remote_copy(
            src_ref=src, dst_ref=dst, send_sem=send, recv_sem=recv, device_id=where, device_id_type=MESH
        )

    state[0, 8:520, :] = field_ref[...]
    pl.semaphore_wait(barrier, 3 + count)
    mix_row = mixrow_ref[0:1, :]
    pending = []
    for it in range(ITERS):
        final = it == ITERS - 1
        now = state.at[it]
        first = field_ref.at[0:8] if it == 0 else now.at[8:16]
        last = field_ref.at[504:512] if it == 0 else now.at[512:520]
        to_west = remote(first, halo.at[it, 1], halo_send.at[it, 0], halo_recv.at[it, 1], {"lon": west})
        to_east = remote(last, halo.at[it, 0], halo_send.at[it, 1], halo_recv.at[it, 0], {"lon": east})
        to_west.start()
        to_east.start()
        pending += [to_west, to_east]
        for r in range(0, 512, 128):
            here = state[it, 8 + r : 136 + r, :]
            squares = split(here * here)
            for half in range(2):
                piece = tuple(s[:, 256 * half : 256 * half + 256] for s in squares)
                out = dot3(piece, (pw_hi[half], pw_lo[half]), NT)
                sums[r : r + 128, 256 * half : 256 * half + 256] = out
            piece = tuple(s[:, 512:576] for s in squares)
            sums[r : r + 128, 512:576] = dot3(piece, (pn_hi[...], pn_lo[...]), NT)
        to_west.wait_recv()
        to_east.wait_recv()
        state[it, 0:8, :] = halo[it, 0]
        state[it, 520:528, :] = halo[it, 1]
        for r in range(0, 512, 128):
            here = state[it, 8 + r : 136 + r, 0:576]
            around = state[it, 7 + r : 135 + r, 0:576] + state[it, 9 + r : 137 + r, 0:576]
            forcing = field_ref[r : r + 128, 0:576] - sums[r : r + 128, 0:576] + mix_row[:, 0:576] * (around - 2.0 * here)
            parts = split(forcing[:, 0:512])
            gs_hi[r : r + 128, :], gs_lo[r : r + 128, :] = parts
            node = forcing[:, 512:576]
            push = dot3(parts, (hc_hi[...], hc_lo[...])) + jnp.concatenate([node, jnp.zeros_like(node)], axis=1)
            injs[it, r // 256, r % 256 : r % 256 + 128, :] = push
        give = remote(injs.at[it, 1 - core], gnode.at[it, core], part_send.at[it, 0], part_recv.at[it, 0], {"lev": partner})
        give.start()
        gnode[it, core] = injs[it, core]
        give.wait()
        inj = jnp.concatenate([gnode[it, 0], gnode[it, 1]], axis=1)
        packed = split(jnp.concatenate([inj[0:128], inj[128:256]], axis=1))
        message = dot3(packed, (msg_hi[...], msg_lo[...]))
        outgo[it, 0] = message[:, 0:128]
        outgo[it, 1] = message[:, 128:256]
        sends = [
            remote(outgo.at[it, 1], incoming.at[it, 1 + lax.rem(chip, 2)], msg_send.at[it, 1],
                   msg_recv.at[it, 1 + lax.rem(chip, 2)], {"lev": across[0]}),
            remote(outgo.at[it, 1], incoming.at[it, 1 + lax.rem(chip, 2)], msg_send.at[it, 2],
                   msg_recv.at[it, 1 + lax.rem(chip, 2)], {"lev": across[1]}),
            remote(outgo.at[it, 0], incoming.at[it, 0], msg_send.at[it, 0], msg_recv.at[it, 0], {"lev": sibling}),
        ]
        for send in sends:
            send.start()
        mine = dot3(split(inj), (own_hi[...], own_lo[...]))
        if final:
            for c in range(0, 512, 256):
                parts = (gs_hi[c : c + 256, :], gs_lo[c : c + 256, :])
                for b in range(4):
                    rows = slice(128 * b, 128 * b + 128)
                    value = dot3((g_hi[rows, :], g_lo[rows, :]), parts, NT)
                    for h in range(2):
                        out_ref[ORDER[2 * b + h], :, c : c + 256] = value[64 * h : 64 * h + 64]
        else:
            for r in range(0, 512, 128):
                parts = (gs_hi[r : r + 128, :], gs_lo[r : r + 128, :])
                state[it + 1, 8 + r : 136 + r, 0:512] = dot3(parts, (g_hi[...], g_lo[...]))
        for slot in range(3):
            arrive = remote(outgo.at[it, 0], incoming.at[it, slot], msg_send.at[it, 0], msg_recv.at[it, slot], {"lev": sibling})
            arrive.wait_recv()
        for send in sends:
            send.wait_send()
        heard = split(jnp.concatenate([incoming[it, 0], incoming[it, 1] + incoming[it, 2]], axis=1))
        total = mine + jnp.concatenate(
            [dot3(heard, (rlo_hi[...], rlo_lo[...])), dot3(heard, (rhi_hi[...], rhi_lo[...]))], axis=0
        )
        nodes[it, 0] = total[:, 0:128]
        nodes[it, 1] = total[:, 128:256]
        give = remote(nodes.at[it, 1 - core], nodebuf.at[it, core], part_send.at[it, 1], part_recv.at[it, 1], {"lev": partner})
        give.start()
        nodebuf[it, core] = nodes[it, core]
        give.wait()
        if final:
            for c in range(2):
                ends = nodebuf[it, c]
                parts = split(ends)
                columns = slice(256 * c, 256 * c + 256)
                for b in range(4):
                    rows = slice(128 * b, 128 * b + 128)
                    value = dot3((hc_hi[rows, :], hc_lo[rows, :]), parts, NT)
                    for h in range(2):
                        out_ref[ORDER[2 * b + h], :, columns] += value[64 * h : 64 * h + 64]
                out_ref[0, :, columns] = ends.T[0:64]
        else:
            for c in range(2):
                ends = nodebuf[it, c]
                rows = slice(8 + 256 * c, 264 + 256 * c)
                state[it + 1, rows, 0:512] += dot3(split(ends), (hr_hi[...], hr_lo[...]))
                state[it + 1, rows, 512:640] = jnp.where(
                    lax.broadcasted_iota(jnp.int32, (256, 128), 1) < S, ends, 0.0
                )
    ones = jnp.ones((8, 512), BF16)
    dot1 = lambda x: lax.dot_general(ones, x, NT, preferred_element_type=F32)
    row = lax.broadcasted_iota(jnp.int32, (8, 128), 0)
    packed = jnp.zeros((8, 128), F32)
    for j in range(5):
        pair = [ORDER[2 * j], ORDER[2 * j + 1]] if j < 4 else [0]
        values = [out_ref[level] for level in pair]
        values = jnp.concatenate(values if j < 4 else values + [jnp.zeros_like(values[0])], axis=0)
        high, low = split(values * values)
        packed = jnp.where(row == j, dot1(high) + dot1(low), packed)
    mysum[...] = packed
    sumbuf[lon] = packed
    columns = 512 * count

    def tell(d, carry):
        copy = remote(mysum, sumbuf.at[lon], sum_send.at[d], sum_recv.at[lon], {"lon": lax.rem(lon + d, count)})
        copy.start()
        return carry

    def told(d, carry):
        source = lax.rem(lon + count - d, count)
        copy = remote(mysum, sumbuf.at[source], sum_send.at[d], sum_recv.at[source], {"lon": source})
        copy.wait_recv()
        copy.wait_send()
        return carry

    lax.fori_loop(1, count, tell, 0)
    lax.fori_loop(1, count, told, 0)
    total = jnp.sum(sumbuf[...], axis=0) * (1.0 / columns)
    for j in range(9):
        level = (ORDER + (0,))[j]
        var_ref[level : level + 1, :] = total[j // 2 : j // 2 + 1, S * (j % 2) : S * (j % 2) + S]
    for copy in pending:
        copy.wait_send()


def vmem(count):
    return [pl.BlockSpec(memory_space=pltpu.VMEM)] * count


def two(shape):
    return [jax.ShapeDtypeStruct(shape, BF16)] * 2


def params(**more):
    return pltpu.CompilerParams(vmem_limit_bytes=60 * 2**20, **more)


def local(previous, loss_matrix, pair_matrix, diffusivity, mixing):
    count = lax.axis_size("lon")
    smem = pl.BlockSpec(memory_space=pltpu.SMEM)
    out = pl.pallas_call(
        setup_kernel,
        out_shape=two((512, 512)) + two((512, 128)) + two((128, 512)) + [jax.ShapeDtypeStruct((96, 128), F32)]
        + two((2, 256, 256)) + two((S, S)) + [jax.ShapeDtypeStruct((512, 640), F32), jax.ShapeDtypeStruct((8, 640), F32)],
        in_specs=[smem, smem] + vmem(3),
        out_specs=tuple(vmem(13)),
        scratch_shapes=[pltpu.VMEM((512, 512), F32)],
        compiler_params=params(),
    )(diffusivity, mixing, loss_matrix, pair_matrix, previous)
    g, hc, hr, pack = out[0:2], out[2:4], out[4:6], out[6]
    pairs, field, mixrow = out[7:11], out[11], out[12]
    packs = pl.pallas_call(
        gather_kernel,
        out_shape=jax.ShapeDtypeStruct((8, 96, 128), F32),
        in_specs=vmem(1),
        out_specs=vmem(1)[0],
        scratch_shapes=[pltpu.SemaphoreType.DMA((7,)), pltpu.SemaphoreType.DMA((7,)), pltpu.SemaphoreType.DMA],
        compiler_params=params(collective_id=0, has_side_effects=True),
    )(pack)
    weights = pl.pallas_call(
        interface_kernel,
        out_shape=two((256, 256)) + two((512, 256)) + two((256, 256)) * 2,
        in_specs=vmem(1),
        out_specs=tuple(vmem(8)),
        scratch_shapes=[pltpu.VMEM((512, 512), F32)] + [pltpu.VMEM((256, S), F32)] * 2
        + [pltpu.VMEM((S, 256), F32)] * 2 + [pltpu.VMEM((256, 256), F32)],
        compiler_params=params(),
    )(packs)
    return tuple(pl.pallas_call(
        functools.partial(solve_kernel, count),
        out_shape=[jax.ShapeDtypeStruct((9, S, 512), F32), jax.ShapeDtypeStruct((9, S), F32)],
        in_specs=vmem(20),
        out_specs=tuple(vmem(2)),
        scratch_shapes=[
            pltpu.VMEM((2, 528, 640), F32),
            pltpu.VMEM((512, 512), BF16),
            pltpu.VMEM((512, 512), BF16),
            pltpu.VMEM((2, 2, 256, 128), F32),
            pltpu.VMEM((2, 2, 256, 128), F32),
            pltpu.VMEM((2, 2, 128, 128), F32),
            pltpu.VMEM((2, 3, 128, 128), F32),
            pltpu.VMEM((2, 2, 256, 128), F32),
            pltpu.VMEM((2, 2, 256, 128), F32),
            pltpu.VMEM((2, 2, 8, 640), F32),
            pltpu.VMEM((512, 640), F32),
            pltpu.VMEM((8, 128), F32),
            pltpu.VMEM((count, 8, 128), F32),
            pltpu.SemaphoreType.DMA((2, 2)),
            pltpu.SemaphoreType.DMA((2, 2)),
            pltpu.SemaphoreType.DMA((2, 2)),
            pltpu.SemaphoreType.DMA((2, 2)),
            pltpu.SemaphoreType.DMA((2, 3)),
            pltpu.SemaphoreType.DMA((2, 3)),
            pltpu.SemaphoreType.DMA((count,)),
            pltpu.SemaphoreType.DMA((count,)),
        ],
        compiler_params=params(collective_id=1, has_side_effects=True),
    )(field, mixrow, *pairs, *g, *hc, *hr, *weights))


def solution(mesh):
    placed = (P("lev", None, "lon"), P("lev", None, None), P("lev", None, None), P("lev"), P("lev"))
    return jax.shard_map(
        local,
        mesh=mesh,
        in_specs=placed,
        out_specs=(P("lev", None, "lon"), P("lev", None)),
        check_vma=False,
    )
```

```python
import functools

import jax
import jax.numpy as jnp
from jax import lax
from jax.experimental import pallas as pl
from jax.experimental.pallas import tpu as pltpu
from jax.sharding import PartitionSpec as P

ITERS = 2
F32 = jnp.float32
BF16 = jnp.bfloat16
MESH = pl.DeviceIdType.MESH
HIGHEST = lax.Precision.HIGHEST

S = 64
ORDER = (1, 2, 3, 4, 6, 8, 7, 5)
NN = (((1,), (0,)), ((), ()))
NT = (((1,), (1,)), ((), ()))
TN = (((0,), (0,)), ((), ()))


def split(x):
    high = x.astype(BF16)
    return high, (x - high.astype(F32)).astype(BF16)


def dot3(a, b, dims=NN):
    one = lambda x, y: lax.dot_general(x, y, dims, preferred_element_type=F32)
    return one(a[0], b[0]) + (one(a[0], b[1]) + one(a[1], b[0]))


def mm(a, b, dims=NN):
    return dot3(split(a), split(b), dims)


def mm_full(a, b, dims=NN):
    return lax.dot_general(a, b, dims, precision=HIGHEST, preferred_element_type=F32)


def eye(n):
    rows = lax.broadcasted_iota(jnp.int32, (n, n), 0)
    return (rows == lax.broadcasted_iota(jnp.int32, (n, n), 1)).astype(F32)


def spd_inverses(blocks, low, high, doublings):
    centre, radius = 0.5 * (high + low), 0.5 * (high - low)
    units = [eye(block.shape[0]) for block in blocks]
    inverses = [unit * (1.0 / centre) for unit in units]
    residuals = [unit - block * (1.0 / centre) for unit, block in zip(units, blocks)]
    term = centre / radius
    for step in range(doublings):
        twice = 2.0 * term * term - 1.0
        gain, shift = 2.0 * term * term / twice, 1.0 / twice
        last = step == doublings - 1
        for i, unit in enumerate(units):
            n = unit.shape[0]
            rest = split(residuals[i])
            if step == 0:
                inverses[i] = (inverses[i] + residuals[i] * (1.0 / centre)) * gain
                if not last:
                    residuals[i] = gain * dot3(rest, rest) - shift * unit
                continue
            known = split(inverses[i])
            if last:
                inverses[i] = gain * (inverses[i] + dot3(known, rest))
                continue
            both = dot3(tuple(jnp.concatenate(p, axis=0) for p in zip(known, rest)), rest)
            inverses[i] = gain * (inverses[i] + both[:n])
            residuals[i] = gain * both[n:] - shift * unit
        term = twice
    exact = [unit - mm_full(block, inverse) for unit, block, inverse in zip(units, blocks, inverses)]
    return [inverse + mm(inverse, rest) for inverse, rest in zip(inverses, exact)]


def wide(grid):
    return jnp.concatenate([jnp.concatenate(row, axis=1) if len(row) > 1 else row[0] for row in grid], axis=0)


def interior(shunt, links):
    one = eye(S)
    zero = jnp.zeros((S, S), F32)
    diag = [shunt[i] + (links[i] + links[i + 1]) * one for i in range(8)]
    tie = [-links[i + 1] * one for i in range(7)]
    upper = wide([
        [diag[0], tie[0], zero, zero],
        [tie[0], diag[1], tie[1], zero],
        [zero, tie[1], diag[2], tie[2]],
        [zero, zero, tie[2], diag[3]],
    ])
    lower = wide([[diag[5], zero, tie[5]], [zero, diag[7], tie[6]], [tie[5], tie[6], diag[6]]])
    upper_inverse, = spd_inverses([upper], 77.0, 8700.0, 6)
    lower_inverse, = spd_inverses([lower], 117.0, 8700.0, 6)
    upper_t = links[4] * upper_inverse[192:256, :]
    lower_t = links[5] * lower_inverse[0:64, :]
    ground_up = jnp.concatenate([shunt[0] + links[0] * one, shunt[1], shunt[2], shunt[3]], axis=0)
    ground_low = jnp.concatenate([shunt[5], shunt[7] + links[8] * one, shunt[6]], axis=0)
    middle = shunt[4] + mm_full(upper_t, ground_up) + mm_full(lower_t, ground_low)
    middle_inverse, = spd_inverses([middle], 90.0, 4700.0, 5)
    spread = jnp.concatenate([upper_t, lower_t, one], axis=1)
    lifted = mm(middle_inverse, spread)
    return upper_inverse, lower_inverse, spread, lifted


def setup(link_ref, mix_ref, loss_ref, pair_ref, prev_ref, g_hi, g_lo, hc_hi, hc_lo, hr_hi, hr_lo, pack_ref,
                 pw_hi, pw_lo, pn_hi, pn_lo, field_ref, mixrow_ref, full):
    one = eye(S)
    links = [link_ref[i] for i in range(9)]
    shunt = [loss_ref[i] + one for i in range(9)]
    upper_inverse, lower_inverse, spread, lifted = interior(shunt[1:], links)
    inverse = mm(spread, lifted, TN)
    full[...] = inverse
    full[0:256, 0:256] += upper_inverse
    full[256:448, 256:448] += lower_inverse
    lane = lax.broadcasted_iota(jnp.int32, (512, 128), 1)
    columns = jnp.where(lane < S, links[0] * full[:, 0:128], links[8] * full[:, 256:384])
    hc_hi[...], hc_lo[...] = split(columns)
    rows = jnp.concatenate([links[0] * full[0:64, :], links[8] * full[320:384, :]], axis=0)
    hr_hi[...], hr_lo[...] = split(rows)
    g_hi[...], g_lo[...] = split(full[...])
    stack = jnp.concatenate([shunt[level] for level in ORDER], axis=0)
    ends = mm_full(rows, stack)
    across = links[8] * rows[0:64, 320:384]
    pack_ref[0:64, :] = jnp.concatenate([shunt[0] + ends[0:64], ends[64:128]], axis=1)
    pack_ref[64:96, :] = jnp.concatenate([across[0:32], across[32:64]], axis=1)
    for half in range(2):
        row = lax.broadcasted_iota(jnp.int32, (256, 256), 0) // S
        column = lax.broadcasted_iota(jnp.int32, (256, 256), 1) // S
        tall = jnp.concatenate([pair_ref[level] for level in ORDER[4 * half : 4 * half + 4]], axis=0)
        tall = jnp.concatenate([tall, tall], axis=1)
        tall = jnp.where(row == column, jnp.concatenate([tall, tall], axis=1), 0.0)
        pw_hi[half], pw_lo[half] = split(tall)
    pn_hi[...], pn_lo[...] = split(pair_ref[0])
    for j in range(4):
        both = jnp.concatenate([prev_ref[ORDER[2 * j]], prev_ref[ORDER[2 * j + 1]]], axis=0)
        field_ref[:, 128 * j : 128 * j + 128] = both.T
    last = jnp.concatenate([prev_ref[0], jnp.zeros_like(prev_ref[0])], axis=0)
    field_ref[:, 512:640] = last.T
    lane = lax.broadcasted_iota(jnp.int32, (8, 640), 1) // S
    row = jnp.zeros((8, 640), F32)
    for j, level in enumerate(ORDER + (0,)):
        row = jnp.where(lane == j, mix_ref[level], row)
    mixrow_ref[...] = row


def unpack(packs, q):
    both, folded = packs(q)
    across = jnp.concatenate([folded[:, 0:S], folded[:, S:]], axis=0)
    return both[:, 0:S], both[:, S:], across


def interface(pack_ref, own_hi, own_lo, msg_hi, msg_lo, rlo_hi, rlo_lo, rhi_hi, rhi_lo, full, wp, wc, rs, rc, own):
    chip = lax.axis_index("lev") // 2
    one = eye(S)
    zero = jnp.zeros((S, S), F32)
    here, below, across = zip(*[
        unpack(lambda q: (pack_ref[q, 0:64, :], pack_ref[q, 64:96, :]), q) for q in range(8)
    ])
    back = [a.T for a in across]
    ground = [here[q] + (below[q - 1] if q else 0.0) for q in range(8)]
    diag = [ground[q] + across[q] + (back[q - 1] if q else 0.0) for q in range(8)]
    upper = wide([
        [diag[0], -across[0], zero, zero],
        [-back[0], diag[1], -across[1], zero],
        [zero, -back[1], diag[2], -across[2]],
        [zero, zero, -back[2], diag[3]],
    ])
    lower = wide([
        [diag[5], -across[5], zero],
        [-back[5], diag[6], -across[6]],
        [zero, -back[6], diag[7]],
    ])
    first = chip < 2
    small = jnp.where(
        first, upper[0:128, 0:128], wide([[1000.0 * one, zero], [zero, diag[7]]])
    )
    upper_inverse, lower_inverse, small_inverse = spd_inverses([upper, lower, small], 9.0, 4700.0, 7)
    upper_t = mm(back[3], upper_inverse[192:256, :])
    lower_t = mm(across[4], lower_inverse[0:64, :])
    middle = (
        ground[4]
        + mm_full(upper_t, jnp.concatenate(ground[0:4], axis=0))
        + mm_full(lower_t, jnp.concatenate([ground[5], ground[6], ground[7] + across[7]], axis=0))
    )
    middle_inverse, = spd_inverses([middle], 9.0, 4700.0, 7)
    spread = jnp.concatenate([upper_t, lower_t, one], axis=1)
    lifted = mm(middle_inverse, spread)
    full[...] = mm(spread, lifted, TN)
    full[0:256, 0:256] += upper_inverse
    full[256:448, 256:448] += lower_inverse
    place = {0: 0, 1: 1, 2: 2, 3: 3, 4: 7, 5: 4, 6: 5, 7: 6}
    link = jnp.where(first, back[1], across[6])
    away = mm(link, small_inverse[64:128, :])

    def block(r, c):
        if r > 7 or c > 7:
            return zero
        r, c = place[r], place[c]
        return full[S * r : S * r + S, S * c : S * c + S]

    def blocks(rows, columns):
        return wide([[block(r, c) for c in columns] for r in rows])

    for c in range(4):
        nodes = (2 * c, 2 * c + 1, 2 * c + 1, 2 * c + 2)

        @pl.when(chip == c)
        def _(c=c, nodes=nodes):
            own[...] = blocks(nodes, nodes)
            wc[...] = blocks(nodes, (4,))
            if c in (0, 3):
                far = [away[:, 0:64], away[:, 64:128]]
                if c == 0:
                    rs[...] = jnp.concatenate([far[0], far[1], far[1], one], axis=1)
                    wp[...] = jnp.concatenate([far[0].T, far[1].T, far[1].T, one], axis=0)
                else:
                    rs[...] = jnp.concatenate([one, far[1], far[1], zero], axis=1)
                    wp[...] = jnp.concatenate([one, far[1].T, far[1].T, zero], axis=0)
            else:
                gate = 2 if c == 1 else 6
                rs[...] = blocks((gate,), nodes)
                wp[...] = blocks(nodes, (gate,))

            def seen(n):
                if n > 7:
                    return zero
                n = place[n]
                return spread[:, S * n : S * n + S]

            rc[...] = jnp.concatenate([seen(n) for n in nodes], axis=1)

    own_hi[...], own_lo[...] = split(own[...])
    none = jnp.zeros((256, S), F32)
    msg = wide([[wp[...], none, wc[...], none], [none, wp[...], none, wc[...]]])
    msg_hi[...], msg_lo[...] = split(msg)
    none = jnp.zeros((S, 256), F32)
    rlo_hi[...], rlo_lo[...] = split(jnp.concatenate([rs[...], none, rc[...], none], axis=0))
    rhi_hi[...], rhi_lo[...] = split(jnp.concatenate([none, rs[...], none, rc[...]], axis=0))


def kernel(count, link_ref, mix_ref, loss_ref, pair_ref, prev_ref, out_ref, var_ref,
           g_hi, g_lo, hc_hi, hc_lo, hr_hi, hr_lo, pack, pw_hi, pw_lo, pn_hi, pn_lo, field_ref, mixrow_ref, full,
           packs, own_hi, own_lo, msg_hi, msg_lo, rlo_hi, rlo_lo, rhi_hi, rhi_lo, wp, wc, rs, rc, own,
           state, gs_hi, gs_lo, gnode, injs, outgo, incoming, nodes, nodebuf, halo, sums, mysum, sumbuf,
           pack_send, pack_recv, halo_send, halo_recv, part_send, part_recv, msg_send, msg_recv, sum_send, sum_recv):
    lev = lax.axis_index("lev")
    lon = lax.axis_index("lon")
    core = lax.rem(lev, 2)
    chip = lev // 2
    partner = lev + 1 - 2 * core
    sibling_chip = chip + 1 - 2 * lax.rem(chip, 2)
    across_base = 2 - 2 * (chip // 2)
    sibling = 2 * sibling_chip + core
    far = lax.rem(chip + 2, 4)
    across = [2 * far + core, 2 * (2 * across_base + 1 - far) + core]
    west, east = lax.rem(lon + count - 1, count), lax.rem(lon + 1, count)

    barrier = pltpu.get_barrier_semaphore()
    others = [lax.rem(lev + d, 8) for d in range(1, 8)]
    for other in others:
        pl.semaphore_signal(barrier, inc=1, device_id={"lev": other}, device_id_type=MESH)

    def greet(d, carry):
        pl.semaphore_signal(barrier, inc=1, device_id={"lon": lax.rem(lon + d, count)}, device_id_type=MESH)
        return carry

    lax.fori_loop(1, count, greet, 0)

    def remote(src, dst, send, recv, where):
        return pltpu.make_async_remote_copy(
            src_ref=src, dst_ref=dst, send_sem=send, recv_sem=recv, device_id=where, device_id_type=MESH
        )

    setup(link_ref, mix_ref, loss_ref, pair_ref, prev_ref, g_hi, g_lo, hc_hi, hc_lo, hr_hi, hr_lo, pack,
          pw_hi, pw_lo, pn_hi, pn_lo, field_ref, mixrow_ref, full)
    pl.semaphore_wait(barrier, 6 + count)
    spread = []
    for d, other in enumerate(others):
        copy = remote(pack, packs.at[lev], pack_send.at[d], pack_recv.at[d], {"lev": other})
        copy.start()
        spread.append(copy)
    packs[lev] = pack[...]
    state[0, 8:520, :] = field_ref[...]
    def product(it):
        if it == ITERS - 1:
            for c in range(0, 512, 256):
                parts = (gs_hi[c : c + 256, :], gs_lo[c : c + 256, :])
                for b in range(4):
                    rows = slice(128 * b, 128 * b + 128)
                    value = dot3((g_hi[rows, :], g_lo[rows, :]), parts, NT)
                    for h in range(2):
                        out_ref[ORDER[2 * b + h], :, c : c + 256] = value[64 * h : 64 * h + 64]
        else:
            for r in range(0, 512, 128):
                parts = (gs_hi[r : r + 128, :], gs_lo[r : r + 128, :])
                state[it + 1, 8 + r : 136 + r, 0:512] = dot3(parts, (g_hi[...], g_lo[...]))

    mix_row = mixrow_ref[0:1, :]
    pending = []
    for it in range(ITERS):
        final = it == ITERS - 1
        now = state.at[it]
        first = field_ref.at[0:8] if it == 0 else now.at[8:16]
        last = field_ref.at[504:512] if it == 0 else now.at[512:520]
        to_west = remote(first, halo.at[it, 1], halo_send.at[it, 0], halo_recv.at[it, 1], {"lon": west})
        to_east = remote(last, halo.at[it, 0], halo_send.at[it, 1], halo_recv.at[it, 0], {"lon": east})
        to_west.start()
        to_east.start()
        pending += [to_west, to_east]
        for r in range(0, 512, 128):
            here = state[it, 8 + r : 136 + r, :]
            squares = split(here * here)
            for half in range(2):
                piece = tuple(s[:, 256 * half : 256 * half + 256] for s in squares)
                out = dot3(piece, (pw_hi[half], pw_lo[half]), NT)
                sums[r : r + 128, 256 * half : 256 * half + 256] = out
            piece = tuple(s[:, 512:576] for s in squares)
            sums[r : r + 128, 512:576] = dot3(piece, (pn_hi[...], pn_lo[...]), NT)
        to_west.wait_recv()
        to_east.wait_recv()
        state[it, 0:8, :] = halo[it, 0]
        state[it, 520:528, :] = halo[it, 1]
        for r in range(0, 512, 128):
            here = state[it, 8 + r : 136 + r, 0:576]
            around = state[it, 7 + r : 135 + r, 0:576] + state[it, 9 + r : 137 + r, 0:576]
            forcing = field_ref[r : r + 128, 0:576] - sums[r : r + 128, 0:576] + mix_row[:, 0:576] * (around - 2.0 * here)
            parts = split(forcing[:, 0:512])
            gs_hi[r : r + 128, :], gs_lo[r : r + 128, :] = parts
            node = forcing[:, 512:576]
            push = dot3(parts, (hc_hi[...], hc_lo[...])) + jnp.concatenate([node, jnp.zeros_like(node)], axis=1)
            injs[it, r // 256, r % 256 : r % 256 + 128, :] = push
        give = remote(injs.at[it, 1 - core], gnode.at[it, core], part_send.at[it, 0], part_recv.at[it, 0], {"lev": partner})
        give.start()
        gnode[it, core] = injs[it, core]
        if it == 0:
            product(it)
            for copy in spread:
                copy.wait()
            interface(packs, own_hi, own_lo, msg_hi, msg_lo, rlo_hi, rlo_lo, rhi_hi, rhi_lo, full, wp, wc, rs, rc, own)
        give.wait()
        inj = jnp.concatenate([gnode[it, 0], gnode[it, 1]], axis=1)
        packed = split(jnp.concatenate([inj[0:128], inj[128:256]], axis=1))
        message = dot3(packed, (msg_hi[...], msg_lo[...]))
        outgo[it, 0] = message[:, 0:128]
        outgo[it, 1] = message[:, 128:256]
        sends = [
            remote(outgo.at[it, 1], incoming.at[it, 1 + lax.rem(chip, 2)], msg_send.at[it, 1],
                   msg_recv.at[it, 1 + lax.rem(chip, 2)], {"lev": across[0]}),
            remote(outgo.at[it, 1], incoming.at[it, 1 + lax.rem(chip, 2)], msg_send.at[it, 2],
                   msg_recv.at[it, 1 + lax.rem(chip, 2)], {"lev": across[1]}),
            remote(outgo.at[it, 0], incoming.at[it, 0], msg_send.at[it, 0], msg_recv.at[it, 0], {"lev": sibling}),
        ]
        for send in sends:
            send.start()
        mine = dot3(split(inj), (own_hi[...], own_lo[...]))
        if it:
            product(it)
        for slot in range(3):
            arrive = remote(outgo.at[it, 0], incoming.at[it, slot], msg_send.at[it, 0], msg_recv.at[it, slot], {"lev": sibling})
            arrive.wait_recv()
        for send in sends:
            send.wait_send()
        heard = split(jnp.concatenate([incoming[it, 0], incoming[it, 1] + incoming[it, 2]], axis=1))
        total = mine + jnp.concatenate(
            [dot3(heard, (rlo_hi[...], rlo_lo[...])), dot3(heard, (rhi_hi[...], rhi_lo[...]))], axis=0
        )
        nodes[it, 0] = total[:, 0:128]
        nodes[it, 1] = total[:, 128:256]
        give = remote(nodes.at[it, 1 - core], nodebuf.at[it, core], part_send.at[it, 1], part_recv.at[it, 1], {"lev": partner})
        give.start()
        nodebuf[it, core] = nodes[it, core]
        give.wait()
        if final:
            for c in range(2):
                ends = nodebuf[it, c]
                parts = split(ends)
                columns = slice(256 * c, 256 * c + 256)
                for b in range(4):
                    rows = slice(128 * b, 128 * b + 128)
                    value = dot3((hc_hi[rows, :], hc_lo[rows, :]), parts, NT)
                    for h in range(2):
                        out_ref[ORDER[2 * b + h], :, columns] += value[64 * h : 64 * h + 64]
                out_ref[0, :, columns] = ends.T[0:64]
        else:
            for c in range(2):
                ends = nodebuf[it, c]
                rows = slice(8 + 256 * c, 264 + 256 * c)
                state[it + 1, rows, 0:512] += dot3(split(ends), (hr_hi[...], hr_lo[...]))
                state[it + 1, rows, 512:640] = jnp.where(
                    lax.broadcasted_iota(jnp.int32, (256, 128), 1) < S, ends, 0.0
                )
    ones = jnp.ones((8, 512), BF16)
    dot1 = lambda x: lax.dot_general(ones, x, NT, preferred_element_type=F32)
    row = lax.broadcasted_iota(jnp.int32, (8, 128), 0)
    packed = jnp.zeros((8, 128), F32)
    for j in range(5):
        pair = [ORDER[2 * j], ORDER[2 * j + 1]] if j < 4 else [0]
        values = [out_ref[level] for level in pair]
        values = jnp.concatenate(values if j < 4 else values + [jnp.zeros_like(values[0])], axis=0)
        high, low = split(values * values)
        packed = jnp.where(row == j, dot1(high) + dot1(low), packed)
    mysum[...] = packed
    sumbuf[lon] = packed
    columns = 512 * count

    def tell(d, carry):
        copy = remote(mysum, sumbuf.at[lon], sum_send.at[d], sum_recv.at[lon], {"lon": lax.rem(lon + d, count)})
        copy.start()
        return carry

    def told(d, carry):
        source = lax.rem(lon + count - d, count)
        copy = remote(mysum, sumbuf.at[source], sum_send.at[d], sum_recv.at[source], {"lon": source})
        copy.wait_recv()
        copy.wait_send()
        return carry

    lax.fori_loop(1, count, tell, 0)
    lax.fori_loop(1, count, told, 0)
    total = jnp.sum(sumbuf[...], axis=0) * (1.0 / columns)
    for j in range(9):
        level = (ORDER + (0,))[j]
        var_ref[level : level + 1, :] = total[j // 2 : j // 2 + 1, S * (j % 2) : S * (j % 2) + S]
    for copy in pending:
        copy.wait_send()


def vmem(count):
    return [pl.BlockSpec(memory_space=pltpu.VMEM)] * count


def local(previous, loss_matrix, pair_matrix, diffusivity, mixing):
    count = lax.axis_size("lon")
    smem = pl.BlockSpec(memory_space=pltpu.SMEM)
    low = lambda *shape: [pltpu.VMEM(shape, BF16)] * 2
    full = lambda *shape: [pltpu.VMEM(shape, F32)]
    sems = lambda *shape: [pltpu.SemaphoreType.DMA(shape)] * 2
    scratch = low(512, 512) + low(512, 128) + low(128, 512) + full(96, 128) + low(2, 256, 256) + low(S, S)
    scratch += full(512, 640) + full(8, 640) + full(512, 512)
    scratch += full(8, 96, 128) + low(256, 256) + low(512, 256) + low(256, 256) * 2
    scratch += full(256, S) * 2 + full(S, 256) * 2 + full(256, 256)
    scratch += full(2, 528, 640) + low(512, 512) + full(2, 2, 256, 128) * 2 + full(2, 2, 128, 128) + full(2, 3, 128, 128)
    scratch += full(2, 2, 256, 128) * 2 + full(2, 2, 8, 640) + full(512, 640) + full(8, 128) + full(count, 8, 128)
    scratch += sems(7) + sems(2, 2) + sems(2, 2) + sems(2, 3) + sems(count)
    return tuple(pl.pallas_call(
        functools.partial(kernel, count),
        out_shape=[jax.ShapeDtypeStruct((9, S, 512), F32), jax.ShapeDtypeStruct((9, S), F32)],
        in_specs=[smem, smem] + vmem(3),
        out_specs=tuple(vmem(2)),
        scratch_shapes=scratch,
        compiler_params=pltpu.CompilerParams(vmem_limit_bytes=60 * 2**20, collective_id=0, has_side_effects=True),
    )(diffusivity, mixing, loss_matrix, pair_matrix, previous))


def solution(mesh):
    placed = (P("lev", None, "lon"), P("lev", None, None), P("lev", None, None), P("lev"), P("lev"))
    return jax.shard_map(
        local,
        mesh=mesh,
        in_specs=placed,
        out_specs=(P("lev", None, "lon"), P("lev", None)),
        check_vma=False,
    )
```

```python
import functools

import jax
import jax.numpy as jnp
from jax import lax
from jax.experimental import pallas as pl
from jax.experimental.pallas import tpu as pltpu
from jax.sharding import PartitionSpec as P

ITERS = 2
F32 = jnp.float32
BF16 = jnp.bfloat16
MESH = pl.DeviceIdType.MESH
HIGHEST = lax.Precision.HIGHEST

S = 64
ORDER = (1, 2, 4, 5, 7, 8, 3, 6)
NN = (((1,), (0,)), ((), ()))
NT = (((1,), (1,)), ((), ()))
TN = (((0,), (0,)), ((), ()))


def split(x):
    high = x.astype(BF16)
    return high, (x - high.astype(F32)).astype(BF16)


def dot3(a, b, dims=NN):
    one = lambda x, y: lax.dot_general(x, y, dims, preferred_element_type=F32)
    return one(a[0], b[0]) + (one(a[0], b[1]) + one(a[1], b[0]))


def mm(a, b, dims=NN):
    return dot3(split(a), split(b), dims)


def mm_full(a, b, dims=NN):
    return lax.dot_general(a, b, dims, precision=HIGHEST, preferred_element_type=F32)


def eye(n):
    rows = lax.broadcasted_iota(jnp.int32, (n, n), 0)
    return (rows == lax.broadcasted_iota(jnp.int32, (n, n), 1)).astype(F32)


def spd_inverses(blocks, lows, high, doublings):
    centres = [0.5 * (high + low) for low in lows]
    units = [eye(block.shape[0]) for block in blocks]
    inverses = [unit * (1.0 / centre) for unit, centre in zip(units, centres)]
    residuals = [unit - block * (1.0 / centre) for unit, block, centre in zip(units, blocks, centres)]
    terms = [(high + low) / (high - low) for low in lows]
    for step in range(doublings):
        last = step == doublings - 1
        for i, unit in enumerate(units):
            twice = 2.0 * terms[i] * terms[i] - 1.0
            gain, shift = (twice + 1.0) / twice, 1.0 / twice
            terms[i] = twice
            centre = centres[i]
            n = unit.shape[0]
            rest = split(residuals[i])
            if step == 0:
                inverses[i] = (inverses[i] + residuals[i] * (1.0 / centre)) * gain
                if not last:
                    residuals[i] = gain * dot3(rest, rest) - shift * unit
                continue
            known = split(inverses[i])
            if last:
                inverses[i] = gain * (inverses[i] + dot3(known, rest))
                continue
            both = dot3(tuple(jnp.concatenate(p, axis=0) for p in zip(known, rest)), rest)
            inverses[i] = gain * (inverses[i] + both[:n])
            residuals[i] = gain * both[n:] - shift * unit
    exact = [unit - mm_full(block, inverse) for unit, block, inverse in zip(units, blocks, inverses)]
    step = lambda x, y: lax.dot_general(x.astype(BF16), y.astype(BF16), NN, preferred_element_type=F32)
    return [inverse + step(inverse, rest) for inverse, rest in zip(inverses, exact)]


def wide(grid):
    return jnp.concatenate([jnp.concatenate(row, axis=1) if len(row) > 1 else row[0] for row in grid], axis=0)


def interior(link_ref, loss_ref, hr_hi, hr_lo, pack_ref, fill):
    one = eye(S)
    zero = jnp.zeros((S, S), F32)
    links = [link_ref[i] for i in range(9)]
    shunt = [loss_ref[i] + one for i in range(9)]
    blocks = []
    for top in (1, 4, 7):
        diag = [shunt[level] + (links[level - 1] + links[level]) * one for level in (top, top + 1)]
        tie = -links[top] * one
        blocks.append(wide([[diag[0], tie], [tie, diag[1]]]))
    pairs = spd_inverses(blocks, [199.0] * 3, 6700.0, 5)
    none = jnp.zeros((S, 128), F32)
    spread = wide([
        [links[2] * pairs[0][S:], links[3] * pairs[1][:S], none],
        [none, links[5] * pairs[1][S:], links[6] * pairs[2][:S]],
    ])
    ground = jnp.concatenate(
        [shunt[1] + links[0] * one, shunt[2], shunt[4], shunt[5], shunt[7], shunt[8] + links[8] * one], axis=0
    )
    own = jnp.concatenate([shunt[3], shunt[6]], axis=0) + mm_full(spread, ground)
    down = links[5] * spread[0:S, 192:256]
    up = links[3] * spread[S:, 128:192]
    fill()
    middle, = spd_inverses([wide([[own[:S] + down, -down], [-up, own[S:] + up]])], [68.6], 3010.0, 5)
    spread = jnp.concatenate([spread, eye(128)], axis=1)
    lifted = mm(middle, spread)
    lane = lax.broadcasted_iota(jnp.int32, (128, 128), 1)
    ends = mm(jnp.where(lane < S, spread[:, 0:128], spread[:, 256:384]), lifted, TN)
    first = jnp.concatenate([ends[0:S, 0:128] + pairs[0][:S], ends[0:S, 128:512]], axis=1)
    last = jnp.concatenate([ends[S:, 0:256], ends[S:, 256:384] + pairs[2][S:], ends[S:, 384:512]], axis=1)
    rows = jnp.concatenate([links[0] * first, links[8] * last], axis=0)
    hr_hi[...], hr_lo[...] = split(rows)
    loads = mm_full(rows, jnp.concatenate([shunt[level] for level in ORDER], axis=0))
    across = links[8] * rows[0:S, 320:384]
    pack_ref[0:64, :] = jnp.concatenate([shunt[0] + loads[0:S], loads[S:]], axis=1)
    pack_ref[64:96, :] = jnp.concatenate([across[0:32], across[32:64]], axis=1)
    return pairs, spread, lifted


def finish_interior(link_ref, pairs, spread, lifted, g_hi, g_lo, hc_hi, hc_lo, full):
    full[...] = mm(spread, lifted, TN)
    for i in range(3):
        at = slice(128 * i, 128 * i + 128)
        full[at, at] += pairs[i]
    lane = lax.broadcasted_iota(jnp.int32, (512, 128), 1)
    hc_hi[...], hc_lo[...] = split(jnp.where(lane < S, link_ref[0] * full[:, 0:128], link_ref[8] * full[:, 256:384]))
    g_hi[...], g_lo[...] = split(full[...])


def pair_weights(pair_ref, pw_hi, pw_lo, pn_hi, pn_lo):
    for half in range(2):
        row = lax.broadcasted_iota(jnp.int32, (256, 256), 0) // S
        column = lax.broadcasted_iota(jnp.int32, (256, 256), 1) // S
        tall = jnp.concatenate([pair_ref[level] for level in ORDER[4 * half : 4 * half + 4]], axis=0)
        tall = jnp.concatenate([tall, tall], axis=1)
        tall = jnp.where(row == column, jnp.concatenate([tall, tall], axis=1), 0.0)
        pw_hi[half], pw_lo[half] = split(tall)
    pn_hi[...], pn_lo[...] = split(pair_ref[0])


def field_of(prev_ref, field_ref):
    for j in range(4):
        both = jnp.concatenate([prev_ref[ORDER[2 * j]], prev_ref[ORDER[2 * j + 1]]], axis=0)
        field_ref[:, 128 * j : 128 * j + 128] = both.T
    last = jnp.concatenate([prev_ref[0], jnp.zeros_like(prev_ref[0])], axis=0)
    field_ref[:, 512:640] = last.T


def mix_row_of(mix_ref, mixrow_ref):
    lane = lax.broadcasted_iota(jnp.int32, (8, 640), 1) // S
    row = jnp.zeros((8, 640), F32)
    for j, level in enumerate(ORDER + (0,)):
        row = jnp.where(lane == j, mix_ref[level], row)
    mixrow_ref[...] = row


def unpack(packs, q):
    both, folded = packs(q)
    across = jnp.concatenate([folded[:, 0:S], folded[:, S:]], axis=0)
    return both[:, 0:S], both[:, S:], across


def interface(pack_ref, own_hi, own_lo, msg_hi, msg_lo, rlo_hi, rlo_lo, rhi_hi, rhi_lo, full, wp, wc, rs, rc, own):
    chip = lax.axis_index("lev") // 2
    one = eye(S)
    zero = jnp.zeros((S, S), F32)
    here, below, across = zip(*[
        unpack(lambda q: (pack_ref[q, 0:64, :], pack_ref[q, 64:96, :]), q) for q in range(8)
    ])
    back = [a.T for a in across]
    ground = [here[q] + (below[q - 1] if q else 0.0) for q in range(8)]
    diag = [ground[q] + across[q] + (back[q - 1] if q else 0.0) for q in range(8)]
    upper = wide([
        [diag[0], -across[0], zero, zero],
        [-back[0], diag[1], -across[1], zero],
        [zero, -back[1], diag[2], -across[2]],
        [zero, zero, -back[2], diag[3]],
    ])
    lower = wide([
        [diag[5], -across[5], zero],
        [-back[5], diag[6], -across[6]],
        [zero, -back[6], diag[7]],
    ])
    first = chip < 2
    small = jnp.where(
        first, upper[0:128, 0:128], wide([[500.0 * one, zero], [zero, diag[7]]])
    )
    upper_inverse, lower_inverse, small_inverse = spd_inverses(
        [upper, lower, small], [9.6, 21.0, 13.9], 2400.0, 6
    )
    upper_t = mm(back[3], upper_inverse[192:256, :])
    lower_t = mm(across[4], lower_inverse[0:64, :])
    middle = (
        ground[4]
        + mm_full(upper_t, jnp.concatenate(ground[0:4], axis=0))
        + mm_full(lower_t, jnp.concatenate([ground[5], ground[6], ground[7] + across[7]], axis=0))
    )
    middle_inverse, = spd_inverses([middle], [28.7], 2400.0, 5)
    spread = jnp.concatenate([upper_t, lower_t, one], axis=1)
    lifted = mm(middle_inverse, spread)
    full[...] = mm(spread, lifted, TN)
    full[0:256, 0:256] += upper_inverse
    full[256:448, 256:448] += lower_inverse
    place = {0: 0, 1: 1, 2: 2, 3: 3, 4: 7, 5: 4, 6: 5, 7: 6}
    link = jnp.where(first, back[1], across[6])
    away = mm(link, small_inverse[64:128, :])

    def block(r, c):
        if r > 7 or c > 7:
            return zero
        r, c = place[r], place[c]
        return full[S * r : S * r + S, S * c : S * c + S]

    def blocks(rows, columns):
        return wide([[block(r, c) for c in columns] for r in rows])

    for c in range(4):
        nodes = (2 * c, 2 * c + 1, 2 * c + 1, 2 * c + 2)

        @pl.when(chip == c)
        def _(c=c, nodes=nodes):
            own[...] = blocks(nodes, nodes)
            wc[...] = blocks(nodes, (4,))
            if c in (0, 3):
                far = [away[:, 0:64], away[:, 64:128]]
                if c == 0:
                    rs[...] = jnp.concatenate([far[0], far[1], far[1], one], axis=1)
                    wp[...] = jnp.concatenate([far[0].T, far[1].T, far[1].T, one], axis=0)
                else:
                    rs[...] = jnp.concatenate([one, far[1], far[1], zero], axis=1)
                    wp[...] = jnp.concatenate([one, far[1].T, far[1].T, zero], axis=0)
            else:
                gate = 2 if c == 1 else 6
                rs[...] = blocks((gate,), nodes)
                wp[...] = blocks(nodes, (gate,))

            def seen(n):
                if n > 7:
                    return zero
                n = place[n]
                return spread[:, S * n : S * n + S]

            rc[...] = jnp.concatenate([seen(n) for n in nodes], axis=1)

    own_hi[...], own_lo[...] = split(own[...])
    none = jnp.zeros((256, S), F32)
    msg = wide([[wp[...], none, wc[...], none], [none, wp[...], none, wc[...]]])
    msg_hi[...], msg_lo[...] = split(msg)
    none = jnp.zeros((S, 256), F32)
    rlo_hi[...], rlo_lo[...] = split(jnp.concatenate([rs[...], none, rc[...], none], axis=0))
    rhi_hi[...], rhi_lo[...] = split(jnp.concatenate([none, rs[...], none, rc[...]], axis=0))


def kernel(count, link_hbm, mix_hbm, loss_hbm, pair_hbm, prev_hbm, out_ref, var_ref,
           link_ref, mix_ref, loss_ref, pair_ref, prev_ref, load_sem,
           g_hi, g_lo, hc_hi, hc_lo, hr_hi, hr_lo, pack, pw_hi, pw_lo, pn_hi, pn_lo, field_ref, mixrow_ref, full,
           packs, own_hi, own_lo, msg_hi, msg_lo, rlo_hi, rlo_lo, rhi_hi, rhi_lo, wp, wc, rs, rc, own,
           state, gs_hi, gs_lo, gnode, injs, outgo, incoming, nodes, nodebuf, halo, sums, mysum, sumbuf,
           pack_send, pack_recv, halo_send, halo_recv, part_send, part_recv, msg_send, msg_recv, sum_send, sum_recv):
    lev = lax.axis_index("lev")
    lon = lax.axis_index("lon")
    core = lax.rem(lev, 2)
    chip = lev // 2
    partner = lev + 1 - 2 * core
    sibling_chip = chip + 1 - 2 * lax.rem(chip, 2)
    across_base = 2 - 2 * (chip // 2)
    sibling = 2 * sibling_chip + core
    far = lax.rem(chip + 2, 4)
    across = [2 * far + core, 2 * (2 * across_base + 1 - far) + core]
    west, east = lax.rem(lon + count - 1, count), lax.rem(lon + 1, count)

    loads = [
        pltpu.make_async_copy(src, dst, load_sem.at[i])
        for i, (src, dst) in enumerate([
            (link_hbm, link_ref), (loss_hbm, loss_ref), (prev_hbm, prev_ref), (pair_hbm, pair_ref), (mix_hbm, mix_ref),
        ])
    ]
    for load in loads:
        load.start()
    barrier = pltpu.get_barrier_semaphore()
    others = [lax.rem(lev + d, 8) for d in range(1, 8)]
    for other in others:
        pl.semaphore_signal(barrier, inc=1, device_id={"lev": other}, device_id_type=MESH)

    def greet(d, carry):
        pl.semaphore_signal(barrier, inc=1, device_id={"lon": lax.rem(lon + d, count)}, device_id_type=MESH)
        return carry

    lax.fori_loop(1, count, greet, 0)

    def remote(src, dst, send, recv, where):
        return pltpu.make_async_remote_copy(
            src_ref=src, dst_ref=dst, send_sem=send, recv_sem=recv, device_id=where, device_id_type=MESH
        )


    def fill():
        loads[2].wait()
        field_of(prev_ref, field_ref)

    loads[0].wait()
    loads[1].wait()
    parts = interior(link_ref, loss_ref, hr_hi, hr_lo, pack, fill)
    pl.semaphore_wait(barrier, 6 + count)
    spread = []
    for d, other in enumerate(others):
        copy = remote(pack, packs.at[lev], pack_send.at[d], pack_recv.at[d], {"lev": other})
        copy.start()
        spread.append(copy)
    packs[lev] = pack[...]
    state[0, 8:520, :] = field_ref[...]
    def product(it):
        if it == ITERS - 1:
            for c in range(0, 512, 256):
                parts = (gs_hi[c : c + 256, :], gs_lo[c : c + 256, :])
                for b in range(4):
                    rows = slice(128 * b, 128 * b + 128)
                    value = dot3((g_hi[rows, :], g_lo[rows, :]), parts, NT)
                    for h in range(2):
                        out_ref[ORDER[2 * b + h], :, c : c + 256] = value[64 * h : 64 * h + 64]
        else:
            for r in range(0, 512, 128):
                parts = (gs_hi[r : r + 128, :], gs_lo[r : r + 128, :])
                state[it + 1, 8 + r : 136 + r, 0:512] = dot3(parts, (g_hi[...], g_lo[...]))

    pending = []
    for it in range(ITERS):
        final = it == ITERS - 1
        now = state.at[it]
        first = field_ref.at[0:8] if it == 0 else now.at[8:16]
        last = field_ref.at[504:512] if it == 0 else now.at[512:520]
        to_west = remote(first, halo.at[it, 1], halo_send.at[it, 0], halo_recv.at[it, 1], {"lon": west})
        to_east = remote(last, halo.at[it, 0], halo_send.at[it, 1], halo_recv.at[it, 0], {"lon": east})
        to_west.start()
        to_east.start()
        pending += [to_west, to_east]
        if it == 0:
            loads[3].wait()
            loads[4].wait()
            mix_row_of(mix_ref, mixrow_ref)
            pair_weights(pair_ref, pw_hi, pw_lo, pn_hi, pn_lo)
            finish_interior(link_ref, *parts, g_hi, g_lo, hc_hi, hc_lo, full)
        for r in range(0, 512, 128):
            here = state[it, 8 + r : 136 + r, :]
            squares = split(here * here)
            for half in range(2):
                piece = tuple(s[:, 256 * half : 256 * half + 256] for s in squares)
                out = dot3(piece, (pw_hi[half], pw_lo[half]), NT)
                sums[r : r + 128, 256 * half : 256 * half + 256] = out
            piece = tuple(s[:, 512:576] for s in squares)
            sums[r : r + 128, 512:576] = dot3(piece, (pn_hi[...], pn_lo[...]), NT)
        to_west.wait_recv()
        to_east.wait_recv()
        state[it, 0:8, :] = halo[it, 0]
        state[it, 520:528, :] = halo[it, 1]
        for r in range(0, 512, 128):
            here = state[it, 8 + r : 136 + r, 0:576]
            around = state[it, 7 + r : 135 + r, 0:576] + state[it, 9 + r : 137 + r, 0:576]
            forcing = field_ref[r : r + 128, 0:576] - sums[r : r + 128, 0:576] + mixrow_ref[0:1, 0:576] * (around - 2.0 * here)
            parts = split(forcing[:, 0:512])
            gs_hi[r : r + 128, :], gs_lo[r : r + 128, :] = parts
            node = forcing[:, 512:576]
            push = dot3(parts, (hc_hi[...], hc_lo[...])) + jnp.concatenate([node, jnp.zeros_like(node)], axis=1)
            injs[it, r // 256, r % 256 : r % 256 + 128, :] = push
        give = remote(injs.at[it, 1 - core], gnode.at[it, core], part_send.at[it, 0], part_recv.at[it, 0], {"lev": partner})
        give.start()
        gnode[it, core] = injs[it, core]
        if it == 0:
            product(it)
            for copy in spread:
                copy.wait()
            interface(packs, own_hi, own_lo, msg_hi, msg_lo, rlo_hi, rlo_lo, rhi_hi, rhi_lo, full, wp, wc, rs, rc, own)
        give.wait()
        inj = jnp.concatenate([gnode[it, 0], gnode[it, 1]], axis=1)
        packed = split(jnp.concatenate([inj[0:128], inj[128:256]], axis=1))
        message = dot3(packed, (msg_hi[...], msg_lo[...]))
        outgo[it, 0] = message[:, 0:128]
        outgo[it, 1] = message[:, 128:256]
        sends = [
            remote(outgo.at[it, 1], incoming.at[it, 1 + lax.rem(chip, 2)], msg_send.at[it, 1],
                   msg_recv.at[it, 1 + lax.rem(chip, 2)], {"lev": across[0]}),
            remote(outgo.at[it, 1], incoming.at[it, 1 + lax.rem(chip, 2)], msg_send.at[it, 2],
                   msg_recv.at[it, 1 + lax.rem(chip, 2)], {"lev": across[1]}),
            remote(outgo.at[it, 0], incoming.at[it, 0], msg_send.at[it, 0], msg_recv.at[it, 0], {"lev": sibling}),
        ]
        for send in sends:
            send.start()
        mine = dot3(split(inj), (own_hi[...], own_lo[...]))
        if it:
            product(it)
        for slot in range(3):
            arrive = remote(outgo.at[it, 0], incoming.at[it, slot], msg_send.at[it, 0], msg_recv.at[it, slot], {"lev": sibling})
            arrive.wait_recv()
        for send in sends:
            send.wait_send()
        heard = split(jnp.concatenate([incoming[it, 0], incoming[it, 1] + incoming[it, 2]], axis=1))
        total = mine + jnp.concatenate(
            [dot3(heard, (rlo_hi[...], rlo_lo[...])), dot3(heard, (rhi_hi[...], rhi_lo[...]))], axis=0
        )
        nodes[it, 0] = total[:, 0:128]
        nodes[it, 1] = total[:, 128:256]
        give = remote(nodes.at[it, 1 - core], nodebuf.at[it, core], part_send.at[it, 1], part_recv.at[it, 1], {"lev": partner})
        give.start()
        nodebuf[it, core] = nodes[it, core]
        give.wait()
        if final:
            for c in range(2):
                ends = nodebuf[it, c]
                parts = split(ends)
                columns = slice(256 * c, 256 * c + 256)
                for b in range(4):
                    rows = slice(128 * b, 128 * b + 128)
                    value = dot3((hc_hi[rows, :], hc_lo[rows, :]), parts, NT)
                    for h in range(2):
                        out_ref[ORDER[2 * b + h], :, columns] += value[64 * h : 64 * h + 64]
                out_ref[0, :, columns] = ends.T[0:64]
        else:
            for c in range(2):
                ends = nodebuf[it, c]
                rows = slice(8 + 256 * c, 264 + 256 * c)
                state[it + 1, rows, 0:512] += dot3(split(ends), (hr_hi[...], hr_lo[...]))
                state[it + 1, rows, 512:640] = jnp.where(
                    lax.broadcasted_iota(jnp.int32, (256, 128), 1) < S, ends, 0.0
                )
    ones = jnp.ones((8, 512), BF16)
    dot1 = lambda x: lax.dot_general(ones, x, NT, preferred_element_type=F32)
    row = lax.broadcasted_iota(jnp.int32, (8, 128), 0)
    packed = jnp.zeros((8, 128), F32)
    for j in range(5):
        pair = [ORDER[2 * j], ORDER[2 * j + 1]] if j < 4 else [0]
        values = [out_ref[level] for level in pair]
        values = jnp.concatenate(values if j < 4 else values + [jnp.zeros_like(values[0])], axis=0)
        high, low = split(values * values)
        packed = jnp.where(row == j, dot1(high) + dot1(low), packed)
    mysum[...] = packed[0:5]
    sumbuf[lon] = packed[0:5]
    columns = 512 * count

    def tell(d, carry):
        copy = remote(mysum, sumbuf.at[lon], sum_send.at[d], sum_recv.at[lon], {"lon": lax.rem(lon + d, count)})
        copy.start()
        return carry

    def told(d, carry):
        source = lax.rem(lon + count - d, count)
        copy = remote(mysum, sumbuf.at[source], sum_send.at[d], sum_recv.at[source], {"lon": source})
        copy.wait_recv()
        copy.wait_send()
        return carry

    lax.fori_loop(1, count, tell, 0)
    lax.fori_loop(1, count, told, 0)
    total = jnp.sum(sumbuf[...], axis=0) * (1.0 / columns)
    for j in range(9):
        level = (ORDER + (0,))[j]
        var_ref[level : level + 1, :] = total[j // 2 : j // 2 + 1, S * (j % 2) : S * (j % 2) + S]
    for copy in pending:
        copy.wait_send()


def put_out(field_ref, sums_ref, out_ref, var_ref, sem):
    copies = [
        pltpu.make_async_copy(field_ref, out_ref, sem.at[0]),
        pltpu.make_async_copy(sums_ref, var_ref, sem.at[1]),
    ]
    for copy in copies:
        copy.start()
    for copy in copies:
        copy.wait()


def vmem(count):
    return [pl.BlockSpec(memory_space=pltpu.VMEM)] * count


def local(previous, loss_matrix, pair_matrix, diffusivity, mixing):
    count = lax.axis_size("lon")
    low = lambda *shape: [pltpu.VMEM(shape, BF16)] * 2
    full = lambda *shape: [pltpu.VMEM(shape, F32)]
    sems = lambda *shape: [pltpu.SemaphoreType.DMA(shape)] * 2
    scratch = [pltpu.SMEM((9,), F32)] * 2 + full(9, S, S) * 2 + full(9, S, 512) + [pltpu.SemaphoreType.DMA((5,))] + low(512, 512) + low(512, 128) + low(128, 512) + full(96, 128) + low(2, 256, 256) + low(S, S)
    scratch += full(512, 640) + full(8, 640) + full(512, 512)
    scratch += full(8, 96, 128) + low(256, 256) + low(512, 256) + low(256, 256) * 2
    scratch += full(256, S) * 2 + full(S, 256) * 2 + full(256, 256)
    scratch += full(2, 528, 640) + low(512, 512) + full(2, 2, 256, 128) * 2 + full(2, 2, 128, 128) + full(2, 3, 128, 128)
    scratch += full(2, 2, 256, 128) * 2 + full(2, 2, 8, 640) + full(512, 640) + full(5, 128) + full(count, 5, 128)
    scratch += sems(7) + sems(2, 2) + sems(2, 2) + sems(2, 3) + sems(count)
    shapes = [jax.ShapeDtypeStruct((9, S, 512), F32), jax.ShapeDtypeStruct((9, S), F32)]
    anywhere = [pl.BlockSpec(memory_space=pl.ANY)] * 2
    done = pl.pallas_call(
        functools.partial(kernel, count),
        out_shape=shapes,
        in_specs=[pl.BlockSpec(memory_space=pltpu.HBM)] * 5,
        out_specs=tuple(vmem(2)),
        scratch_shapes=scratch,
        compiler_params=pltpu.CompilerParams(vmem_limit_bytes=32 * 2**20, collective_id=0, has_side_effects=True),
    )(*[pltpu.with_memory_space_constraint(x, pltpu.HBM) for x in (diffusivity, mixing, loss_matrix, pair_matrix, previous)])
    return tuple(pl.pallas_call(
        put_out,
        out_shape=shapes,
        in_specs=vmem(2),
        out_specs=tuple(anywhere),
        scratch_shapes=[pltpu.SemaphoreType.DMA((2,))],
        compiler_params=pltpu.CompilerParams(vmem_limit_bytes=8 * 2**20),
    )(*done))


def solution(mesh):
    placed = (P("lev", None, "lon"), P("lev", None, None), P("lev", None, None), P("lev"), P("lev"))
    return jax.shard_map(
        local,
        mesh=mesh,
        in_specs=placed,
        out_specs=(P("lev", None, "lon"), P("lev", None)),
        check_vma=False,
    )
```

```python
import functools

import jax
import jax.numpy as jnp
from jax import lax
from jax.experimental import pallas as pl
from jax.experimental.pallas import tpu as pltpu
from jax.sharding import PartitionSpec as P

ITERS = 2
F32 = jnp.float32
BF16 = jnp.bfloat16
MESH = pl.DeviceIdType.MESH
HIGHEST = lax.Precision.HIGHEST

S = 64
ORDER = (1, 2, 4, 5, 7, 8, 3, 6)
NN = (((1,), (0,)), ((), ()))
NT = (((1,), (1,)), ((), ()))
TN = (((0,), (0,)), ((), ()))


def split(x):
    high = x.astype(BF16)
    return high, (x - high.astype(F32)).astype(BF16)


def dot3(a, b, dims=NN):
    one = lambda x, y: lax.dot_general(x, y, dims, preferred_element_type=F32)
    return one(a[0], b[0]) + (one(a[0], b[1]) + one(a[1], b[0]))


def mm(a, b, dims=NN):
    return dot3(split(a), split(b), dims)


def mm_full(a, b, dims=NN):
    return lax.dot_general(a, b, dims, precision=HIGHEST, preferred_element_type=F32)


def eye(n):
    rows = lax.broadcasted_iota(jnp.int32, (n, n), 0)
    return (rows == lax.broadcasted_iota(jnp.int32, (n, n), 1)).astype(F32)


def spd_inverses(blocks, lows, high, doublings):
    centres = [0.5 * (high + low) for low in lows]
    units = [eye(block.shape[0]) for block in blocks]
    inverses = [unit * (1.0 / centre) for unit, centre in zip(units, centres)]
    residuals = [unit - block * (1.0 / centre) for unit, block, centre in zip(units, blocks, centres)]
    terms = [(high + low) / (high - low) for low in lows]
    for step in range(doublings):
        last = step == doublings - 1
        for i, unit in enumerate(units):
            twice = 2.0 * terms[i] * terms[i] - 1.0
            gain, shift = (twice + 1.0) / twice, 1.0 / twice
            terms[i] = twice
            centre = centres[i]
            n = unit.shape[0]
            rest = split(residuals[i])
            if step == 0:
                inverses[i] = (inverses[i] + residuals[i] * (1.0 / centre)) * gain
                if not last:
                    residuals[i] = gain * dot3(rest, rest) - shift * unit
                continue
            known = split(inverses[i])
            if last:
                inverses[i] = gain * (inverses[i] + dot3(known, rest))
                continue
            both = dot3(tuple(jnp.concatenate(p, axis=0) for p in zip(known, rest)), rest)
            inverses[i] = gain * (inverses[i] + both[:n])
            residuals[i] = gain * both[n:] - shift * unit
    exact = [unit - mm_full(block, inverse) for unit, block, inverse in zip(units, blocks, inverses)]
    step = lambda x, y: lax.dot_general(x.astype(BF16), y.astype(BF16), NN, preferred_element_type=F32)
    return [inverse + step(inverse, rest) for inverse, rest in zip(inverses, exact)]


def wide(grid):
    return jnp.concatenate([jnp.concatenate(row, axis=1) if len(row) > 1 else row[0] for row in grid], axis=0)


def interior(link_ref, loss_ref, row_ref, pack_ref, fill):
    one = eye(S)
    zero = jnp.zeros((S, S), F32)
    links = [link_ref[i] for i in range(9)]
    shunt = [loss_ref[i] + one for i in range(9)]
    blocks = []
    for top in (1, 4, 7):
        diag = [shunt[level] + (links[level - 1] + links[level]) * one for level in (top, top + 1)]
        tie = -links[top] * one
        blocks.append(wide([[diag[0], tie], [tie, diag[1]]]))
    pairs = spd_inverses(blocks, [199.0] * 3, 6700.0, 5)
    none = jnp.zeros((S, 128), F32)
    spread = wide([
        [links[2] * pairs[0][S:], links[3] * pairs[1][:S], none],
        [none, links[5] * pairs[1][S:], links[6] * pairs[2][:S]],
    ])
    ground = jnp.concatenate(
        [shunt[1] + links[0] * one, shunt[2], shunt[4], shunt[5], shunt[7], shunt[8] + links[8] * one], axis=0
    )
    own = jnp.concatenate([shunt[3], shunt[6]], axis=0) + mm_full(spread, ground)
    down = links[5] * spread[0:S, 192:256]
    up = links[3] * spread[S:, 128:192]
    fill()
    middle, = spd_inverses([wide([[own[:S] + down, -down], [-up, own[S:] + up]])], [68.6], 3010.0, 5)
    spread = jnp.concatenate([spread, eye(128)], axis=1)
    lifted = mm(middle, spread)
    lane = lax.broadcasted_iota(jnp.int32, (128, 128), 1)
    ends = mm(jnp.where(lane < S, spread[:, 0:128], spread[:, 256:384]), lifted, TN)
    first = jnp.concatenate([ends[0:S, 0:128] + pairs[0][:S], ends[0:S, 128:512]], axis=1)
    last = jnp.concatenate([ends[S:, 0:256], ends[S:, 256:384] + pairs[2][S:], ends[S:, 384:512]], axis=1)
    rows = jnp.concatenate([links[0] * first, links[8] * last], axis=0)
    row_ref[...] = rows
    loads = mm_full(rows, jnp.concatenate([shunt[level] for level in ORDER], axis=0))
    across = links[8] * rows[0:S, 320:384]
    pack_ref[0:64, :] = jnp.concatenate([shunt[0] + loads[0:S], loads[S:]], axis=1)
    pack_ref[64:96, :] = jnp.concatenate([across[0:32], across[32:64]], axis=1)
    return pairs, spread, lifted


def finish_interior(pairs, spread, lifted, full):
    full[...] = mm(spread, lifted, TN)
    for i in range(3):
        at = slice(128 * i, 128 * i + 128)
        full[at, at] += pairs[i]


def pair_weights(pair_ref, pw_hi, pw_lo, pn_hi, pn_lo):
    for half in range(2):
        row = lax.broadcasted_iota(jnp.int32, (256, 256), 0) // S
        column = lax.broadcasted_iota(jnp.int32, (256, 256), 1) // S
        tall = jnp.concatenate([pair_ref[level] for level in ORDER[4 * half : 4 * half + 4]], axis=0)
        tall = jnp.concatenate([tall, tall], axis=1)
        tall = jnp.where(row == column, jnp.concatenate([tall, tall], axis=1), 0.0)
        pw_hi[half], pw_lo[half] = split(tall)
    pn_hi[...], pn_lo[...] = split(pair_ref[0])


def field_of(prev_ref, field_ref):
    for j in range(4):
        both = jnp.concatenate([prev_ref[ORDER[2 * j]], prev_ref[ORDER[2 * j + 1]]], axis=0)
        field_ref[:, 128 * j : 128 * j + 128] = both.T
    last = jnp.concatenate([prev_ref[0], jnp.zeros_like(prev_ref[0])], axis=0)
    field_ref[:, 512:640] = last.T


def mix_row_of(mix_ref, mixrow_ref):
    lane = lax.broadcasted_iota(jnp.int32, (8, 640), 1) // S
    row = jnp.zeros((8, 640), F32)
    for j, level in enumerate(ORDER + (0,)):
        row = jnp.where(lane == j, mix_ref[level], row)
    mixrow_ref[...] = row


def unpack(packs, q):
    both, folded = packs(q)
    across = jnp.concatenate([folded[:, 0:S], folded[:, S:]], axis=0)
    return both[:, 0:S], both[:, S:], across


def interface(pack_ref, own_hi, own_lo, msg_hi, msg_lo, rlo_hi, rlo_lo, rhi_hi, rhi_lo, full, wp, wc, rs, rc, own):
    chip = lax.axis_index("lev") // 2
    one = eye(S)
    zero = jnp.zeros((S, S), F32)
    here, below, across = zip(*[
        unpack(lambda q: (pack_ref[q, 0:64, :], pack_ref[q, 64:96, :]), q) for q in range(8)
    ])
    back = [a.T for a in across]
    ground = [here[q] + (below[q - 1] if q else 0.0) for q in range(8)]
    diag = [ground[q] + across[q] + (back[q - 1] if q else 0.0) for q in range(8)]
    upper = wide([
        [diag[0], -across[0], zero, zero],
        [-back[0], diag[1], -across[1], zero],
        [zero, -back[1], diag[2], -across[2]],
        [zero, zero, -back[2], diag[3]],
    ])
    lower = wide([
        [diag[5], -across[5], zero],
        [-back[5], diag[6], -across[6]],
        [zero, -back[6], diag[7]],
    ])
    first = chip < 2
    small = jnp.where(
        first, upper[0:128, 0:128], wide([[500.0 * one, zero], [zero, diag[7]]])
    )
    upper_inverse, lower_inverse, small_inverse = spd_inverses(
        [upper, lower, small], [9.6, 21.0, 13.9], 2400.0, 6
    )
    upper_t = mm(back[3], upper_inverse[192:256, :])
    lower_t = mm(across[4], lower_inverse[0:64, :])
    middle = (
        ground[4]
        + mm_full(upper_t, jnp.concatenate(ground[0:4], axis=0))
        + mm_full(lower_t, jnp.concatenate([ground[5], ground[6], ground[7] + across[7]], axis=0))
    )
    middle_inverse, = spd_inverses([middle], [28.7], 2400.0, 5)
    spread = jnp.concatenate([upper_t, lower_t, one], axis=1)
    lifted = mm(middle_inverse, spread)
    full[...] = mm(spread, lifted, TN)
    full[0:256, 0:256] += upper_inverse
    full[256:448, 256:448] += lower_inverse
    place = {0: 0, 1: 1, 2: 2, 3: 3, 4: 7, 5: 4, 6: 5, 7: 6}
    link = jnp.where(first, back[1], across[6])
    away = mm(link, small_inverse[64:128, :])

    def block(r, c):
        if r > 7 or c > 7:
            return zero
        r, c = place[r], place[c]
        return full[S * r : S * r + S, S * c : S * c + S]

    def blocks(rows, columns):
        return wide([[block(r, c) for c in columns] for r in rows])

    for c in range(4):
        nodes = (2 * c, 2 * c + 1, 2 * c + 1, 2 * c + 2)

        @pl.when(chip == c)
        def _(c=c, nodes=nodes):
            own[...] = blocks(nodes, nodes)
            wc[...] = blocks(nodes, (4,))
            if c in (0, 3):
                far = [away[:, 0:64], away[:, 64:128]]
                if c == 0:
                    rs[...] = jnp.concatenate([far[0], far[1], far[1], one], axis=1)
                    wp[...] = jnp.concatenate([far[0].T, far[1].T, far[1].T, one], axis=0)
                else:
                    rs[...] = jnp.concatenate([one, far[1], far[1], zero], axis=1)
                    wp[...] = jnp.concatenate([one, far[1].T, far[1].T, zero], axis=0)
            else:
                gate = 2 if c == 1 else 6
                rs[...] = blocks((gate,), nodes)
                wp[...] = blocks(nodes, (gate,))

            def seen(n):
                if n > 7:
                    return zero
                n = place[n]
                return spread[:, S * n : S * n + S]

            rc[...] = jnp.concatenate([seen(n) for n in nodes], axis=1)

    own_hi[...], own_lo[...] = split(own[...])
    none = jnp.zeros((256, S), F32)
    msg = wide([[wp[...], none, wc[...], none], [none, wp[...], none, wc[...]]])
    msg_hi[...], msg_lo[...] = split(msg)
    none = jnp.zeros((S, 256), F32)
    rlo_hi[...], rlo_lo[...] = split(jnp.concatenate([rs[...], none, rc[...], none], axis=0))
    rhi_hi[...], rhi_lo[...] = split(jnp.concatenate([none, rs[...], none, rc[...]], axis=0))


def kernel(count, link_hbm, mix_hbm, loss_hbm, pair_hbm, prev_hbm, out_any, var_ref,
           link_ref, mix_ref, loss_ref, pair_ref, prev_ref, load_sem,
           full, row, g_hi, g_lo, hr_hi, hr_lo, hc_hi, hc_lo, pack, pw_hi, pw_lo, pn_hi, pn_lo, field, mixrow,
           packs, inverse, own_hi, own_lo, msg_hi, msg_lo, rlo_hi, rlo_lo, rhi_hi, rhi_lo, wp, wc, rs, rc, own,
           state, gs_hi, gs_lo, injs, outgo, incoming, sums, outs, part, part_in, mysum, sumbuf,
           pack_send, pack_recv, give_send, give_recv, halo_send, halo_recv, msg_send, msg_recv, out_send, out_recv,
           sum_send, sum_recv):
    lev = lax.axis_index("lev")
    lon = lax.axis_index("lon")
    core = lax.rem(lev, 2)
    chip = lev // 2
    partner = lev + 1 - 2 * core
    base = lev - core
    sibling = 2 * (chip + 1 - 2 * lax.rem(chip, 2)) + core
    across_base = 2 - 2 * (chip // 2)
    far = lax.rem(chip + 2, 4)
    across = [2 * far + core, 2 * (2 * across_base + 1 - far) + core]
    west, east = lax.rem(lon + count - 1, count), lax.rem(lon + 1, count)
    loads = [
        pltpu.make_async_copy(src, dst, load_sem.at[i])
        for i, (src, dst) in enumerate([
            (link_hbm, link_ref), (loss_hbm, loss_ref), (prev_hbm, prev_ref), (pair_hbm, pair_ref.at[core]), (mix_hbm, mix_ref),
        ])
    ]
    for load in loads:
        load.start()
    barrier = pltpu.get_barrier_semaphore()
    others = [lax.rem(lev + d, 8) for d in range(1, 8)]
    for other in others:
        pl.semaphore_signal(barrier, inc=1, device_id={"lev": other}, device_id_type=MESH)
    for side in (west, east):
        pl.semaphore_signal(barrier, inc=1, device_id={"lev": partner, "lon": side}, device_id_type=MESH)

    def greet(d, carry):
        pl.semaphore_signal(barrier, inc=1, device_id={"lon": lax.rem(lon + d, count)}, device_id_type=MESH)
        return carry

    lax.fori_loop(1, count, greet, 0)

    def remote(src, dst, send, recv, where):
        return pltpu.make_async_remote_copy(
            src_ref=src, dst_ref=dst, send_sem=send, recv_sem=recv, device_id=where, device_id_type=MESH
        )

    def rows_at(start, size):
        return pl.ds(pl.multiple_of(start, 8), size)

    pending = []

    def start(copy):
        copy.start()
        pending.append(copy)
        return copy

    def fill():
        loads[2].wait()
        field_of(prev_ref, field)

    loads[0].wait()
    loads[1].wait()
    parts = interior(link_ref, loss_ref, row.at[core], pack, fill)
    loads[3].wait()
    loads[4].wait()
    mix_row_of(mix_ref, mixrow.at[core])
    pl.semaphore_wait(barrier, 8 + count)
    spread = []
    for d, other in enumerate(others):
        copy = remote(pack, packs.at[lev], pack_send.at[d], pack_recv.at[d], {"lev": other})
        copy.start()
        spread.append(copy)
    packs[lev] = pack[...]
    away = 1 - core
    gives = [
        start(remote(src, dst, give_send.at[i], give_recv.at[i], {"lev": partner}))
        for i, (src, dst) in enumerate([
            (field.at[rows_at(248 * away, 264)], state.at[0, core, rows_at(8 * core, 264)]),
            (pair_ref.at[core], pair_ref.at[core]),
            (mixrow.at[core], mixrow.at[core]),
            (row.at[core], row.at[core]),
        ])
    ]
    outer = [
        start(remote(field.at[0:8], state.at[0, core, 264:272], halo_send.at[0, 0], halo_recv.at[0, core],
                     {"lev": base + 1, "lon": west})),
        start(remote(field.at[504:512], state.at[0, core, 0:8], halo_send.at[0, 1], halo_recv.at[0, core],
                     {"lev": base, "lon": east})),
    ]
    state[0, core, rows_at(8 * away, 264), :] = field[rows_at(248 * core, 264), :]
    finish_interior(*parts, full.at[core])
    give_full = start(remote(full.at[core], full.at[core], give_send.at[4], give_recv.at[4], {"lev": partner}))

    def pair_term(it, s):
        for r in range(0, 256, 128):
            here = state[it, s, 8 + r : 136 + r, :]
            squares = split(here * here)
            for half in range(2):
                piece = tuple(x[:, 256 * half : 256 * half + 256] for x in squares)
                sums[s, r : r + 128, 256 * half : 256 * half + 256] = dot3(piece, (pw_hi[s, half], pw_lo[s, half]), NT)
            piece = tuple(x[:, 512:576] for x in squares)
            sums[s, r : r + 128, 512:576] = dot3(piece, (pn_hi[s], pn_lo[s]), NT)

    def forcing_term(it, s):
        for r in range(0, 256, 128):
            here = state[it, s, 8 + r : 136 + r, 0:576]
            around = state[it, s, 7 + r : 135 + r, 0:576] + state[it, s, 9 + r : 137 + r, 0:576]
            forcing = state[0, s, 8 + r : 136 + r, 0:576] - sums[s, r : r + 128, 0:576]
            forcing += mixrow[s, 0:1, 0:576] * (around - 2.0 * here)
            pieces = split(forcing[:, 0:512])
            gs_hi[s, r : r + 128, :], gs_lo[s, r : r + 128, :] = pieces
            node = forcing[:, 512:576]
            push = dot3(pieces, (hr_hi[s], hr_lo[s]), NT)
            injs[s, r : r + 128, :] = push + jnp.concatenate([node, jnp.zeros_like(node)], axis=1)

    def weights(s):
        pair_weights(pair_ref.at[s], pw_hi.at[s], pw_lo.at[s], pn_hi.at[s], pn_lo.at[s])
        hr_hi[s], hr_lo[s] = split(row[s])

    def product(it, s):
        if it == ITERS - 1:
            for b in range(4):
                rows = slice(128 * b, 128 * b + 128)
                value = dot3((g_hi[s, rows, :], g_lo[s, rows, :]), (gs_hi[s], gs_lo[s]), NT)
                for h in range(2):
                    outs[s, ORDER[2 * b + h]] = value[64 * h : 64 * h + 64]
        else:
            for r in range(0, 256, 128):
                pieces = (gs_hi[s, r : r + 128, :], gs_lo[s, r : r + 128, :])
                state[it + 1, s, 8 + r : 136 + r, 0:512] = dot3(pieces, (g_hi[s], g_lo[s]))

    weights(core)
    pair_term(0, core)
    for slot in range(2):
        pltpu.make_async_copy(field.at[0:8], state.at[0, 0, 0:8], halo_recv.at[0, slot]).wait()
    forcing_term(0, core)
    for give in gives:
        give.wait_recv()
    weights(away)
    pair_term(0, away)
    forcing_term(0, away)
    for copy in spread:
        copy.wait()
    interface(packs, own_hi, own_lo, msg_hi, msg_lo, rlo_hi, rlo_lo, rhi_hi, rhi_lo, inverse, wp, wc, rs, rc, own)
    for it in range(ITERS):
        final = it == ITERS - 1
        if it:
            inner_from, inner_to = 8 + 248 * away, 264 * core
            outer_from, outer_to = 8 + 248 * core, 264 * away
            halos = [
                start(remote(state.at[it, :, rows_at(a, 8), :], state.at[it, :, rows_at(b, 8), :],
                             halo_send.at[it, i], halo_recv.at[it, i], where))
                for i, (a, b, where) in enumerate([
                    (outer_from, outer_to, {"lev": partner, "lon": west + (east - west) * core}),
                    (inner_from, inner_to, {"lev": partner}),
                ])
            ]
            for s in range(2):
                pair_term(it, s)
            for halo in halos:
                halo.wait_recv()
            for s in range(2):
                forcing_term(it, s)
        inj = jnp.concatenate([injs[0], injs[1]], axis=1)
        packed = split(jnp.concatenate([inj[0:128], inj[128:256]], axis=1))
        message = dot3(packed, (msg_hi[...], msg_lo[...]))
        outgo[it, 0] = message[:, 0:128]
        outgo[it, 1] = message[:, 128:256]
        slot = 1 + lax.rem(chip, 2)
        start(remote(outgo.at[it, 1], incoming.at[it, slot], msg_send.at[it, 1], msg_recv.at[it, slot], {"lev": across[0]}))
        start(remote(outgo.at[it, 1], incoming.at[it, slot], msg_send.at[it, 2], msg_recv.at[it, slot], {"lev": across[1]}))
        start(remote(outgo.at[it, 0], incoming.at[it, 0], msg_send.at[it, 0], msg_recv.at[it, 0], {"lev": sibling}))
        mine = dot3(split(inj), (own_hi[...], own_lo[...]))
        if it == 0:
            give_full.wait_recv()
            for s in range(2):
                g_hi[s], g_lo[s] = split(full[s])
                hc_hi[s], hc_lo[s] = split(row[s].T)
        for s in range(2):
            product(it, s)
        for slot in range(3):
            pltpu.make_async_copy(outgo.at[it, 0], incoming.at[it, slot], msg_recv.at[it, slot]).wait()
        heard = split(jnp.concatenate([incoming[it, 0], incoming[it, 1] + incoming[it, 2]], axis=1))
        total = mine + jnp.concatenate(
            [dot3(heard, (rlo_hi[...], rlo_lo[...])), dot3(heard, (rhi_hi[...], rhi_lo[...]))], axis=0
        )
        for s in range(2):
            ends = total[:, 128 * s : 128 * s + 128]
            pieces = split(ends)
            if final:
                for b in range(4):
                    rows = slice(128 * b, 128 * b + 128)
                    value = dot3((hc_hi[s, rows, :], hc_lo[s, rows, :]), pieces, NT)
                    for h in range(2):
                        outs[s, ORDER[2 * b + h]] += value[64 * h : 64 * h + 64]
                outs[s, 0] = ends.T[0:64]
            else:
                state[it + 1, s, 8:264, 0:512] += dot3(pieces, (hr_hi[s], hr_lo[s]))
                state[it + 1, s, 8:264, 512:640] = jnp.where(
                    lax.broadcasted_iota(jnp.int32, (256, 128), 1) < S, ends, 0.0
                )
    ones = jnp.ones((8, 256), BF16)
    dot1 = lambda x: lax.dot_general(ones, x, NT, preferred_element_type=F32)
    line = lax.broadcasted_iota(jnp.int32, (8, 128), 0)
    for s in range(2):
        packed = jnp.zeros((8, 128), F32)
        for j in range(5):
            values = [outs[s, level] for level in ((ORDER + (0,))[2 * j : 2 * j + 2])]
            values = jnp.concatenate(values if j < 4 else values + [jnp.zeros_like(values[0])], axis=0)
            high, low = split(values * values)
            packed = jnp.where(line == j, dot1(high) + dot1(low), packed)
        part[s] = packed[0:5]
    give = start(remote(part.at[away], part_in, out_send.at[0], out_recv.at[0], {"lev": partner}))
    keep = pltpu.make_async_copy(outs.at[core], out_any.at[core], load_sem.at[0])
    keep.start()
    back = start(remote(outs.at[away], out_any.at[core], out_send.at[1], out_recv.at[1], {"lev": partner}))
    give.wait_recv()
    mine = part[core] + part_in[...]
    mysum[...] = mine
    sumbuf[lon] = mine

    def tell(d, carry):
        copy = remote(mysum, sumbuf.at[lon], sum_send.at[d], sum_recv.at[lon], {"lon": lax.rem(lon + d, count)})
        copy.start()
        return carry

    def told(d, carry):
        source = lax.rem(lon + count - d, count)
        copy = remote(mysum, sumbuf.at[source], sum_send.at[d], sum_recv.at[source], {"lon": source})
        copy.wait_recv()
        copy.wait_send()
        return carry

    lax.fori_loop(1, count, tell, 0)
    lax.fori_loop(1, count, told, 0)
    total = jnp.sum(sumbuf[...], axis=0) * (1.0 / (512 * count))
    for j in range(9):
        level = (ORDER + (0,))[j]
        var_ref[level : level + 1, :] = total[j // 2 : j // 2 + 1, S * (j % 2) : S * (j % 2) + S]
    keep.wait()
    back.wait_recv()
    for copy in pending:
        copy.wait_send()


def put_out(field_ref, sums_ref, out_ref, var_ref, sem):
    copies = [
        pltpu.make_async_copy(field_ref.at[half], out_ref.at[:, :, pl.ds(256 * half, 256)], sem.at[half])
        for half in range(2)
    ]
    copies.append(pltpu.make_async_copy(sums_ref, var_ref, sem.at[2]))
    for copy in copies:
        copy.start()
    for copy in copies:
        copy.wait()


def vmem(count):
    return [pl.BlockSpec(memory_space=pltpu.VMEM)] * count


def local(previous, loss_matrix, pair_matrix, diffusivity, mixing):
    count = lax.axis_size("lon")
    low = lambda *shape: [pltpu.VMEM(shape, BF16)] * 2
    full = lambda *shape: [pltpu.VMEM(shape, F32)]
    sems = lambda *shape: [pltpu.SemaphoreType.DMA(shape)] * 2
    scratch = [pltpu.SMEM((9,), F32)] * 2 + full(9, S, S) + full(2, 9, S, S) + full(9, S, 512) + [pltpu.SemaphoreType.DMA((5,))]
    scratch += full(2, 512, 512) + full(2, 128, 512) + low(2, 512, 512) + low(2, 128, 512) + low(2, 512, 128) + full(96, 128)
    scratch += low(2, 2, 256, 256) + low(2, S, S) + full(512, 640) + full(2, 8, 640)
    scratch += full(8, 96, 128) + full(512, 512) + low(256, 256) + low(512, 256) + low(256, 256) * 2
    scratch += full(256, S) * 2 + full(S, 256) * 2 + full(256, 256)
    scratch += full(2, 2, 272, 640) + low(2, 256, 512) + full(2, 256, 128) + full(2, 2, 128, 128) + full(2, 3, 128, 128)
    scratch += full(2, 256, 640) + full(2, 9, S, 256) + full(2, 5, 128) + full(5, 128) * 2 + full(count, 5, 128)
    scratch += sems(7) + sems(5) + sems(2, 2) + sems(2, 3) + sems(2) + sems(count)
    shapes = [jax.ShapeDtypeStruct((9, S, 512), F32), jax.ShapeDtypeStruct((9, S), F32)]
    halves = jax.ShapeDtypeStruct((2, 9, S, 256), F32)
    anywhere = [pl.BlockSpec(memory_space=pl.ANY)] * 2
    done = pl.pallas_call(
        functools.partial(kernel, count),
        out_shape=[halves, shapes[1]],
        in_specs=[pl.BlockSpec(memory_space=pltpu.HBM)] * 5,
        out_specs=(anywhere[0], vmem(1)[0]),
        scratch_shapes=scratch,
        compiler_params=pltpu.CompilerParams(vmem_limit_bytes=32 * 2**20, collective_id=0, has_side_effects=True),
    )(*[pltpu.with_memory_space_constraint(x, pltpu.HBM) for x in (diffusivity, mixing, loss_matrix, pair_matrix, previous)])
    return tuple(pl.pallas_call(
        put_out,
        out_shape=shapes,
        in_specs=vmem(2),
        out_specs=tuple(anywhere),
        scratch_shapes=[pltpu.SemaphoreType.DMA((3,))],
        compiler_params=pltpu.CompilerParams(vmem_limit_bytes=8 * 2**20),
    )(*done))


def solution(mesh):
    placed = (P("lev", None, "lon"), P("lev", None, None), P("lev", None, None), P("lev"), P("lev"))
    return jax.shard_map(
        local,
        mesh=mesh,
        in_specs=placed,
        out_specs=(P("lev", None, "lon"), P("lev", None)),
        check_vma=False,
    )
```

```python
import functools

import jax
import jax.numpy as jnp
from jax import lax
from jax.experimental import pallas as pl
from jax.experimental.pallas import tpu as pltpu
from jax.sharding import PartitionSpec as P

ITERS = 2
F32 = jnp.float32
BF16 = jnp.bfloat16
MESH = pl.DeviceIdType.MESH
HIGHEST = lax.Precision.HIGHEST

S = 64
ORDER = (1, 2, 4, 5, 7, 8, 3, 6)
NN = (((1,), (0,)), ((), ()))
NT = (((1,), (1,)), ((), ()))
TN = (((0,), (0,)), ((), ()))


def split(x):
    high = x.astype(BF16)
    return high, (x - high.astype(F32)).astype(BF16)


def dot3(a, b, dims=NN):
    one = lambda x, y: lax.dot_general(x, y, dims, preferred_element_type=F32)
    return one(a[0], b[0]) + (one(a[0], b[1]) + one(a[1], b[0]))


def mm(a, b, dims=NN):
    return dot3(split(a), split(b), dims)


def mm_full(a, b, dims=NN):
    return lax.dot_general(a, b, dims, precision=HIGHEST, preferred_element_type=F32)


def eye(n):
    rows = lax.broadcasted_iota(jnp.int32, (n, n), 0)
    return (rows == lax.broadcasted_iota(jnp.int32, (n, n), 1)).astype(F32)


def spd_inverses(blocks, lows, high, doublings):
    centres = [0.5 * (high + low) for low in lows]
    units = [eye(block.shape[0]) for block in blocks]
    inverses = [unit * (1.0 / centre) for unit, centre in zip(units, centres)]
    residuals = [unit - block * (1.0 / centre) for unit, block, centre in zip(units, blocks, centres)]
    terms = [(high + low) / (high - low) for low in lows]
    for step in range(doublings):
        last = step == doublings - 1
        for i, unit in enumerate(units):
            twice = 2.0 * terms[i] * terms[i] - 1.0
            gain, shift = (twice + 1.0) / twice, 1.0 / twice
            terms[i] = twice
            centre = centres[i]
            n = unit.shape[0]
            rest = split(residuals[i])
            if step == 0:
                inverses[i] = (inverses[i] + residuals[i] * (1.0 / centre)) * gain
                if not last:
                    residuals[i] = gain * dot3(rest, rest) - shift * unit
                continue
            known = split(inverses[i])
            if last:
                inverses[i] = gain * (inverses[i] + dot3(known, rest))
                continue
            both = dot3(tuple(jnp.concatenate(p, axis=0) for p in zip(known, rest)), rest)
            inverses[i] = gain * (inverses[i] + both[:n])
            residuals[i] = gain * both[n:] - shift * unit
    exact = [unit - mm_full(block, inverse) for unit, block, inverse in zip(units, blocks, inverses)]
    step = lambda x, y: lax.dot_general(x.astype(BF16), y.astype(BF16), NN, preferred_element_type=F32)
    return [inverse + step(inverse, rest) for inverse, rest in zip(inverses, exact)]


def wide(grid):
    return jnp.concatenate([jnp.concatenate(row, axis=1) if len(row) > 1 else row[0] for row in grid], axis=0)


def interior(link_ref, loss_ref, row_ref, pack_ref):
    one = eye(S)
    zero = jnp.zeros((S, S), F32)
    links = [link_ref[i] for i in range(9)]
    shunt = [loss_ref[i] + one for i in range(9)]
    blocks = []
    for top in (1, 4, 7):
        diag = [shunt[level] + (links[level - 1] + links[level]) * one for level in (top, top + 1)]
        tie = -links[top] * one
        blocks.append(wide([[diag[0], tie], [tie, diag[1]]]))
    pairs = spd_inverses(blocks, [199.0] * 3, 6700.0, 5)
    none = jnp.zeros((S, 128), F32)
    spread = wide([
        [links[2] * pairs[0][S:], links[3] * pairs[1][:S], none],
        [none, links[5] * pairs[1][S:], links[6] * pairs[2][:S]],
    ])
    ground = jnp.concatenate(
        [shunt[1] + links[0] * one, shunt[2], shunt[4], shunt[5], shunt[7], shunt[8] + links[8] * one], axis=0
    )
    own = jnp.concatenate([shunt[3], shunt[6]], axis=0) + mm_full(spread, ground)
    down = links[5] * spread[0:S, 192:256]
    up = links[3] * spread[S:, 128:192]
    middle, = spd_inverses([wide([[own[:S] + down, -down], [-up, own[S:] + up]])], [68.6], 3010.0, 5)
    spread = jnp.concatenate([spread, eye(128)], axis=1)
    lifted = mm(middle, spread)
    lane = lax.broadcasted_iota(jnp.int32, (128, 128), 1)
    ends = mm(jnp.where(lane < S, spread[:, 0:128], spread[:, 256:384]), lifted, TN)
    first = jnp.concatenate([ends[0:S, 0:128] + pairs[0][:S], ends[0:S, 128:512]], axis=1)
    last = jnp.concatenate([ends[S:, 0:256], ends[S:, 256:384] + pairs[2][S:], ends[S:, 384:512]], axis=1)
    rows = jnp.concatenate([links[0] * first, links[8] * last], axis=0)
    row_ref[...] = rows
    loads = mm_full(rows, jnp.concatenate([shunt[level] for level in ORDER], axis=0))
    across = links[8] * rows[0:S, 320:384]
    pack_ref[0:64, :] = jnp.concatenate([shunt[0] + loads[0:S], loads[S:]], axis=1)
    pack_ref[64:96, :] = jnp.concatenate([across[0:32], across[32:64]], axis=1)
    return pairs, spread, lifted


def finish_interior(pairs, spread, lifted, full):
    full[...] = mm(spread, lifted, TN)
    for i in range(3):
        at = slice(128 * i, 128 * i + 128)
        full[at, at] += pairs[i]


def pair_weights(pair_ref, pw_hi, pw_lo, pn_hi, pn_lo):
    for half in range(2):
        row = lax.broadcasted_iota(jnp.int32, (256, 256), 0) // S
        column = lax.broadcasted_iota(jnp.int32, (256, 256), 1) // S
        tall = jnp.concatenate([pair_ref[level] for level in ORDER[4 * half : 4 * half + 4]], axis=0)
        tall = jnp.concatenate([tall, tall], axis=1)
        tall = jnp.where(row == column, jnp.concatenate([tall, tall], axis=1), 0.0)
        pw_hi[half], pw_lo[half] = split(tall)
    pn_hi[...], pn_lo[...] = split(pair_ref[0])


def field_of(prev_ref, field_ref):
    for j in range(4):
        both = jnp.concatenate([prev_ref[ORDER[2 * j]], prev_ref[ORDER[2 * j + 1]]], axis=0)
        field_ref[:, 128 * j : 128 * j + 128] = both.T
    last = jnp.concatenate([prev_ref[0], jnp.zeros_like(prev_ref[0])], axis=0)
    field_ref[:, 512:640] = last.T


def mix_row_of(mix_ref, mixrow_ref):
    lane = lax.broadcasted_iota(jnp.int32, (8, 640), 1) // S
    row = jnp.zeros((8, 640), F32)
    for j, level in enumerate(ORDER + (0,)):
        row = jnp.where(lane == j, mix_ref[level], row)
    mixrow_ref[...] = row


def unpack(packs, q):
    both, folded = packs(q)
    across = jnp.concatenate([folded[:, 0:S], folded[:, S:]], axis=0)
    return both[:, 0:S], both[:, S:], across


def interface(pack_ref, own_hi, own_lo, msg_hi, msg_lo, rlo_hi, rlo_lo, rhi_hi, rhi_lo, wp, wc, rs, rc, own):
    chip = lax.axis_index("lev") // 2
    one = eye(S)
    zero = jnp.zeros((S, S), F32)
    here, below, across = zip(*[
        unpack(lambda q: (pack_ref[q, 0:64, :], pack_ref[q, 64:96, :]), q) for q in range(8)
    ])
    back = [a.T for a in across]
    ground = [here[q] + (below[q - 1] if q else 0.0) for q in range(8)]
    diag = [ground[q] + across[q] + (back[q - 1] if q else 0.0) for q in range(8)]
    upper = wide([
        [diag[0], -across[0], zero, zero],
        [-back[0], diag[1], -across[1], zero],
        [zero, -back[1], diag[2], -across[2]],
        [zero, zero, -back[2], diag[3]],
    ])
    lower = wide([
        [diag[5], -across[5], zero],
        [-back[5], diag[6], -across[6]],
        [zero, -back[6], diag[7]],
    ])
    first = chip < 2
    small = jnp.where(
        first, upper[0:128, 0:128], wide([[500.0 * one, zero], [zero, diag[7]]])
    )
    upper_inverse, lower_inverse, small_inverse = spd_inverses(
        [upper, lower, small], [9.6, 21.0, 13.9], 2400.0, 6
    )
    upper_t = mm(back[3], upper_inverse[192:256, :])
    lower_t = mm(across[4], lower_inverse[0:64, :])
    middle = (
        ground[4]
        + mm_full(upper_t, jnp.concatenate(ground[0:4], axis=0))
        + mm_full(lower_t, jnp.concatenate([ground[5], ground[6], ground[7] + across[7]], axis=0))
    )
    middle_inverse, = spd_inverses([middle], [28.7], 2400.0, 5)
    spread = jnp.concatenate([upper_t, lower_t, one], axis=1)
    lifted = mm(middle_inverse, spread)
    place = {0: 0, 1: 1, 2: 2, 3: 3, 4: 7, 5: 4, 6: 5, 7: 6}
    link = jnp.where(first, back[1], across[6])
    away = mm(link, small_inverse[64:128, :])

    for c in range(4):
        nodes = (2 * c, 2 * c + 1, 2 * c + 1, 2 * c + 2)

        @pl.when(chip == c)
        def _(c=c, nodes=nodes):
            real = [n for n in range(2 * c, 2 * c + 3) if n < 8]
            against = real if 4 in real else real + [4]
            part = lambda x, n: x[:, S * place[n] : S * place[n] + S]
            both = [jnp.concatenate([part(x, n) for n in which], axis=1) for x, which in ((spread, real), (lifted, against))]
            product = mm(both[0], both[1], TN)

            def block(r, k):
                if r not in real or k not in against:
                    return zero
                i, j = real.index(r), against.index(k)
                value = product[S * i : S * i + S, S * j : S * j + S]
                i, j = place[r], place[k]
                if i < 4 and j < 4:
                    value += upper_inverse[S * i : S * i + S, S * j : S * j + S]
                elif 4 <= i < 7 and 4 <= j < 7:
                    value += lower_inverse[S * (i - 4) : S * (i - 3), S * (j - 4) : S * (j - 3)]
                return value

            def blocks(rows, columns):
                return wide([[block(r, k) for k in columns] for r in rows])

            own[...] = blocks(nodes, nodes)
            wc[...] = blocks(nodes, (4,))
            if c in (0, 3):
                far = [away[:, 0:64], away[:, 64:128]]
                if c == 0:
                    rs[...] = jnp.concatenate([far[0], far[1], far[1], one], axis=1)
                    wp[...] = jnp.concatenate([far[0].T, far[1].T, far[1].T, one], axis=0)
                else:
                    rs[...] = jnp.concatenate([one, far[1], far[1], zero], axis=1)
                    wp[...] = jnp.concatenate([one, far[1].T, far[1].T, zero], axis=0)
            else:
                gate = 2 if c == 1 else 6
                rs[...] = blocks((gate,), nodes)
                wp[...] = blocks(nodes, (gate,))

            def seen(n):
                if n > 7:
                    return zero
                n = place[n]
                return spread[:, S * n : S * n + S]

            rc[...] = jnp.concatenate([seen(n) for n in nodes], axis=1)

    own_hi[...], own_lo[...] = split(own[...])
    none = jnp.zeros((256, S), F32)
    msg = wide([[wp[...], none, wc[...], none], [none, wp[...], none, wc[...]]])
    msg_hi[...], msg_lo[...] = split(msg)
    none = jnp.zeros((S, 256), F32)
    rlo_hi[...], rlo_lo[...] = split(jnp.concatenate([rs[...], none, rc[...], none], axis=0))
    rhi_hi[...], rhi_lo[...] = split(jnp.concatenate([none, rs[...], none, rc[...]], axis=0))


def kernel(count, deep, link_hbm, mix_hbm, loss_hbm, pair_hbm, prev_hbm, out_any, sumbuf,
           link_ref, mix_ref, loss_ref, pair_ref, prev_ref, load_sem,
           full, row, g_hi, g_lo, hr_hi, hr_lo, hc_hi, hc_lo, pack, pw_hi, pw_lo, pn_hi, pn_lo, field, mixrow,
           packs, own_hi, own_lo, msg_hi, msg_lo, rlo_hi, rlo_lo, rhi_hi, rhi_lo, wp, wc, rs, rc, own,
           state, gs_hi, gs_lo, injs, outgo, incoming, sums, outs, ends_ref, part, part_in, mysum,
           pack_send, pack_recv, give_send, give_recv, halo_send, halo_recv, msg_send, msg_recv, out_send, out_recv,
           sum_send, sum_recv):
    lev = lax.axis_index("lev")
    lon = lax.axis_index("lon")
    core = lax.rem(lev, 2)
    chip = lev // 2
    partner = lev + 1 - 2 * core
    base = lev - core
    sibling = 2 * (chip + 1 - 2 * lax.rem(chip, 2)) + core
    across_base = 2 - 2 * (chip // 2)
    far = lax.rem(chip + 2, 4)
    across = [2 * far + core, 2 * (2 * across_base + 1 - far) + core]
    west, east = lax.rem(lon + count - 1, count), lax.rem(lon + 1, count)
    loads = [
        pltpu.make_async_copy(src, dst, load_sem.at[i])
        for i, (src, dst) in enumerate([
            (link_hbm, link_ref), (loss_hbm, loss_ref), (prev_hbm, prev_ref), (pair_hbm, pair_ref.at[core]), (mix_hbm, mix_ref),
        ])
    ]
    for load in loads:
        load.start()
    barrier = pltpu.get_barrier_semaphore()
    others = [lax.rem(lev + d, 8) for d in range(1, 8)]
    for other in others:
        pl.semaphore_signal(barrier, inc=1, device_id={"lev": other}, device_id_type=MESH)
    for side in (west, east):
        pl.semaphore_signal(barrier, inc=1, device_id={"lev": partner, "lon": side}, device_id_type=MESH)

    def greet(d, carry):
        pl.semaphore_signal(barrier, inc=1, device_id={"lon": lax.rem(lon + d, count)}, device_id_type=MESH)
        return carry

    lax.fori_loop(1, count, greet, 0)

    def remote(src, dst, send, recv, where):
        return pltpu.make_async_remote_copy(
            src_ref=src, dst_ref=dst, send_sem=send, recv_sem=recv, device_id=where, device_id_type=MESH
        )

    def rows_at(start, size):
        return pl.ds(pl.multiple_of(start, 8), size)

    pending = []

    def start(copy):
        copy.start()
        pending.append(copy)
        return copy

    loads[0].wait()
    loads[1].wait()
    parts = interior(link_ref, loss_ref, row.at[core], pack)
    loads[3].wait()
    loads[4].wait()
    mix_row_of(mix_ref, mixrow.at[core])
    pl.semaphore_wait(barrier, 8 + count)
    packs[lev] = pack[...]
    spread = [
        start(remote(pack, packs.at[lev], pack_send.at[i], pack_recv.at[i], {"lev": target}))
        for i, target in enumerate([2 * lax.rem(chip + d, 4) + core for d in (2, 1, 3)] + [partner])
    ]
    loads[2].wait()
    field_of(prev_ref, field)

    def hand_on(i, d):
        spread[i].wait_recv()
        source = 2 * lax.rem(chip + 4 - d, 4) + core
        return start(remote(packs.at[source], packs.at[source], pack_send.at[4 + i], pack_recv.at[4 + i], {"lev": partner}))

    away = 1 - core
    gives = [
        start(remote(src, dst, give_send.at[i], give_recv.at[i], {"lev": partner}))
        for i, (src, dst) in enumerate([
            (field.at[rows_at(248 * away, 264)], state.at[0, core, rows_at(8 * core, 264)]),
            (pair_ref.at[core], pair_ref.at[core]),
            (mixrow.at[core], mixrow.at[core]),
            (row.at[core], row.at[core]),
        ])
    ]
    outer = [
        start(remote(field.at[0:8], state.at[0, core, 264:272], halo_send.at[0, 0], halo_recv.at[0, core],
                     {"lev": base + 1, "lon": west})),
        start(remote(field.at[504:512], state.at[0, core, 0:8], halo_send.at[0, 1], halo_recv.at[0, core],
                     {"lev": base, "lon": east})),
    ]
    state[0, core, rows_at(8 * away, 264), :] = field[rows_at(248 * core, 264), :]
    finish_interior(*parts, full.at[core])
    give_full = start(remote(full.at[core], full.at[core], give_send.at[4], give_recv.at[4], {"lev": partner}))

    def pair_term(it, s):
        for r in range(0, 256, 128):
            here = state[it, s, 8 + r : 136 + r, :]
            squares = split(here * here)
            for half in range(2):
                piece = tuple(x[:, 256 * half : 256 * half + 256] for x in squares)
                sums[s, r : r + 128, 256 * half : 256 * half + 256] = dot3(piece, (pw_hi[s, half], pw_lo[s, half]), NT)
            piece = tuple(x[:, 512:576] for x in squares)
            sums[s, r : r + 128, 512:576] = dot3(piece, (pn_hi[s], pn_lo[s]), NT)

    def forcing_term(it, s, chunks=((0, 128), (128, 128))):
        for r, n in chunks:
            here = state[it, s, 8 + r : 8 + r + n, 0:576]
            around = state[it, s, 7 + r : 7 + r + n, 0:576] + state[it, s, 9 + r : 9 + r + n, 0:576]
            forcing = state[0, s, 8 + r : 8 + r + n, 0:576] - sums[s, r : r + n, 0:576]
            forcing += mixrow[s, 0:1, 0:576] * (around - 2.0 * here)
            pieces = split(forcing[:, 0:512])
            gs_hi[s, r : r + n, :], gs_lo[s, r : r + n, :] = pieces
            node = forcing[:, 512:576]
            push = dot3(pieces, (hr_hi[s], hr_lo[s]), NT)
            injs[s, r : r + n, :] = push + jnp.concatenate([node, jnp.zeros_like(node)], axis=1)

    def weights(s):
        pair_weights(pair_ref.at[s], pw_hi.at[s], pw_lo.at[s], pn_hi.at[s], pn_lo.at[s])
        hr_hi[s], hr_lo[s] = split(row[s])

    def product(it, s):
        if it == ITERS - 1:
            for b in range(4):
                rows = slice(128 * b, 128 * b + 128)
                value = dot3((g_hi[s, rows, :], g_lo[s, rows, :]), (gs_hi[s], gs_lo[s]), NT)
                for h in range(2):
                    outs[s, ORDER[2 * b + h]] = value[64 * h : 64 * h + 64]
        else:
            for r in range(0, 256, 128):
                pieces = (gs_hi[s, r : r + 128, :], gs_lo[s, r : r + 128, :])
                state[it + 1, s, 8 + r : 136 + r, 0:512] = dot3(pieces, (g_hi[s], g_lo[s]))

    weights(core)
    pair_term(0, core)
    for slot in range(2):
        pltpu.make_async_copy(field.at[0:8], state.at[0, 0, 0:8], halo_recv.at[0, slot]).wait()
    forcing_term(0, core)
    handed = [hand_on(1, 1), hand_on(2, 3)]
    for give in gives:
        give.wait_recv()
    weights(away)
    handed.append(hand_on(0, 2))
    pair_term(0, away)
    forcing_term(0, away)
    for copy in [spread[3]] + handed:
        copy.wait_recv()
    interface(packs, own_hi, own_lo, msg_hi, msg_lo, rlo_hi, rlo_lo, rhi_hi, rhi_lo, wp, wc, rs, rc, own)
    for it in range(ITERS):
        final = it == ITERS - 1
        if it:
            inner_from, inner_to = 8 + 248 * away, 264 * core
            outer_from, outer_to = 8 + 248 * core, 264 * away
            halos = [
                start(remote(state.at[it, :, rows_at(a, 8), :], state.at[it, :, rows_at(b, 8), :],
                             halo_send.at[it, i], halo_recv.at[it, i], where))
                for i, (a, b, where) in enumerate([
                    (outer_from, outer_to, {"lev": partner, "lon": west + (east - west) * core}),
                    (inner_from, inner_to, {"lev": partner}),
                ])
            ]
            for s in range(2):
                pair_term(it, s)
            for s in range(2):
                forcing_term(it, s, ((16, 112), (128, 112)))
            for halo in halos:
                halo.wait_recv()
            for s in range(2):
                forcing_term(it, s, ((0, 16), (240, 16)))
        inj = jnp.concatenate([injs[0], injs[1]], axis=1)
        packed = split(jnp.concatenate([inj[0:128], inj[128:256]], axis=1))
        message = dot3(packed, (msg_hi[...], msg_lo[...]))
        outgo[it, 0] = message[:, 0:128]
        outgo[it, 1] = message[:, 128:256]
        slot = 1 + lax.rem(chip, 2)
        start(remote(outgo.at[it, 1], incoming.at[it, slot], msg_send.at[it, 1], msg_recv.at[it, slot], {"lev": across[0]}))
        start(remote(outgo.at[it, 1], incoming.at[it, slot], msg_send.at[it, 2], msg_recv.at[it, slot], {"lev": across[1]}))
        start(remote(outgo.at[it, 0], incoming.at[it, 0], msg_send.at[it, 0], msg_recv.at[it, 0], {"lev": sibling}))
        mine = dot3(split(inj), (own_hi[...], own_lo[...]))
        if it == 0:
            give_full.wait_recv()
            for s in range(2):
                g_hi[s], g_lo[s] = split(full[s])
                hc_hi[s], hc_lo[s] = split(row[s].T)
        for s in range(2):
            product(it, s)
        for slot in range(3):
            pltpu.make_async_copy(outgo.at[it, 0], incoming.at[it, slot], msg_recv.at[it, slot]).wait()
        heard = split(jnp.concatenate([incoming[it, 0], incoming[it, 1] + incoming[it, 2]], axis=1))
        total = mine + jnp.concatenate(
            [dot3(heard, (rlo_hi[...], rlo_lo[...])), dot3(heard, (rhi_hi[...], rhi_lo[...]))], axis=0
        )
        if not final:
            for s in range(2):
                ends = total[:, 128 * s : 128 * s + 128]
                state[it + 1, s, 8:264, 0:512] += dot3(split(ends), (hr_hi[s], hr_lo[s]))
                state[it + 1, s, 8:264, 512:640] = jnp.where(
                    lax.broadcasted_iota(jnp.int32, (256, 128), 1) < S, ends, 0.0
                )
    ends_ref[0] = total[:, 0:128]
    ends_ref[1] = total[:, 128:256]
    ones = jnp.ones((8, 256), BF16)
    dot1 = lambda x: lax.dot_general(ones, x, NT, preferred_element_type=F32)
    line = lax.broadcasted_iota(jnp.int32, (8, 128), 0)

    def finish(s):
        ends = ends_ref[s]
        pieces = split(ends)
        squares = jnp.zeros((8, 128), F32)
        for b in range(5):
            if b < 4:
                rows = slice(128 * b, 128 * b + 128)
                value = dot3((hc_hi[s, rows, :], hc_lo[s, rows, :]), pieces, NT)
                value += jnp.concatenate([outs[s, ORDER[2 * b]], outs[s, ORDER[2 * b + 1]]], axis=0)
                outs[s, ORDER[2 * b]] = value[0:64]
                outs[s, ORDER[2 * b + 1]] = value[64:128]
            else:
                value = jnp.concatenate([ends.T[0:64], jnp.zeros((64, 256), F32)], axis=0)
                outs[s, 0] = value[0:64]
            high, low = split(value * value)
            squares = jnp.where(line == b, dot1(high) + dot1(low), squares)
        part[s] = squares[0:5]

    finish(away)
    give = start(remote(part.at[away], part_in, out_send.at[0], out_recv.at[0], {"lev": partner}))
    back = start(remote(outs.at[away], out_any.at[core], out_send.at[1], out_recv.at[1], {"lev": partner}))
    finish(core)
    keep = pltpu.make_async_copy(outs.at[core], out_any.at[core], load_sem.at[0])
    keep.start()
    give.wait_recv()
    mysum[...] = part[core] + part_in[...]
    own_sum = pltpu.make_async_copy(mysum, sumbuf.at[lon], load_sem.at[1])
    own_sum.start()
    steps = [(dy, dz) for dy in range(deep) for dz in range(count // deep) if dy or dz]
    steps.sort(key=lambda step: -min(step[0], deep - step[0]) - min(step[1], count // deep - step[1]))
    wide_z = count // deep
    y, z = lon // wide_z, lax.rem(lon, wide_z)
    at = lambda dy, dz: lax.rem(y + dy, deep) * wide_z + lax.rem(z + dz, wide_z)
    for i, (dy, dz) in enumerate(steps):
        start(remote(mysum, sumbuf.at[lon], sum_send.at[i], sum_recv.at[lon], {"lon": at(dy, dz)}))
    keep.wait()
    back.wait_recv()
    own_sum.wait()
    for copy in pending:
        copy.wait_send()
    for dy, dz in reversed(steps):
        source = at(deep - dy, wide_z - dz)
        pltpu.make_async_copy(mysum, sumbuf.at[source], sum_recv.at[source]).wait()


def put_out(field_any, sums_ref, out_ref, var_ref, sem):
    copies = [
        pltpu.make_async_copy(field_any.at[half], out_ref.at[:, :, pl.ds(256 * half, 256)], sem.at[half])
        for half in range(2)
    ]
    for copy in copies:
        copy.start()
    count = sums_ref.shape[0]
    total = jnp.sum(sums_ref[...], axis=0) * (1.0 / (512 * count))
    for j in range(9):
        level = (ORDER + (0,))[j]
        var_ref[level : level + 1, :] = total[j // 2 : j // 2 + 1, S * (j % 2) : S * (j % 2) + S]
    for copy in copies:
        copy.wait()


def vmem(count):
    return [pl.BlockSpec(memory_space=pltpu.VMEM)] * count


def local(previous, loss_matrix, pair_matrix, diffusivity, mixing):
    count = lax.axis_size("lon")
    low = lambda *shape: [pltpu.VMEM(shape, BF16)] * 2
    full = lambda *shape: [pltpu.VMEM(shape, F32)]
    sems = lambda *shape: [pltpu.SemaphoreType.DMA(shape)] * 2
    scratch = [pltpu.SMEM((9,), F32)] * 2 + full(9, S, S) + full(2, 9, S, S) + full(9, S, 512) + [pltpu.SemaphoreType.DMA((5,))]
    scratch += full(2, 512, 512) + full(2, 128, 512) + low(2, 512, 512) + low(2, 128, 512) + low(2, 512, 128) + full(96, 128)
    scratch += low(2, 2, 256, 256) + low(2, S, S) + full(512, 640) + full(2, 8, 640)
    scratch += full(8, 96, 128) + low(256, 256) + low(512, 256) + low(256, 256) * 2
    scratch += full(256, S) * 2 + full(S, 256) * 2 + full(256, 256)
    scratch += full(2, 2, 272, 640) + low(2, 256, 512) + full(2, 256, 128) + full(2, 2, 128, 128) + full(2, 3, 128, 128)
    scratch += full(2, 256, 640) + full(2, 9, S, 256) + full(2, 256, 128) + full(2, 5, 128) + full(5, 128) * 2
    scratch += sems(7) + sems(5) + sems(2, 2) + sems(2, 3) + sems(2) + sems(count)
    shapes = [jax.ShapeDtypeStruct((9, S, 512), F32), jax.ShapeDtypeStruct((9, S), F32)]
    halves = jax.ShapeDtypeStruct((2, 9, S, 256), F32)
    anywhere = [pl.BlockSpec(memory_space=pl.ANY)] * 2
    done = pl.pallas_call(
        functools.partial(kernel, count, 4 if count % 4 == 0 else 1),
        out_shape=[halves, jax.ShapeDtypeStruct((count, 5, 128), F32)],
        in_specs=[pl.BlockSpec(memory_space=pltpu.HBM)] * 5,
        out_specs=tuple(anywhere),
        scratch_shapes=scratch,
        compiler_params=pltpu.CompilerParams(vmem_limit_bytes=32 * 2**20, collective_id=0, has_side_effects=True),
    )(*[pltpu.with_memory_space_constraint(x, pltpu.HBM) for x in (diffusivity, mixing, loss_matrix, pair_matrix, previous)])
    return tuple(pl.pallas_call(
        put_out,
        out_shape=shapes,
        in_specs=anywhere[:1] + vmem(1),
        out_specs=(anywhere[0], vmem(1)[0]),
        scratch_shapes=[pltpu.SemaphoreType.DMA((2,))],
        compiler_params=pltpu.CompilerParams(vmem_limit_bytes=8 * 2**20),
    )(*done))


def solution(mesh):
    placed = (P("lev", None, "lon"), P("lev", None, None), P("lev", None, None), P("lev"), P("lev"))
    return jax.shard_map(
        local,
        mesh=mesh,
        in_specs=placed,
        out_specs=(P("lev", None, "lon"), P("lev", None)),
        check_vma=False,
    )
```

```python
import functools

import jax
import jax.numpy as jnp
from jax import lax
from jax.experimental import pallas as pl
from jax.experimental.pallas import tpu as pltpu
from jax.sharding import PartitionSpec as P

ITERS = 2
F32 = jnp.float32
BF16 = jnp.bfloat16
MESH = pl.DeviceIdType.MESH
HIGHEST = lax.Precision.HIGHEST

S = 64
ORDER = (1, 2, 4, 5, 7, 8, 3, 6)
NN = (((1,), (0,)), ((), ()))
NT = (((1,), (1,)), ((), ()))
TN = (((0,), (0,)), ((), ()))


def split(x):
    high = x.astype(BF16)
    return high, (x - high.astype(F32)).astype(BF16)


def dot3(a, b, dims=NN):
    one = lambda x, y: lax.dot_general(x, y, dims, preferred_element_type=F32)
    return one(a[0], b[0]) + (one(a[0], b[1]) + one(a[1], b[0]))


def mm(a, b, dims=NN):
    return dot3(split(a), split(b), dims)


def mm_full(a, b, dims=NN):
    return lax.dot_general(a, b, dims, precision=HIGHEST, preferred_element_type=F32)


def eye(n):
    rows = lax.broadcasted_iota(jnp.int32, (n, n), 0)
    return (rows == lax.broadcasted_iota(jnp.int32, (n, n), 1)).astype(F32)


def spd_inverses(blocks, lows, high, doublings):
    centres = [0.5 * (high + low) for low in lows]
    units = [eye(block.shape[0]) for block in blocks]
    inverses = [unit * (1.0 / centre) for unit, centre in zip(units, centres)]
    residuals = [unit - block * (1.0 / centre) for unit, block, centre in zip(units, blocks, centres)]
    terms = [(high + low) / (high - low) for low in lows]
    for step in range(doublings):
        last = step == doublings - 1
        for i, unit in enumerate(units):
            twice = 2.0 * terms[i] * terms[i] - 1.0
            gain, shift = (twice + 1.0) / twice, 1.0 / twice
            terms[i] = twice
            centre = centres[i]
            n = unit.shape[0]
            rest = split(residuals[i])
            if step == 0:
                inverses[i] = (inverses[i] + residuals[i] * (1.0 / centre)) * gain
                if not last:
                    residuals[i] = gain * dot3(rest, rest) - shift * unit
                continue
            known = split(inverses[i])
            if last:
                inverses[i] = gain * (inverses[i] + dot3(known, rest))
                continue
            both = dot3(tuple(jnp.concatenate(p, axis=0) for p in zip(known, rest)), rest)
            inverses[i] = gain * (inverses[i] + both[:n])
            residuals[i] = gain * both[n:] - shift * unit
    exact = [unit - mm_full(block, inverse) for unit, block, inverse in zip(units, blocks, inverses)]
    step = lambda x, y: lax.dot_general(x.astype(BF16), y.astype(BF16), NN, preferred_element_type=F32)
    return [inverse + step(inverse, rest) for inverse, rest in zip(inverses, exact)]


def wide(grid):
    return jnp.concatenate([jnp.concatenate(row, axis=1) if len(row) > 1 else row[0] for row in grid], axis=0)


def interior(link_ref, loss_ref, row_ref, pack_ref):
    one = eye(S)
    zero = jnp.zeros((S, S), F32)
    links = [link_ref[i] for i in range(9)]
    shunt = [loss_ref[i] + one for i in range(9)]
    blocks = []
    for top in (1, 4, 7):
        diag = [shunt[level] + (links[level - 1] + links[level]) * one for level in (top, top + 1)]
        tie = -links[top] * one
        blocks.append(wide([[diag[0], tie], [tie, diag[1]]]))
    pairs = spd_inverses(blocks, [199.0] * 3, 6700.0, 5)
    none = jnp.zeros((S, 128), F32)
    spread = wide([
        [links[2] * pairs[0][S:], links[3] * pairs[1][:S], none],
        [none, links[5] * pairs[1][S:], links[6] * pairs[2][:S]],
    ])
    ground = jnp.concatenate(
        [shunt[1] + links[0] * one, shunt[2], shunt[4], shunt[5], shunt[7], shunt[8] + links[8] * one], axis=0
    )
    own = jnp.concatenate([shunt[3], shunt[6]], axis=0) + mm_full(spread, ground)
    down = links[5] * spread[0:S, 192:256]
    up = links[3] * spread[S:, 128:192]
    middle, = spd_inverses([wide([[own[:S] + down, -down], [-up, own[S:] + up]])], [68.6], 3010.0, 5)
    spread = jnp.concatenate([spread, eye(128)], axis=1)
    lifted = mm(middle, spread)
    lane = lax.broadcasted_iota(jnp.int32, (128, 128), 1)
    ends = mm(jnp.where(lane < S, spread[:, 0:128], spread[:, 256:384]), lifted, TN)
    first = jnp.concatenate([ends[0:S, 0:128] + pairs[0][:S], ends[0:S, 128:512]], axis=1)
    last = jnp.concatenate([ends[S:, 0:256], ends[S:, 256:384] + pairs[2][S:], ends[S:, 384:512]], axis=1)
    rows = jnp.concatenate([links[0] * first, links[8] * last], axis=0)
    row_ref[...] = rows
    loads = mm_full(rows, jnp.concatenate([shunt[level] for level in ORDER], axis=0))
    across = links[8] * rows[0:S, 320:384]
    pack_ref[0:64, :] = jnp.concatenate([shunt[0] + loads[0:S], loads[S:]], axis=1)
    pack_ref[64:96, :] = jnp.concatenate([across[0:32], across[32:64]], axis=1)
    return pairs, spread, lifted


def finish_interior(pairs, spread, lifted, full):
    full[...] = mm(spread, lifted, TN)
    for i in range(3):
        at = slice(128 * i, 128 * i + 128)
        full[at, at] += pairs[i]


def pair_weights(pair_ref, pw_hi, pw_lo, pn_hi, pn_lo):
    for half in range(2):
        row = lax.broadcasted_iota(jnp.int32, (256, 256), 0) // S
        column = lax.broadcasted_iota(jnp.int32, (256, 256), 1) // S
        tall = jnp.concatenate([pair_ref[level] for level in ORDER[4 * half : 4 * half + 4]], axis=0)
        tall = jnp.concatenate([tall, tall], axis=1)
        tall = jnp.where(row == column, jnp.concatenate([tall, tall], axis=1), 0.0)
        pw_hi[half], pw_lo[half] = split(tall)
    pn_hi[...], pn_lo[...] = split(pair_ref[0])


def field_of(prev_ref, field_ref):
    for j in range(4):
        both = jnp.concatenate([prev_ref[ORDER[2 * j]], prev_ref[ORDER[2 * j + 1]]], axis=0)
        field_ref[:, 128 * j : 128 * j + 128] = both.T
    last = jnp.concatenate([prev_ref[0], jnp.zeros_like(prev_ref[0])], axis=0)
    field_ref[:, 512:640] = last.T


def mix_row_of(mix_ref, mixrow_ref):
    lane = lax.broadcasted_iota(jnp.int32, (8, 640), 1) // S
    row = jnp.zeros((8, 640), F32)
    for j, level in enumerate(ORDER + (0,)):
        row = jnp.where(lane == j, mix_ref[level], row)
    mixrow_ref[...] = row


def unpack(packs, q):
    both, folded = packs(q)
    across = jnp.concatenate([folded[:, 0:S], folded[:, S:]], axis=0)
    return both[:, 0:S], both[:, S:], across


def interface(pack_ref, own_hi, own_lo, msg_hi, msg_lo, rlo_hi, rlo_lo, rhi_hi, rhi_lo, wp, wc, rs, rc, own):
    chip = lax.axis_index("lev") // 2
    one = eye(S)
    zero = jnp.zeros((S, S), F32)
    here, below, across = zip(*[
        unpack(lambda q: (pack_ref[q, 0:64, :], pack_ref[q, 64:96, :]), q) for q in range(8)
    ])
    back = [a.T for a in across]
    ground = [here[q] + (below[q - 1] if q else 0.0) for q in range(8)]
    diag = [ground[q] + across[q] + (back[q - 1] if q else 0.0) for q in range(8)]
    upper = wide([
        [diag[0], -across[0], zero, zero],
        [-back[0], diag[1], -across[1], zero],
        [zero, -back[1], diag[2], -across[2]],
        [zero, zero, -back[2], diag[3]],
    ])
    lower = wide([
        [diag[5], -across[5], zero],
        [-back[5], diag[6], -across[6]],
        [zero, -back[6], diag[7]],
    ])
    first = chip < 2
    small = jnp.where(
        first, upper[0:128, 0:128], wide([[500.0 * one, zero], [zero, diag[7]]])
    )
    upper_inverse, lower_inverse, small_inverse = spd_inverses(
        [upper, lower, small], [9.6, 21.0, 13.9], 2400.0, 6
    )
    upper_t = mm(back[3], upper_inverse[192:256, :])
    lower_t = mm(across[4], lower_inverse[0:64, :])
    middle = (
        ground[4]
        + mm_full(upper_t, jnp.concatenate(ground[0:4], axis=0))
        + mm_full(lower_t, jnp.concatenate([ground[5], ground[6], ground[7] + across[7]], axis=0))
    )
    middle_inverse, = spd_inverses([middle], [28.7], 2400.0, 5)
    spread = jnp.concatenate([upper_t, lower_t, one], axis=1)
    lifted = mm(middle_inverse, spread)
    place = {0: 0, 1: 1, 2: 2, 3: 3, 4: 7, 5: 4, 6: 5, 7: 6}
    link = jnp.where(first, back[1], across[6])
    away = mm(link, small_inverse[64:128, :])

    for c in range(4):
        nodes = (2 * c, 2 * c + 1, 2 * c + 1, 2 * c + 2)

        @pl.when(chip == c)
        def _(c=c, nodes=nodes):
            real = [n for n in range(2 * c, 2 * c + 3) if n < 8]
            against = real if 4 in real else real + [4]
            part = lambda x, n: x[:, S * place[n] : S * place[n] + S]
            both = [jnp.concatenate([part(x, n) for n in which], axis=1) for x, which in ((spread, real), (lifted, against))]
            product = mm(both[0], both[1], TN)

            def block(r, k):
                if r not in real or k not in against:
                    return zero
                i, j = real.index(r), against.index(k)
                value = product[S * i : S * i + S, S * j : S * j + S]
                i, j = place[r], place[k]
                if i < 4 and j < 4:
                    value += upper_inverse[S * i : S * i + S, S * j : S * j + S]
                elif 4 <= i < 7 and 4 <= j < 7:
                    value += lower_inverse[S * (i - 4) : S * (i - 3), S * (j - 4) : S * (j - 3)]
                return value

            def blocks(rows, columns):
                return wide([[block(r, k) for k in columns] for r in rows])

            own[...] = blocks(nodes, nodes)
            wc[...] = blocks(nodes, (4,))
            if c in (0, 3):
                far = [away[:, 0:64], away[:, 64:128]]
                if c == 0:
                    rs[...] = jnp.concatenate([far[0], far[1], far[1], one], axis=1)
                    wp[...] = jnp.concatenate([far[0].T, far[1].T, far[1].T, one], axis=0)
                else:
                    rs[...] = jnp.concatenate([one, far[1], far[1], zero], axis=1)
                    wp[...] = jnp.concatenate([one, far[1].T, far[1].T, zero], axis=0)
            else:
                gate = 2 if c == 1 else 6
                rs[...] = blocks((gate,), nodes)
                wp[...] = blocks(nodes, (gate,))

            def seen(n):
                if n > 7:
                    return zero
                n = place[n]
                return spread[:, S * n : S * n + S]

            rc[...] = jnp.concatenate([seen(n) for n in nodes], axis=1)

    own_hi[...], own_lo[...] = split(own[...])
    none = jnp.zeros((256, S), F32)
    msg = wide([[wp[...], none, wc[...], none], [none, wp[...], none, wc[...]]])
    msg_hi[...], msg_lo[...] = split(msg)
    none = jnp.zeros((S, 256), F32)
    rlo_hi[...], rlo_lo[...] = split(jnp.concatenate([rs[...], none, rc[...], none], axis=0))
    rhi_hi[...], rhi_lo[...] = split(jnp.concatenate([none, rs[...], none, rc[...]], axis=0))


def kernel(count, deep, link_hbm, mix_hbm, loss_hbm, pair_hbm, prev_hbm, out_any, var_ref,
           link_ref, mix_ref, loss_ref, pair_ref, prev_ref, load_sem,
           full, row, g_hi, g_lo, hr_hi, hr_lo, hc_hi, hc_lo, pack, pw_hi, pw_lo, pn_hi, pn_lo, field, mixrow,
           packs, own_hi, own_lo, msg_hi, msg_lo, rlo_hi, rlo_lo, rhi_hi, rhi_lo, wp, wc, rs, rc, own,
           state, gs_hi, gs_lo, injs, outgo, incoming, sums, outs, part, part_in, mysum, sumbuf,
           pack_send, pack_recv, give_send, give_recv, halo_send, halo_recv, msg_send, msg_recv, out_send, out_recv,
           sum_send, sum_recv):
    lev = lax.axis_index("lev")
    lon = lax.axis_index("lon")
    core = lax.rem(lev, 2)
    chip = lev // 2
    partner = lev + 1 - 2 * core
    base = lev - core
    sibling = 2 * (chip + 1 - 2 * lax.rem(chip, 2)) + core
    across_base = 2 - 2 * (chip // 2)
    far = lax.rem(chip + 2, 4)
    across = [2 * far + core, 2 * (2 * across_base + 1 - far) + core]
    west, east = lax.rem(lon + count - 1, count), lax.rem(lon + 1, count)
    loads = [
        pltpu.make_async_copy(src, dst, load_sem.at[i])
        for i, (src, dst) in enumerate([
            (link_hbm, link_ref), (loss_hbm, loss_ref), (prev_hbm, prev_ref), (pair_hbm, pair_ref.at[core]), (mix_hbm, mix_ref),
        ])
    ]
    for load in loads:
        load.start()
    barrier = pltpu.get_barrier_semaphore()
    others = [lax.rem(lev + d, 8) for d in range(1, 8)]
    for other in others:
        pl.semaphore_signal(barrier, inc=1, device_id={"lev": other}, device_id_type=MESH)
    for side in (west, east):
        pl.semaphore_signal(barrier, inc=1, device_id={"lev": partner, "lon": side}, device_id_type=MESH)

    def greet(d, carry):
        pl.semaphore_signal(barrier, inc=1, device_id={"lon": lax.rem(lon + d, count)}, device_id_type=MESH)
        return carry

    lax.fori_loop(1, count, greet, 0)

    def remote(src, dst, send, recv, where):
        return pltpu.make_async_remote_copy(
            src_ref=src, dst_ref=dst, send_sem=send, recv_sem=recv, device_id=where, device_id_type=MESH
        )

    def rows_at(start, size):
        return pl.ds(pl.multiple_of(start, 8), size)

    pending = []

    def start(copy):
        copy.start()
        pending.append(copy)
        return copy

    loads[0].wait()
    loads[1].wait()
    parts = interior(link_ref, loss_ref, row.at[core], pack)
    loads[3].wait()
    loads[4].wait()
    mix_row_of(mix_ref, mixrow.at[core])
    pl.semaphore_wait(barrier, 8 + count)
    packs[lev] = pack[...]
    spread = [
        start(remote(pack, packs.at[lev], pack_send.at[i], pack_recv.at[i], {"lev": target}))
        for i, target in enumerate([2 * lax.rem(chip + d, 4) + core for d in (2, 1, 3)] + [partner])
    ]
    loads[2].wait()
    field_of(prev_ref, field)

    def hand_on(i, d):
        spread[i].wait_recv()
        source = 2 * lax.rem(chip + 4 - d, 4) + core
        return start(remote(packs.at[source], packs.at[source], pack_send.at[4 + i], pack_recv.at[4 + i], {"lev": partner}))

    away = 1 - core
    gives = [
        start(remote(src, dst, give_send.at[i], give_recv.at[i], {"lev": partner}))
        for i, (src, dst) in enumerate([
            (field.at[rows_at(248 * away, 264)], state.at[0, core, rows_at(8 * core, 264)]),
            (pair_ref.at[core], pair_ref.at[core]),
            (mixrow.at[core], mixrow.at[core]),
            (row.at[core], row.at[core]),
        ])
    ]
    outer = [
        start(remote(field.at[0:8], state.at[0, core, 264:272], halo_send.at[0, 0], halo_recv.at[0, core],
                     {"lev": base + 1, "lon": west})),
        start(remote(field.at[504:512], state.at[0, core, 0:8], halo_send.at[0, 1], halo_recv.at[0, core],
                     {"lev": base, "lon": east})),
    ]
    state[0, core, rows_at(8 * away, 264), :] = field[rows_at(248 * core, 264), :]
    finish_interior(*parts, full.at[core])
    give_full = start(remote(full.at[core], full.at[core], give_send.at[4], give_recv.at[4], {"lev": partner}))

    def pair_term(it, s):
        for r in range(0, 256, 128):
            here = state[it, s, 8 + r : 136 + r, :]
            squares = split(here * here)
            for half in range(2):
                piece = tuple(x[:, 256 * half : 256 * half + 256] for x in squares)
                sums[s, r : r + 128, 256 * half : 256 * half + 256] = dot3(piece, (pw_hi[s, half], pw_lo[s, half]), NT)
            piece = tuple(x[:, 512:576] for x in squares)
            sums[s, r : r + 128, 512:576] = dot3(piece, (pn_hi[s], pn_lo[s]), NT)

    def forcing_term(it, s, chunks=((0, 128), (128, 128))):
        for r, n in chunks:
            here = state[it, s, 8 + r : 8 + r + n, 0:576]
            around = state[it, s, 7 + r : 7 + r + n, 0:576] + state[it, s, 9 + r : 9 + r + n, 0:576]
            forcing = state[0, s, 8 + r : 8 + r + n, 0:576] - sums[s, r : r + n, 0:576]
            forcing += mixrow[s, 0:1, 0:576] * (around - 2.0 * here)
            pieces = split(forcing[:, 0:512])
            gs_hi[s, r : r + n, :], gs_lo[s, r : r + n, :] = pieces
            node = forcing[:, 512:576]
            push = dot3(pieces, (hr_hi[s], hr_lo[s]), NT)
            injs[s, r : r + n, :] = push + jnp.concatenate([node, jnp.zeros_like(node)], axis=1)

    def weights(s):
        pair_weights(pair_ref.at[s], pw_hi.at[s], pw_lo.at[s], pn_hi.at[s], pn_lo.at[s])
        hr_hi[s], hr_lo[s] = split(row[s])

    def product(it, s):
        if it == ITERS - 1:
            for b in range(4):
                rows = slice(128 * b, 128 * b + 128)
                value = dot3((g_hi[s, rows, :], g_lo[s, rows, :]), (gs_hi[s], gs_lo[s]), NT)
                for h in range(2):
                    outs[s, ORDER[2 * b + h]] = value[64 * h : 64 * h + 64]
        else:
            for r in range(0, 256, 128):
                pieces = (gs_hi[s, r : r + 128, :], gs_lo[s, r : r + 128, :])
                state[it + 1, s, 8 + r : 136 + r, 0:512] = dot3(pieces, (g_hi[s], g_lo[s]))

    middle, edges = ((16, 112), (128, 112)), ((0, 16), (240, 16))
    weights(core)
    pair_term(0, core)
    forcing_term(0, core, middle)
    for give in gives:
        give.wait_recv()
    weights(away)
    handed = [hand_on(1, 1), hand_on(2, 3)]
    pair_term(0, away)
    forcing_term(0, away, middle)
    handed.append(hand_on(0, 2))
    for slot in range(2):
        pltpu.make_async_copy(field.at[0:8], state.at[0, 0, 0:8], halo_recv.at[0, slot]).wait()
    for s in range(2):
        forcing_term(0, s, edges)
    for copy in [spread[3]] + handed:
        copy.wait_recv()
    interface(packs, own_hi, own_lo, msg_hi, msg_lo, rlo_hi, rlo_lo, rhi_hi, rhi_lo, wp, wc, rs, rc, own)
    for it in range(ITERS):
        final = it == ITERS - 1
        if it:
            for s in range(2):
                pair_term(it, s)
            for s in range(2):
                forcing_term(it, s, middle)
            for halo in halos:
                halo.wait_recv()
            for s in range(2):
                forcing_term(it, s, edges)
        inj = jnp.concatenate([injs[0], injs[1]], axis=1)
        packed = split(jnp.concatenate([inj[0:128], inj[128:256]], axis=1))
        message = dot3(packed, (msg_hi[...], msg_lo[...]))
        outgo[it, 0] = message[:, 0:128]
        outgo[it, 1] = message[:, 128:256]
        slot = 1 + lax.rem(chip, 2)
        start(remote(outgo.at[it, 1], incoming.at[it, slot], msg_send.at[it, 1], msg_recv.at[it, slot], {"lev": across[0]}))
        start(remote(outgo.at[it, 1], incoming.at[it, slot], msg_send.at[it, 2], msg_recv.at[it, slot], {"lev": across[1]}))
        start(remote(outgo.at[it, 0], incoming.at[it, 0], msg_send.at[it, 0], msg_recv.at[it, 0], {"lev": sibling}))
        mine = dot3(split(inj), (own_hi[...], own_lo[...]))
        if it == 0:
            give_full.wait_recv()
            for s in range(2):
                g_hi[s], g_lo[s] = split(full[s])
                hc_hi[s], hc_lo[s] = split(row[s].T)
        for s in range(2):
            product(it, s)
        for slot in range(3):
            pltpu.make_async_copy(outgo.at[it, 0], incoming.at[it, slot], msg_recv.at[it, slot]).wait()
        heard = split(jnp.concatenate([incoming[it, 0], incoming[it, 1] + incoming[it, 2]], axis=1))
        total = mine + jnp.concatenate(
            [dot3(heard, (rlo_hi[...], rlo_lo[...])), dot3(heard, (rhi_hi[...], rhi_lo[...]))], axis=0
        )
        total_of = [total[:, 128 * s : 128 * s + 128] for s in range(2)]
        if not final:
            def land(s, low, high):
                ends = total_of[s][low:high]
                rows = slice(8 + low, 8 + high)
                state[it + 1, s, rows, 0:512] += dot3(split(ends), (hr_hi[s], hr_lo[s]))
                state[it + 1, s, rows, 512:640] = jnp.where(
                    lax.broadcasted_iota(jnp.int32, (high - low, 128), 1) < S, ends, 0.0
                )

            for s in range(2):
                land(s, 0, 16)
                land(s, 240, 256)
            inner_from, inner_to = 8 + 248 * away, 264 * core
            outer_from, outer_to = 8 + 248 * core, 264 * away
            halos = [
                start(remote(state.at[it + 1, :, rows_at(a, 8), :], state.at[it + 1, :, rows_at(b, 8), :],
                             halo_send.at[it + 1, i], halo_recv.at[it + 1, i], where))
                for i, (a, b, where) in enumerate([
                    (outer_from, outer_to, {"lev": partner, "lon": west + (east - west) * core}),
                    (inner_from, inner_to, {"lev": partner}),
                ])
            ]
            for s in range(2):
                land(s, 16, 240)
            continue
        for s in range(2):
            pieces = split(total_of[s])
            for b in range(4):
                rows = slice(128 * b, 128 * b + 128)
                value = dot3((hc_hi[s, rows, :], hc_lo[s, rows, :]), pieces, NT)
                for h in range(2):
                    outs[s, ORDER[2 * b + h]] += value[64 * h : 64 * h + 64]
            outs[s, 0] = total_of[s].T[0:64]
    ones = jnp.ones((8, 256), BF16)
    dot1 = lambda x: lax.dot_general(ones, x, NT, preferred_element_type=F32)
    line = lax.broadcasted_iota(jnp.int32, (8, 128), 0)

    def squares_of(s):
        packed = jnp.zeros((8, 128), F32)
        for j in range(5):
            values = [outs[s, level] for level in ((ORDER + (0,))[2 * j : 2 * j + 2])]
            values = jnp.concatenate(values if j < 4 else values + [jnp.zeros_like(values[0])], axis=0)
            high, low = split(values * values)
            packed = jnp.where(line == j, dot1(high) + dot1(low), packed)
        part[s] = packed

    squares_of(away)
    give = start(remote(part.at[away], part_in, out_send.at[0], out_recv.at[0], {"lev": partner}))
    back = start(remote(outs.at[away], out_any.at[core], out_send.at[1], out_recv.at[1], {"lev": partner}))
    keep = pltpu.make_async_copy(outs.at[core], out_any.at[core], load_sem.at[0])
    keep.start()
    squares_of(core)
    give.wait_recv()
    mine = part[core] + part_in[...]
    mysum[...] = mine
    wide_z = count // deep
    y, z = lon // wide_z, lax.rem(lon, wide_z)
    steps = [(dy, dz) for dy in range(deep) for dz in range(wide_z) if dy or dz]
    steps.sort(key=lambda step: -min(step[0], deep - step[0]) - min(step[1], wide_z - step[1]))
    for i, (dy, dz) in enumerate(steps):
        target = lax.rem(y + dy, deep) * wide_z + lax.rem(z + dz, wide_z)
        slot = lax.rem(count + lon - target - 1, count)
        remote(mysum, sumbuf.at[slot], sum_send, sum_recv, {"lon": target}).start()
    keep.wait()
    back.wait_recv()
    for copy in pending:
        copy.wait_send()
    if steps:
        slots = sumbuf.at[0 : len(steps)]
        pltpu.make_async_copy(slots, slots, sum_send).wait()
        pltpu.make_async_copy(slots, slots, sum_recv).wait()
        mine = mine + jnp.sum(sumbuf[...], axis=0)
    total = mine * (1.0 / (512 * count))
    for j in range(9):
        level = (ORDER + (0,))[j]
        var_ref[level : level + 1, :] = total[j // 2 : j // 2 + 1, S * (j % 2) : S * (j % 2) + S]


def put_out(field_any, sums_any, out_ref, var_ref, sem):
    copies = [
        pltpu.make_async_copy(field_any.at[half], out_ref.at[:, :, pl.ds(256 * half, 256)], sem.at[half])
        for half in range(2)
    ]
    copies.append(pltpu.make_async_copy(sums_any, var_ref, sem.at[2]))
    for copy in copies:
        copy.start()
    for copy in copies:
        copy.wait()


def vmem(count):
    return [pl.BlockSpec(memory_space=pltpu.VMEM)] * count


def local(previous, loss_matrix, pair_matrix, diffusivity, mixing):
    count = lax.axis_size("lon")
    low = lambda *shape: [pltpu.VMEM(shape, BF16)] * 2
    full = lambda *shape: [pltpu.VMEM(shape, F32)]
    sems = lambda *shape: [pltpu.SemaphoreType.DMA(shape)] * 2
    scratch = [pltpu.SMEM((9,), F32)] * 2 + full(9, S, S) + full(2, 9, S, S) + full(9, S, 512) + [pltpu.SemaphoreType.DMA((5,))]
    scratch += full(2, 512, 512) + full(2, 128, 512) + low(2, 512, 512) + low(2, 128, 512) + low(2, 512, 128) + full(96, 128)
    scratch += low(2, 2, 256, 256) + low(2, S, S) + full(512, 640) + full(2, 8, 640)
    scratch += full(8, 96, 128) + low(256, 256) + low(512, 256) + low(256, 256) * 2
    scratch += full(256, S) * 2 + full(S, 256) * 2 + full(256, 256)
    scratch += full(2, 2, 272, 640) + low(2, 256, 512) + full(2, 256, 128) + full(2, 2, 128, 128) + full(2, 3, 128, 128)
    scratch += full(2, 256, 640) + full(2, 9, S, 256) + full(2, 8, 128) + full(8, 128) * 2 + full(max(count - 1, 1), 8, 128)
    scratch += sems(7) + sems(5) + sems(2, 2) + sems(2, 3) + sems(2) + [pltpu.SemaphoreType.DMA] * 2
    shapes = [jax.ShapeDtypeStruct((9, S, 512), F32), jax.ShapeDtypeStruct((9, S), F32)]
    halves = jax.ShapeDtypeStruct((2, 9, S, 256), F32)
    anywhere = [pl.BlockSpec(memory_space=pl.ANY)] * 2
    done = pl.pallas_call(
        functools.partial(kernel, count, 4 if count % 4 == 0 else 1),
        out_shape=[halves, shapes[1]],
        in_specs=[pl.BlockSpec(memory_space=pltpu.HBM)] * 5,
        out_specs=(anywhere[0], vmem(1)[0]),
        scratch_shapes=scratch,
        compiler_params=pltpu.CompilerParams(vmem_limit_bytes=32 * 2**20, collective_id=0, has_side_effects=True),
    )(*[pltpu.with_memory_space_constraint(x, pltpu.HBM) for x in (diffusivity, mixing, loss_matrix, pair_matrix, previous)])
    return tuple(pl.pallas_call(
        put_out,
        out_shape=shapes,
        in_specs=anywhere,
        out_specs=tuple(anywhere),
        scratch_shapes=[pltpu.SemaphoreType.DMA((3,))],
        compiler_params=pltpu.CompilerParams(vmem_limit_bytes=8 * 2**20),
    )(*done))


def solution(mesh):
    placed = (P("lev", None, "lon"), P("lev", None, None), P("lev", None, None), P("lev"), P("lev"))
    return jax.shard_map(
        local,
        mesh=mesh,
        in_specs=placed,
        out_specs=(P("lev", None, "lon"), P("lev", None)),
        check_vma=False,
    )
```

```python
import functools

import jax
import jax.numpy as jnp
from jax import lax
from jax.experimental import pallas as pl
from jax.experimental.pallas import tpu as pltpu
from jax.sharding import PartitionSpec as P

ITERS = 2
F32 = jnp.float32
BF16 = jnp.bfloat16
MESH = pl.DeviceIdType.MESH
HIGHEST = lax.Precision.HIGHEST

S = 64
ORDER = (1, 2, 4, 5, 7, 8, 3, 6)
NN = (((1,), (0,)), ((), ()))
NT = (((1,), (1,)), ((), ()))
TN = (((0,), (0,)), ((), ()))


def split(x):
    high = x.astype(BF16)
    return high, (x - high.astype(F32)).astype(BF16)


def dot3(a, b, dims=NN):
    one = lambda x, y: lax.dot_general(x, y, dims, preferred_element_type=F32)
    return one(a[0], b[0]) + (one(a[0], b[1]) + one(a[1], b[0]))


def mm(a, b, dims=NN):
    return dot3(split(a), split(b), dims)


def mm_full(a, b, dims=NN):
    return lax.dot_general(a, b, dims, precision=HIGHEST, preferred_element_type=F32)


def eye(n):
    rows = lax.broadcasted_iota(jnp.int32, (n, n), 0)
    return (rows == lax.broadcasted_iota(jnp.int32, (n, n), 1)).astype(F32)


def spd_inverses(blocks, lows, high, doublings):
    centres = [0.5 * (high + low) for low in lows]
    units = [eye(block.shape[0]) for block in blocks]
    inverses = [unit * (1.0 / centre) for unit, centre in zip(units, centres)]
    residuals = [unit - block * (1.0 / centre) for unit, block, centre in zip(units, blocks, centres)]
    terms = [(high + low) / (high - low) for low in lows]
    for step in range(doublings):
        last = step == doublings - 1
        for i, unit in enumerate(units):
            twice = 2.0 * terms[i] * terms[i] - 1.0
            gain, shift = (twice + 1.0) / twice, 1.0 / twice
            terms[i] = twice
            centre = centres[i]
            n = unit.shape[0]
            late = step >= doublings - 2
            parts = (lambda x: (x.astype(BF16),)) if late else split
            product = (lambda x, y: lax.dot_general(x[0], y[0], NN, preferred_element_type=F32)) if late else dot3
            rest = parts(residuals[i])
            if step == 0:
                inverses[i] = (inverses[i] + residuals[i] * (1.0 / centre)) * gain
                if not last:
                    residuals[i] = gain * product(rest, rest) - shift * unit
                continue
            known = parts(inverses[i])
            if last:
                inverses[i] = gain * (inverses[i] + product(known, rest))
                continue
            both = product(tuple(jnp.concatenate(p, axis=0) for p in zip(known, rest)), rest)
            inverses[i] = gain * (inverses[i] + both[:n])
            residuals[i] = gain * both[n:] - shift * unit
    exact = [unit - mm_full(block, inverse) for unit, block, inverse in zip(units, blocks, inverses)]
    step = lambda x, y: lax.dot_general(x.astype(BF16), y.astype(BF16), NN, preferred_element_type=F32)
    return [inverse + step(inverse, rest) for inverse, rest in zip(inverses, exact)]


def wide(grid):
    return jnp.concatenate([jnp.concatenate(row, axis=1) if len(row) > 1 else row[0] for row in grid], axis=0)


def interior(link_ref, loss_ref, row_ref, pack_ref):
    one = eye(S)
    zero = jnp.zeros((S, S), F32)
    links = [link_ref[i] for i in range(9)]
    shunt = [loss_ref[i] + one for i in range(9)]
    blocks = []
    for top in (1, 4, 7):
        diag = [shunt[level] + (links[level - 1] + links[level]) * one for level in (top, top + 1)]
        tie = -links[top] * one
        blocks.append(wide([[diag[0], tie], [tie, diag[1]]]))
    pairs = spd_inverses(blocks, [199.0] * 3, 6700.0, 5)
    none = jnp.zeros((S, 128), F32)
    spread = wide([
        [links[2] * pairs[0][S:], links[3] * pairs[1][:S], none],
        [none, links[5] * pairs[1][S:], links[6] * pairs[2][:S]],
    ])
    ground = jnp.concatenate(
        [shunt[1] + links[0] * one, shunt[2], shunt[4], shunt[5], shunt[7], shunt[8] + links[8] * one], axis=0
    )
    own = jnp.concatenate([shunt[3], shunt[6]], axis=0) + mm_full(spread, ground)
    down = links[5] * spread[0:S, 192:256]
    up = links[3] * spread[S:, 128:192]
    middle, = spd_inverses([wide([[own[:S] + down, -down], [-up, own[S:] + up]])], [68.6], 3010.0, 5)
    spread = jnp.concatenate([spread, eye(128)], axis=1)
    lifted = mm(middle, spread)
    lane = lax.broadcasted_iota(jnp.int32, (128, 128), 1)
    ends = mm(jnp.where(lane < S, spread[:, 0:128], spread[:, 256:384]), lifted, TN)
    first = jnp.concatenate([ends[0:S, 0:128] + pairs[0][:S], ends[0:S, 128:512]], axis=1)
    last = jnp.concatenate([ends[S:, 0:256], ends[S:, 256:384] + pairs[2][S:], ends[S:, 384:512]], axis=1)
    rows = jnp.concatenate([links[0] * first, links[8] * last], axis=0)
    row_ref[...] = rows
    loads = mm_full(rows, jnp.concatenate([shunt[level] for level in ORDER], axis=0))
    across = links[8] * rows[0:S, 320:384]
    pack_ref[0:64, :] = jnp.concatenate([shunt[0] + loads[0:S], loads[S:]], axis=1)
    pack_ref[64:96, :] = jnp.concatenate([across[0:32], across[32:64]], axis=1)
    return pairs, spread, lifted


def finish_interior(pairs, spread, lifted, full):
    full[...] = mm(spread, lifted, TN)
    for i in range(3):
        at = slice(128 * i, 128 * i + 128)
        full[at, at] += pairs[i]


def pair_weights(pair_ref, pw_hi, pw_lo, pn_hi, pn_lo):
    for half in range(2):
        row = lax.broadcasted_iota(jnp.int32, (256, 256), 0) // S
        column = lax.broadcasted_iota(jnp.int32, (256, 256), 1) // S
        tall = jnp.concatenate([pair_ref[level] for level in ORDER[4 * half : 4 * half + 4]], axis=0)
        tall = jnp.concatenate([tall, tall], axis=1)
        tall = jnp.where(row == column, jnp.concatenate([tall, tall], axis=1), 0.0)
        pw_hi[half], pw_lo[half] = split(tall)
    pn_hi[...], pn_lo[...] = split(pair_ref[0])


def field_of(prev_ref, field_ref):
    for j in range(4):
        both = jnp.concatenate([prev_ref[ORDER[2 * j]], prev_ref[ORDER[2 * j + 1]]], axis=0)
        field_ref[:, 128 * j : 128 * j + 128] = both.T
    last = jnp.concatenate([prev_ref[0], jnp.zeros_like(prev_ref[0])], axis=0)
    field_ref[:, 512:640] = last.T


def mix_row_of(mix_ref, mixrow_ref):
    lane = lax.broadcasted_iota(jnp.int32, (8, 640), 1) // S
    row = jnp.zeros((8, 640), F32)
    for j, level in enumerate(ORDER + (0,)):
        row = jnp.where(lane == j, mix_ref[level], row)
    mixrow_ref[...] = row


def unpack(packs, q):
    both, folded = packs(q)
    across = jnp.concatenate([folded[:, 0:S], folded[:, S:]], axis=0)
    return both[:, 0:S], both[:, S:], across


def interface(pack_ref, own_hi, own_lo, msg_hi, msg_lo, rlo_hi, rlo_lo, rhi_hi, rhi_lo, wp, wc, rs, rc, own):
    chip = lax.axis_index("lev") // 2
    one = eye(S)
    zero = jnp.zeros((S, S), F32)
    here, below, across = zip(*[
        unpack(lambda q: (pack_ref[q, 0:64, :], pack_ref[q, 64:96, :]), q) for q in range(8)
    ])
    back = [a.T for a in across]
    ground = [here[q] + (below[q - 1] if q else 0.0) for q in range(8)]
    diag = [ground[q] + across[q] + (back[q - 1] if q else 0.0) for q in range(8)]
    upper = wide([
        [diag[0], -across[0], zero, zero],
        [-back[0], diag[1], -across[1], zero],
        [zero, -back[1], diag[2], -across[2]],
        [zero, zero, -back[2], diag[3]],
    ])
    lower = wide([
        [diag[5], -across[5], zero],
        [-back[5], diag[6], -across[6]],
        [zero, -back[6], diag[7]],
    ])
    first = chip < 2
    small = jnp.where(
        first, upper[0:128, 0:128], wide([[500.0 * one, zero], [zero, diag[7]]])
    )
    upper_inverse, lower_inverse, small_inverse = spd_inverses(
        [upper, lower, small], [9.6, 21.0, 13.9], 2400.0, 6
    )
    upper_t = mm(back[3], upper_inverse[192:256, :])
    lower_t = mm(across[4], lower_inverse[0:64, :])
    middle = (
        ground[4]
        + mm_full(upper_t, jnp.concatenate(ground[0:4], axis=0))
        + mm_full(lower_t, jnp.concatenate([ground[5], ground[6], ground[7] + across[7]], axis=0))
    )
    middle_inverse, = spd_inverses([middle], [28.7], 2400.0, 5)
    spread = jnp.concatenate([upper_t, lower_t, one], axis=1)
    lifted = mm(middle_inverse, spread)
    place = {0: 0, 1: 1, 2: 2, 3: 3, 4: 7, 5: 4, 6: 5, 7: 6}
    link = jnp.where(first, back[1], across[6])
    away = mm(link, small_inverse[64:128, :])

    for c in range(4):
        nodes = (2 * c, 2 * c + 1, 2 * c + 1, 2 * c + 2)

        @pl.when(chip == c)
        def _(c=c, nodes=nodes):
            real = [n for n in range(2 * c, 2 * c + 3) if n < 8]
            against = real if 4 in real else real + [4]
            part = lambda x, n: x[:, S * place[n] : S * place[n] + S]
            both = [jnp.concatenate([part(x, n) for n in which], axis=1) for x, which in ((spread, real), (lifted, against))]
            product = mm(both[0], both[1], TN)

            def block(r, k):
                if r not in real or k not in against:
                    return zero
                i, j = real.index(r), against.index(k)
                value = product[S * i : S * i + S, S * j : S * j + S]
                i, j = place[r], place[k]
                if i < 4 and j < 4:
                    value += upper_inverse[S * i : S * i + S, S * j : S * j + S]
                elif 4 <= i < 7 and 4 <= j < 7:
                    value += lower_inverse[S * (i - 4) : S * (i - 3), S * (j - 4) : S * (j - 3)]
                return value

            def blocks(rows, columns):
                return wide([[block(r, k) for k in columns] for r in rows])

            own[...] = blocks(nodes, nodes)
            wc[...] = blocks(nodes, (4,))
            if c in (0, 3):
                far = [away[:, 0:64], away[:, 64:128]]
                if c == 0:
                    rs[...] = jnp.concatenate([far[0], far[1], far[1], one], axis=1)
                    wp[...] = jnp.concatenate([far[0].T, far[1].T, far[1].T, one], axis=0)
                else:
                    rs[...] = jnp.concatenate([one, far[1], far[1], zero], axis=1)
                    wp[...] = jnp.concatenate([one, far[1].T, far[1].T, zero], axis=0)
            else:
                gate = 2 if c == 1 else 6
                rs[...] = blocks((gate,), nodes)
                wp[...] = blocks(nodes, (gate,))

            def seen(n):
                if n > 7:
                    return zero
                n = place[n]
                return spread[:, S * n : S * n + S]

            rc[...] = jnp.concatenate([seen(n) for n in nodes], axis=1)

    own_hi[...], own_lo[...] = split(own[...])
    none = jnp.zeros((256, S), F32)
    msg = wide([[wp[...], none, wc[...], none], [none, wp[...], none, wc[...]]])
    msg_hi[...], msg_lo[...] = split(msg)
    none = jnp.zeros((S, 256), F32)
    rlo_hi[...], rlo_lo[...] = split(jnp.concatenate([rs[...], none, rc[...], none], axis=0))
    rhi_hi[...], rhi_lo[...] = split(jnp.concatenate([none, rs[...], none, rc[...]], axis=0))


def kernel(count, deep, link_hbm, mix_hbm, loss_hbm, pair_hbm, prev_hbm, out_any, var_ref,
           link_ref, mix_ref, loss_ref, pair_ref, prev_ref, load_sem,
           full, row, g_hi, g_lo, hr_hi, hr_lo, hc_hi, hc_lo, pack, pw_hi, pw_lo, pn_hi, pn_lo, field, mixrow,
           packs, own_hi, own_lo, msg_hi, msg_lo, rlo_hi, rlo_lo, rhi_hi, rhi_lo, wp, wc, rs, rc, own,
           state, gs_hi, gs_lo, injs, outgo, incoming, sums, outs, ends_ref, part, part_in, mysum, sumbuf,
           pack_send, pack_recv, give_send, give_recv, halo_send, halo_recv, msg_send, msg_recv, out_send, out_recv,
           sum_send, sum_recv):
    lev = lax.axis_index("lev")
    lon = lax.axis_index("lon")
    core = lax.rem(lev, 2)
    chip = lev // 2
    partner = lev + 1 - 2 * core
    base = lev - core
    sibling = 2 * (chip + 1 - 2 * lax.rem(chip, 2)) + core
    across_base = 2 - 2 * (chip // 2)
    far = lax.rem(chip + 2, 4)
    across = [2 * far + core, 2 * (2 * across_base + 1 - far) + core]
    west, east = lax.rem(lon + count - 1, count), lax.rem(lon + 1, count)
    loads = [
        pltpu.make_async_copy(src, dst, load_sem.at[i])
        for i, (src, dst) in enumerate([
            (link_hbm, link_ref), (loss_hbm, loss_ref), (prev_hbm, prev_ref), (pair_hbm, pair_ref.at[core]), (mix_hbm, mix_ref),
        ])
    ]
    for load in loads:
        load.start()
    barrier = pltpu.get_barrier_semaphore()
    others = [lax.rem(lev + d, 8) for d in range(1, 8)]
    for other in others:
        pl.semaphore_signal(barrier, inc=1, device_id={"lev": other}, device_id_type=MESH)
    for side in (west, east):
        pl.semaphore_signal(barrier, inc=1, device_id={"lev": partner, "lon": side}, device_id_type=MESH)

    def greet(d, carry):
        pl.semaphore_signal(barrier, inc=1, device_id={"lon": lax.rem(lon + d, count)}, device_id_type=MESH)
        return carry

    lax.fori_loop(1, count, greet, 0)

    def remote(src, dst, send, recv, where):
        return pltpu.make_async_remote_copy(
            src_ref=src, dst_ref=dst, send_sem=send, recv_sem=recv, device_id=where, device_id_type=MESH
        )

    def rows_at(start, size):
        return pl.ds(pl.multiple_of(start, 8), size)

    pending = []

    def start(copy):
        copy.start()
        pending.append(copy)
        return copy

    loads[0].wait()
    loads[1].wait()
    parts = interior(link_ref, loss_ref, row.at[core], pack)
    loads[3].wait()
    loads[4].wait()
    mix_row_of(mix_ref, mixrow.at[core])
    pl.semaphore_wait(barrier, 8 + count)
    packs[lev] = pack[...]
    spread = [
        start(remote(pack, packs.at[lev], pack_send.at[i], pack_recv.at[i], {"lev": target}))
        for i, target in enumerate([2 * lax.rem(chip + d, 4) + core for d in (2, 1, 3)] + [partner])
    ]
    loads[2].wait()
    field_of(prev_ref, field)

    def hand_on(i, d):
        spread[i].wait_recv()
        source = 2 * lax.rem(chip + 4 - d, 4) + core
        return start(remote(packs.at[source], packs.at[source], pack_send.at[4 + i], pack_recv.at[4 + i], {"lev": partner}))

    away = 1 - core
    gives = [
        start(remote(src, dst, give_send.at[i], give_recv.at[i], {"lev": partner}))
        for i, (src, dst) in enumerate([
            (field.at[rows_at(248 * away, 264)], state.at[0, core, rows_at(8 * core, 264)]),
            (pair_ref.at[core], pair_ref.at[core]),
            (mixrow.at[core], mixrow.at[core]),
            (row.at[core], row.at[core]),
        ])
    ]
    outer = [
        start(remote(field.at[0:8], state.at[0, core, 264:272], halo_send.at[0, 0], halo_recv.at[0, core],
                     {"lev": base + 1, "lon": west})),
        start(remote(field.at[504:512], state.at[0, core, 0:8], halo_send.at[0, 1], halo_recv.at[0, core],
                     {"lev": base, "lon": east})),
    ]
    state[0, core, rows_at(8 * away, 264), :] = field[rows_at(248 * core, 264), :]
    finish_interior(*parts, full.at[core])

    def pair_term(it, s):
        for r in range(0, 256, 128):
            here = state[it, s, 8 + r : 136 + r, :]
            squares = split(here * here)
            for half in range(2):
                piece = tuple(x[:, 256 * half : 256 * half + 256] for x in squares)
                sums[s, r : r + 128, 256 * half : 256 * half + 256] = dot3(piece, (pw_hi[s, half], pw_lo[s, half]), NT)
            piece = tuple(x[:, 512:576] for x in squares)
            sums[s, r : r + 128, 512:576] = dot3(piece, (pn_hi[s], pn_lo[s]), NT)

    def forcing_term(it, s, chunks=((0, 128), (128, 128))):
        for r, n in chunks:
            here = state[it, s, 8 + r : 8 + r + n, 0:576]
            around = state[it, s, 7 + r : 7 + r + n, 0:576] + state[it, s, 9 + r : 9 + r + n, 0:576]
            forcing = state[0, s, 8 + r : 8 + r + n, 0:576] - sums[s, r : r + n, 0:576]
            forcing += mixrow[s, 0:1, 0:576] * (around - 2.0 * here)
            pieces = split(forcing[:, 0:512])
            gs_hi[s, r : r + n, :], gs_lo[s, r : r + n, :] = pieces
            node = forcing[:, 512:576]
            push = dot3(pieces, (hr_hi[s], hr_lo[s]), NT)
            injs[s, r : r + n, :] = push + jnp.concatenate([node, jnp.zeros_like(node)], axis=1)

    def weights(s):
        pair_weights(pair_ref.at[s], pw_hi.at[s], pw_lo.at[s], pn_hi.at[s], pn_lo.at[s])
        hr_hi[s], hr_lo[s] = split(row[s])

    def product(it, s):
        if it == ITERS - 1:
            for b in range(4):
                rows = slice(128 * b, 128 * b + 128)
                value = dot3((g_hi[s, rows, :], g_lo[s, rows, :]), (gs_hi[s], gs_lo[s]), NT)
                for h in range(2):
                    outs[s, ORDER[2 * b + h]] = value[64 * h : 64 * h + 64]
        else:
            for r in range(0, 256, 128):
                pieces = (gs_hi[s, r : r + 128, :], gs_lo[s, r : r + 128, :])
                state[it + 1, s, 8 + r : 136 + r, 0:512] = dot3(pieces, (g_hi[s], g_lo[s]))

    middle, edges = ((16, 112), (128, 112)), ((0, 16), (240, 16))
    weights(core)
    pair_term(0, core)
    forcing_term(0, core, middle)
    for give in gives:
        give.wait_recv()
    weights(away)
    handed = [hand_on(1, 1), hand_on(2, 3)]
    pair_term(0, away)
    forcing_term(0, away, middle)
    handed.append(hand_on(0, 2))
    give_full = start(remote(full.at[core], full.at[core], give_send.at[4], give_recv.at[4], {"lev": partner}))
    for slot in range(2):
        pltpu.make_async_copy(field.at[0:8], state.at[0, 0, 0:8], halo_recv.at[0, slot]).wait()
    for s in range(2):
        forcing_term(0, s, edges)
    for copy in [spread[3]] + handed:
        copy.wait_recv()
    interface(packs, own_hi, own_lo, msg_hi, msg_lo, rlo_hi, rlo_lo, rhi_hi, rhi_lo, wp, wc, rs, rc, own)
    for it in range(ITERS):
        final = it == ITERS - 1
        if it:
            for s in range(2):
                pair_term(it, s)
            for s in range(2):
                forcing_term(it, s, middle)
            for halo in halos:
                halo.wait_recv()
            for s in range(2):
                forcing_term(it, s, edges)
        inj = jnp.concatenate([injs[0], injs[1]], axis=1)
        packed = split(jnp.concatenate([inj[0:128], inj[128:256]], axis=1))
        message = dot3(packed, (msg_hi[...], msg_lo[...]))
        outgo[it, 0] = message[:, 0:128]
        outgo[it, 1] = message[:, 128:256]
        slot = 1 + lax.rem(chip, 2)
        start(remote(outgo.at[it, 1], incoming.at[it, slot], msg_send.at[it, 1], msg_recv.at[it, slot], {"lev": across[0]}))
        start(remote(outgo.at[it, 1], incoming.at[it, slot], msg_send.at[it, 2], msg_recv.at[it, slot], {"lev": across[1]}))
        start(remote(outgo.at[it, 0], incoming.at[it, 0], msg_send.at[it, 0], msg_recv.at[it, 0], {"lev": sibling}))
        mine = dot3(split(inj), (own_hi[...], own_lo[...]))
        if it == 0:
            give_full.wait_recv()
            for s in range(2):
                g_hi[s], g_lo[s] = split(full[s])
                hc_hi[s], hc_lo[s] = split(row[s].T)
        for s in range(2):
            product(it, s)
        for slot in range(3):
            pltpu.make_async_copy(outgo.at[it, 0], incoming.at[it, slot], msg_recv.at[it, slot]).wait()
        heard = split(jnp.concatenate([incoming[it, 0], incoming[it, 1] + incoming[it, 2]], axis=1))
        total = mine + jnp.concatenate(
            [dot3(heard, (rlo_hi[...], rlo_lo[...])), dot3(heard, (rhi_hi[...], rhi_lo[...]))], axis=0
        )
        total_of = [total[:, 128 * s : 128 * s + 128] for s in range(2)]
        if not final:
            def land(s, low, high):
                ends = total_of[s][low:high]
                rows = slice(8 + low, 8 + high)
                state[it + 1, s, rows, 0:512] += dot3(split(ends), (hr_hi[s], hr_lo[s]))
                state[it + 1, s, rows, 512:640] = jnp.where(
                    lax.broadcasted_iota(jnp.int32, (high - low, 128), 1) < S, ends, 0.0
                )

            for s in range(2):
                land(s, 0, 16)
                land(s, 240, 256)
            inner_from, inner_to = 8 + 248 * away, 264 * core
            outer_from, outer_to = 8 + 248 * core, 264 * away
            halos = [
                start(remote(state.at[it + 1, :, rows_at(a, 8), :], state.at[it + 1, :, rows_at(b, 8), :],
                             halo_send.at[it + 1, i], halo_recv.at[it + 1, i], where))
                for i, (a, b, where) in enumerate([
                    (outer_from, outer_to, {"lev": partner, "lon": west + (east - west) * core}),
                    (inner_from, inner_to, {"lev": partner}),
                ])
            ]
            for s in range(2):
                land(s, 16, 240)
            continue
    ones = jnp.ones((8, 256), BF16)
    dot1 = lambda x: lax.dot_general(ones, x, NT, preferred_element_type=F32)
    line = lax.broadcasted_iota(jnp.int32, (8, 128), 0)

    ends_ref[0], ends_ref[1] = total_of

    def last_values(s):
        pieces = split(ends_ref[s])
        for b in range(4):
            rows = slice(128 * b, 128 * b + 128)
            value = dot3((hc_hi[s, rows, :], hc_lo[s, rows, :]), pieces, NT)
            for h in range(2):
                outs[s, ORDER[2 * b + h]] += value[64 * h : 64 * h + 64]
        outs[s, 0] = ends_ref[s].T[0:64]

    def squares_of(s):
        packed = jnp.zeros((8, 128), F32)
        for j in range(5):
            values = [outs[s, level] for level in ((ORDER + (0,))[2 * j : 2 * j + 2])]
            values = jnp.concatenate(values if j < 4 else values + [jnp.zeros_like(values[0])], axis=0)
            high, low = split(values * values)
            packed = jnp.where(line == j, dot1(high) + dot1(low), packed)
        part[s] = packed

    last_values(away)
    squares_of(away)
    give = start(remote(part.at[away], part_in, out_send.at[0], out_recv.at[0], {"lev": partner}))
    back = start(remote(outs.at[away], out_any.at[core], out_send.at[1], out_recv.at[1], {"lev": partner}))
    last_values(core)
    keep = pltpu.make_async_copy(outs.at[core], out_any.at[core], load_sem.at[0])
    keep.start()
    squares_of(core)
    give.wait_recv()
    mine = part[core] + part_in[...]
    mysum[...] = mine
    wide_z = count // deep
    y, z = lon // wide_z, lax.rem(lon, wide_z)
    steps = [(dy, dz) for dy in range(deep) for dz in range(wide_z) if dy or dz]
    steps.sort(key=lambda step: -min(step[0], deep - step[0]) - min(step[1], wide_z - step[1]))
    for i, (dy, dz) in enumerate(steps):
        target = lax.rem(y + dy, deep) * wide_z + lax.rem(z + dz, wide_z)
        slot = lax.rem(count + lon - target - 1, count)
        remote(mysum.at[0:5], sumbuf.at[slot, 0:5], sum_send, sum_recv, {"lon": target}).start()
    keep.wait()
    back.wait_recv()
    for copy in pending:
        copy.wait_send()
    if steps:
        slots = sumbuf.at[0 : len(steps), 0:5]
        pltpu.make_async_copy(slots, slots, sum_send).wait()
        pltpu.make_async_copy(slots, slots, sum_recv).wait()
        mine = mine[0:5] + jnp.sum(sumbuf[:, 0:5], axis=0)
    total = mine * (1.0 / (512 * count))
    for j in range(9):
        level = (ORDER + (0,))[j]
        var_ref[level : level + 1, :] = total[j // 2 : j // 2 + 1, S * (j % 2) : S * (j % 2) + S]


def put_out(field_any, sums_any, out_ref, var_ref, sem):
    copies = [
        pltpu.make_async_copy(
            field_any.at[half, pl.ds(level, 3)], out_ref.at[pl.ds(level, 3), :, pl.ds(256 * half, 256)], sem.at[3 * half + level // 3]
        )
        for half in range(2)
        for level in (0, 3, 6)
    ]
    copies.append(pltpu.make_async_copy(sums_any, var_ref, sem.at[6]))
    for copy in copies:
        copy.start()
    for copy in copies:
        copy.wait()


def vmem(count):
    return [pl.BlockSpec(memory_space=pltpu.VMEM)] * count


def local(previous, loss_matrix, pair_matrix, diffusivity, mixing):
    count = lax.axis_size("lon")
    low = lambda *shape: [pltpu.VMEM(shape, BF16)] * 2
    full = lambda *shape: [pltpu.VMEM(shape, F32)]
    sems = lambda *shape: [pltpu.SemaphoreType.DMA(shape)] * 2
    scratch = [pltpu.SMEM((9,), F32)] * 2 + full(9, S, S) + full(2, 9, S, S) + full(9, S, 512) + [pltpu.SemaphoreType.DMA((5,))]
    scratch += full(2, 512, 512) + full(2, 128, 512) + low(2, 512, 512) + low(2, 128, 512) + low(2, 512, 128) + full(96, 128)
    scratch += low(2, 2, 256, 256) + low(2, S, S) + full(512, 640) + full(2, 8, 640)
    scratch += full(8, 96, 128) + low(256, 256) + low(512, 256) + low(256, 256) * 2
    scratch += full(256, S) * 2 + full(S, 256) * 2 + full(256, 256)
    scratch += full(2, 2, 272, 640) + low(2, 256, 512) + full(2, 256, 128) + full(2, 2, 128, 128) + full(2, 3, 128, 128)
    scratch += full(2, 256, 640) + full(2, 9, S, 256) + full(2, 256, 128) + full(2, 8, 128) + full(8, 128) * 2 + full(max(count - 1, 1), 8, 128)
    scratch += sems(7) + sems(5) + sems(2, 2) + sems(2, 3) + sems(2) + [pltpu.SemaphoreType.DMA] * 2
    shapes = [jax.ShapeDtypeStruct((9, S, 512), F32), jax.ShapeDtypeStruct((9, S), F32)]
    halves = jax.ShapeDtypeStruct((2, 9, S, 256), F32)
    anywhere = [pl.BlockSpec(memory_space=pl.ANY)] * 2
    done = pl.pallas_call(
        functools.partial(kernel, count, 4 if count % 4 == 0 else 1),
        out_shape=[halves, shapes[1]],
        in_specs=[pl.BlockSpec(memory_space=pltpu.HBM)] * 5,
        out_specs=(anywhere[0], vmem(1)[0]),
        scratch_shapes=scratch,
        compiler_params=pltpu.CompilerParams(vmem_limit_bytes=32 * 2**20, collective_id=0, has_side_effects=True),
    )(*[pltpu.with_memory_space_constraint(x, pltpu.HBM) for x in (diffusivity, mixing, loss_matrix, pair_matrix, previous)])
    return tuple(pl.pallas_call(
        put_out,
        out_shape=shapes,
        in_specs=anywhere,
        out_specs=tuple(anywhere),
        scratch_shapes=[pltpu.SemaphoreType.DMA((7,))],
        compiler_params=pltpu.CompilerParams(vmem_limit_bytes=8 * 2**20),
    )(*done))


def solution(mesh):
    placed = (P("lev", None, "lon"), P("lev", None, None), P("lev", None, None), P("lev"), P("lev"))
    return jax.shard_map(
        local,
        mesh=mesh,
        in_specs=placed,
        out_specs=(P("lev", None, "lon"), P("lev", None)),
        check_vma=False,
    )
```

```python
import functools

import jax
import jax.numpy as jnp
from jax import lax
from jax.experimental import pallas as pl
from jax.experimental.pallas import tpu as pltpu
from jax.sharding import PartitionSpec as P

ITERS = 2
F32 = jnp.float32
BF16 = jnp.bfloat16
MESH = pl.DeviceIdType.MESH

S = 64
ORDER = (1, 2, 4, 5, 7, 8, 3, 6)
NN = (((1,), (0,)), ((), ()))
NT = (((1,), (1,)), ((), ()))
TN = (((0,), (0,)), ((), ()))


def split(x):
    high = x.astype(BF16)
    return high, (x - high.astype(F32)).astype(BF16)


def dot3(a, b, dims=NN):
    one = lambda x, y: lax.dot_general(x, y, dims, preferred_element_type=F32)
    return one(a[0], b[0]) + (one(a[0], b[1]) + one(a[1], b[0]))


def mm(a, b, dims=NN):
    return dot3(split(a), split(b), dims)


def eye(n):
    rows = lax.broadcasted_iota(jnp.int32, (n, n), 0)
    return (rows == lax.broadcasted_iota(jnp.int32, (n, n), 1)).astype(F32)


def spd_inverses(blocks, lows, high, doublings):
    centres = [0.5 * (high + low) for low in lows]
    units = [eye(block.shape[0]) for block in blocks]
    inverses = [unit * (1.0 / centre) for unit, centre in zip(units, centres)]
    residuals = [unit - block * (1.0 / centre) for unit, block, centre in zip(units, blocks, centres)]
    terms = [(high + low) / (high - low) for low in lows]
    for step in range(doublings):
        last = step == doublings - 1
        for i, unit in enumerate(units):
            twice = 2.0 * terms[i] * terms[i] - 1.0
            gain, shift = (twice + 1.0) / twice, 1.0 / twice
            terms[i] = twice
            centre = centres[i]
            n = unit.shape[0]
            late = step >= doublings - 2
            parts = (lambda x: (x.astype(BF16),)) if late else split
            product = (lambda x, y: lax.dot_general(x[0], y[0], NN, preferred_element_type=F32)) if late else dot3
            rest = parts(residuals[i])
            if step == 0:
                inverses[i] = (inverses[i] + residuals[i] * (1.0 / centre)) * gain
                if not last:
                    residuals[i] = gain * product(rest, rest) - shift * unit
                continue
            known = parts(inverses[i])
            if last:
                inverses[i] = gain * (inverses[i] + product(known, rest))
                continue
            both = product(tuple(jnp.concatenate(p, axis=0) for p in zip(known, rest)), rest)
            inverses[i] = gain * (inverses[i] + both[:n])
            residuals[i] = gain * both[n:] - shift * unit
    exact = [unit - mm(block, inverse) for unit, block, inverse in zip(units, blocks, inverses)]
    step = lambda x, y: lax.dot_general(x.astype(BF16), y.astype(BF16), NN, preferred_element_type=F32)
    return [inverse + step(inverse, rest) for inverse, rest in zip(inverses, exact)]


def wide(grid):
    return jnp.concatenate([jnp.concatenate(row, axis=1) if len(row) > 1 else row[0] for row in grid], axis=0)


def interior(link_ref, loss_ref, pack_ref):
    one = eye(S)
    zero = jnp.zeros((S, S), F32)
    links = [link_ref[i] for i in range(9)]
    shunt = [loss_ref[i] + one for i in range(9)]
    blocks = []
    for top in (1, 4, 7):
        diag = [shunt[level] + (links[level - 1] + links[level]) * one for level in (top, top + 1)]
        tie = -links[top] * one
        blocks.append(wide([[diag[0], tie], [tie, diag[1]]]))
    pairs = spd_inverses(blocks, [199.0] * 3, 6700.0, 5)
    none = jnp.zeros((S, 128), F32)
    spread = wide([
        [links[2] * pairs[0][S:], links[3] * pairs[1][:S], none],
        [none, links[5] * pairs[1][S:], links[6] * pairs[2][:S]],
    ])
    ground = jnp.concatenate(
        [shunt[1] + links[0] * one, shunt[2], shunt[4], shunt[5], shunt[7], shunt[8] + links[8] * one], axis=0
    )
    own = jnp.concatenate([shunt[3], shunt[6]], axis=0) + mm(spread, ground)
    down = links[5] * spread[0:S, 192:256]
    up = links[3] * spread[S:, 128:192]
    lane = lax.broadcasted_iota(jnp.int32, (128, 128), 1)
    ends = jnp.where(lane < S, spread[:, 0:128], spread[:, 256:384])
    stack = jnp.concatenate([shunt[level] for level in ORDER], axis=0)
    through = mm(spread, stack[0:384]) + stack[384:512]
    direct = [mm(pairs[0][:S], stack[0:128]), mm(pairs[2][S:], stack[256:384])]
    middle, = spd_inverses([wide([[own[:S] + down, -down], [-up, own[S:] + up]])], [68.6], 3010.0, 5)
    seen = mm(ends, middle, TN)
    loads = mm(seen, through)
    across = (links[0] * links[8]) * mm(seen[0:S], spread)[:, 320:384]
    pack_ref[0:64, :] = jnp.concatenate(
        [shunt[0] + links[0] * (loads[0:S] + direct[0]), links[8] * (loads[S:] + direct[1])], axis=1
    )
    pack_ref[64:96, :] = jnp.concatenate([across[0:32], across[32:64]], axis=1)
    return pairs, jnp.concatenate([spread, eye(128)], axis=1), middle, seen


def end_rows(link_ref, row_ref, pairs, spread, middle, seen):
    ends = mm(seen, spread)
    first = jnp.concatenate([ends[0:S, 0:128] + pairs[0][:S], ends[0:S, 128:512]], axis=1)
    last = jnp.concatenate([ends[S:, 0:256], ends[S:, 256:384] + pairs[2][S:], ends[S:, 384:512]], axis=1)
    row_ref[...] = jnp.concatenate([link_ref[0] * first, link_ref[8] * last], axis=0)


def finish_interior(full, pairs, spread, middle, seen):
    full[...] = mm(spread, mm(middle, spread), TN)
    for i in range(3):
        at = slice(128 * i, 128 * i + 128)
        full[at, at] += pairs[i]


def pair_weights(pair_ref, pw_hi, pw_lo, pn_hi, pn_lo):
    for half in range(2):
        row = lax.broadcasted_iota(jnp.int32, (256, 256), 0) // S
        column = lax.broadcasted_iota(jnp.int32, (256, 256), 1) // S
        tall = jnp.concatenate([pair_ref[level] for level in ORDER[4 * half : 4 * half + 4]], axis=0)
        tall = jnp.concatenate([tall, tall], axis=1)
        tall = jnp.where(row == column, jnp.concatenate([tall, tall], axis=1), 0.0)
        pw_hi[half], pw_lo[half] = split(tall)
    pn_hi[...], pn_lo[...] = split(pair_ref[0])


def field_of(prev_ref, field_ref):
    for j in range(4):
        both = jnp.concatenate([prev_ref[ORDER[2 * j]], prev_ref[ORDER[2 * j + 1]]], axis=0)
        field_ref[:, 128 * j : 128 * j + 128] = both.T
    last = jnp.concatenate([prev_ref[0], jnp.zeros_like(prev_ref[0])], axis=0)
    field_ref[:, 512:640] = last.T


def mix_row_of(mix_ref, mixrow_ref):
    lane = lax.broadcasted_iota(jnp.int32, (8, 640), 1) // S
    row = jnp.zeros((8, 640), F32)
    for j, level in enumerate(ORDER + (0,)):
        row = jnp.where(lane == j, mix_ref[level], row)
    mixrow_ref[...] = row


def unpack(packs, q):
    both, folded = packs(q)
    across = jnp.concatenate([folded[:, 0:S], folded[:, S:]], axis=0)
    return both[:, 0:S], both[:, S:], across


def interface(pack_ref, own_hi, own_lo, msg_hi, msg_lo, rlo_hi, rlo_lo, rhi_hi, rhi_lo, wp, wc, rs, rc, own):
    chip = lax.axis_index("lev") // 2
    one = eye(S)
    zero = jnp.zeros((S, S), F32)
    here, below, across = zip(*[
        unpack(lambda q: (pack_ref[q, 0:64, :], pack_ref[q, 64:96, :]), q) for q in range(8)
    ])
    back = [a.T for a in across]
    ground = [here[q] + (below[q - 1] if q else 0.0) for q in range(8)]
    diag = [ground[q] + across[q] + (back[q - 1] if q else 0.0) for q in range(8)]
    upper = wide([
        [diag[0], -across[0], zero, zero],
        [-back[0], diag[1], -across[1], zero],
        [zero, -back[1], diag[2], -across[2]],
        [zero, zero, -back[2], diag[3]],
    ])
    lower = wide([
        [diag[5], -across[5], zero],
        [-back[5], diag[6], -across[6]],
        [zero, -back[6], diag[7]],
    ])
    first = chip < 2
    small = jnp.where(
        first, upper[0:128, 0:128], wide([[500.0 * one, zero], [zero, diag[7]]])
    )
    upper_inverse, lower_inverse, small_inverse = spd_inverses(
        [upper, lower, small], [9.6, 21.0, 13.9], 2400.0, 6
    )
    upper_t = mm(back[3], upper_inverse[192:256, :])
    lower_t = mm(across[4], lower_inverse[0:64, :])
    middle = (
        ground[4]
        + mm(upper_t, jnp.concatenate(ground[0:4], axis=0))
        + mm(lower_t, jnp.concatenate([ground[5], ground[6], ground[7] + across[7]], axis=0))
    )
    middle_inverse, = spd_inverses([middle], [28.7], 2400.0, 5)
    spread = jnp.concatenate([upper_t, lower_t, one], axis=1)
    lifted = mm(middle_inverse, spread)
    place = {0: 0, 1: 1, 2: 2, 3: 3, 4: 7, 5: 4, 6: 5, 7: 6}
    link = jnp.where(first, back[1], across[6])
    away = mm(link, small_inverse[64:128, :])

    for c in range(4):
        nodes = (2 * c, 2 * c + 1, 2 * c + 1, 2 * c + 2)

        @pl.when(chip == c)
        def _(c=c, nodes=nodes):
            real = [n for n in range(2 * c, 2 * c + 3) if n < 8]
            against = real if 4 in real else real + [4]
            part = lambda x, n: x[:, S * place[n] : S * place[n] + S]
            both = [jnp.concatenate([part(x, n) for n in which], axis=1) for x, which in ((spread, real), (lifted, against))]
            product = mm(both[0], both[1], TN)

            def block(r, k):
                if r not in real or k not in against:
                    return zero
                i, j = real.index(r), against.index(k)
                value = product[S * i : S * i + S, S * j : S * j + S]
                i, j = place[r], place[k]
                if i < 4 and j < 4:
                    value += upper_inverse[S * i : S * i + S, S * j : S * j + S]
                elif 4 <= i < 7 and 4 <= j < 7:
                    value += lower_inverse[S * (i - 4) : S * (i - 3), S * (j - 4) : S * (j - 3)]
                return value

            def blocks(rows, columns):
                return wide([[block(r, k) for k in columns] for r in rows])

            own[...] = blocks(nodes, nodes)
            wc[...] = blocks(nodes, (4,))
            if c in (0, 3):
                far = [away[:, 0:64], away[:, 64:128]]
                if c == 0:
                    rs[...] = jnp.concatenate([far[0], far[1], far[1], one], axis=1)
                    wp[...] = jnp.concatenate([far[0].T, far[1].T, far[1].T, one], axis=0)
                else:
                    rs[...] = jnp.concatenate([one, far[1], far[1], zero], axis=1)
                    wp[...] = jnp.concatenate([one, far[1].T, far[1].T, zero], axis=0)
            else:
                gate = 2 if c == 1 else 6
                rs[...] = blocks((gate,), nodes)
                wp[...] = blocks(nodes, (gate,))

            def seen(n):
                if n > 7:
                    return zero
                n = place[n]
                return spread[:, S * n : S * n + S]

            rc[...] = jnp.concatenate([seen(n) for n in nodes], axis=1)

    own_hi[...], own_lo[...] = split(own[...])
    none = jnp.zeros((256, S), F32)
    msg = wide([[wp[...], none, wc[...], none], [none, wp[...], none, wc[...]]])
    msg_hi[...], msg_lo[...] = split(msg)
    none = jnp.zeros((S, 256), F32)
    rlo_hi[...], rlo_lo[...] = split(jnp.concatenate([rs[...], none, rc[...], none], axis=0))
    rhi_hi[...], rhi_lo[...] = split(jnp.concatenate([none, rs[...], none, rc[...]], axis=0))


def kernel(count, deep, link_hbm, mix_hbm, loss_hbm, pair_hbm, prev_hbm, out_any, var_ref,
           link_ref, mix_ref, loss_ref, pair_ref, prev_ref, load_sem,
           full, row, g_hi, g_lo, hr_hi, hr_lo, hc_hi, hc_lo, pack, pw_hi, pw_lo, pn_hi, pn_lo, field, mixrow,
           packs, own_hi, own_lo, msg_hi, msg_lo, rlo_hi, rlo_lo, rhi_hi, rhi_lo, wp, wc, rs, rc, own,
           state, gs_hi, gs_lo, injs, outgo, incoming, out_most, in_most, out_edge, in_edge, sums, outs, ends_ref, part, part_in, mysum, sumbuf,
           pack_send, pack_recv, give_send, give_recv, halo_send, halo_recv, msg_send, msg_recv, out_send, out_recv,
           sum_send, sum_recv):
    lev = lax.axis_index("lev")
    lon = lax.axis_index("lon")
    core = lax.rem(lev, 2)
    chip = lev // 2
    partner = lev + 1 - 2 * core
    base = lev - core
    sibling = 2 * (chip + 1 - 2 * lax.rem(chip, 2)) + core
    across_base = 2 - 2 * (chip // 2)
    far = lax.rem(chip + 2, 4)
    across = [2 * far + core, 2 * (2 * across_base + 1 - far) + core]
    west, east = lax.rem(lon + count - 1, count), lax.rem(lon + 1, count)
    loads = [
        pltpu.make_async_copy(src, dst, load_sem.at[i])
        for i, (src, dst) in enumerate([
            (link_hbm, link_ref), (loss_hbm, loss_ref), (prev_hbm, prev_ref), (pair_hbm, pair_ref.at[core]), (mix_hbm, mix_ref),
        ])
    ]
    for load in loads:
        load.start()
    barrier = pltpu.get_barrier_semaphore()
    others = [lax.rem(lev + d, 8) for d in range(1, 8)]
    for other in others:
        pl.semaphore_signal(barrier, inc=1, device_id={"lev": other}, device_id_type=MESH)
    for side in (west, east):
        pl.semaphore_signal(barrier, inc=1, device_id={"lev": partner, "lon": side}, device_id_type=MESH)

    def greet(d, carry):
        pl.semaphore_signal(barrier, inc=1, device_id={"lon": lax.rem(lon + d, count)}, device_id_type=MESH)
        return carry

    lax.fori_loop(1, count, greet, 0)

    def remote(src, dst, send, recv, where):
        return pltpu.make_async_remote_copy(
            src_ref=src, dst_ref=dst, send_sem=send, recv_sem=recv, device_id=where, device_id_type=MESH
        )

    def rows_at(start, size):
        return pl.ds(pl.multiple_of(start, 8), size)

    pending = []

    def start(copy):
        copy.start()
        pending.append(copy)
        return copy

    loads[0].wait()
    loads[1].wait()
    parts = interior(link_ref, loss_ref, pack)
    loads[3].wait()
    loads[4].wait()
    mix_row_of(mix_ref, mixrow.at[core])
    pl.semaphore_wait(barrier, 8 + count)
    packs[lev] = pack[...]
    spread = [
        start(remote(pack, packs.at[lev], pack_send.at[i], pack_recv.at[i], {"lev": target}))
        for i, target in enumerate([2 * lax.rem(chip + d, 4) + core for d in (2, 1, 3)] + [partner])
    ]
    end_rows(link_ref, row.at[core], *parts)
    loads[2].wait()
    field_of(prev_ref, field)

    def hand_on(i, d):
        spread[i].wait_recv()
        source = 2 * lax.rem(chip + 4 - d, 4) + core
        return start(remote(packs.at[source], packs.at[source], pack_send.at[4 + i], pack_recv.at[4 + i], {"lev": partner}))

    away = 1 - core
    gives = [
        start(remote(src, dst, give_send.at[i], give_recv.at[i], {"lev": partner}))
        for i, (src, dst) in enumerate([
            (field.at[rows_at(248 * away, 264)], state.at[0, core, rows_at(8 * core, 264)]),
            (pair_ref.at[core], pair_ref.at[core]),
            (mixrow.at[core], mixrow.at[core]),
            (row.at[core], row.at[core]),
        ])
    ]
    outer = [
        start(remote(field.at[0:8], state.at[0, core, 264:272], halo_send.at[0, 0], halo_recv.at[0, core],
                     {"lev": base + 1, "lon": west})),
        start(remote(field.at[504:512], state.at[0, core, 0:8], halo_send.at[0, 1], halo_recv.at[0, core],
                     {"lev": base, "lon": east})),
    ]
    state[0, core, rows_at(8 * away, 264), :] = field[rows_at(248 * core, 264), :]
    finish_interior(full.at[core], *parts)

    def pair_term(it, s):
        here = state[it, s, 8:264, :]
        squares = split(here * here)
        for half in range(2):
            piece = tuple(x[:, 256 * half : 256 * half + 256] for x in squares)
            sums[s, :, 256 * half : 256 * half + 256] = dot3(piece, (pw_hi[s, half], pw_lo[s, half]), NT)
        piece = tuple(x[:, 512:576] for x in squares)
        sums[s, :, 512:576] = dot3(piece, (pn_hi[s], pn_lo[s]), NT)

    def forcing_term(it, s, chunks):
        forcing = []
        for r, n in chunks:
            here = state[it, s, 8 + r : 8 + r + n, 0:576]
            around = state[it, s, 7 + r : 7 + r + n, 0:576] + state[it, s, 9 + r : 9 + r + n, 0:576]
            value = state[0, s, 8 + r : 8 + r + n, 0:576] - sums[s, r : r + n, 0:576]
            forcing.append(value + mixrow[s, 0:1, 0:576] * (around - 2.0 * here))
        forcing = jnp.concatenate(forcing, axis=0) if len(forcing) > 1 else forcing[0]
        pieces = split(forcing[:, 0:512])
        node = forcing[:, 512:576]
        push = dot3(pieces, (hr_hi[s], hr_lo[s]), NT) + jnp.concatenate([node, jnp.zeros_like(node)], axis=1)
        at = 0
        for r, n in chunks:
            gs_hi[s, r : r + n, :], gs_lo[s, r : r + n, :] = (x[at : at + n] for x in pieces)
            injs[s, r : r + n, :] = push[at : at + n]
            at += n

    def weights(s):
        pair_weights(pair_ref.at[s], pw_hi.at[s], pw_lo.at[s], pn_hi.at[s], pn_lo.at[s])
        hr_hi[s], hr_lo[s] = split(row[s])

    def product(it, s):
        if it == ITERS - 1:
            for b in range(4):
                rows = slice(128 * b, 128 * b + 128)
                value = dot3((g_hi[s, rows, :], g_lo[s, rows, :]), (gs_hi[s], gs_lo[s]), NT)
                for h in range(2):
                    outs[s, ORDER[2 * b + h]] = value[64 * h : 64 * h + 64]
        else:
            state[it + 1, s, 8:264, 0:512] = dot3((gs_hi[s], gs_lo[s]), (g_hi[s], g_lo[s]))

    middle, edges = ((16, 224),), ((0, 16), (240, 16))
    weights(core)
    pair_term(0, core)
    forcing_term(0, core, middle)
    for give in gives:
        give.wait_recv()
    weights(away)
    handed = [hand_on(1, 1), hand_on(2, 3)]
    pair_term(0, away)
    forcing_term(0, away, middle)
    handed.append(hand_on(0, 2))
    give_full = start(remote(full.at[core], full.at[core], give_send.at[4], give_recv.at[4], {"lev": partner}))
    for slot in range(2):
        pltpu.make_async_copy(field.at[0:8], state.at[0, 0, 0:8], halo_recv.at[0, slot]).wait()
    for s in range(2):
        forcing_term(0, s, edges)
    for copy in [spread[3]] + handed:
        copy.wait_recv()
    interface(packs, own_hi, own_lo, msg_hi, msg_lo, rlo_hi, rlo_lo, rhi_hi, rhi_lo, wp, wc, rs, rc, own)
    for it in range(ITERS):
        final = it == ITERS - 1
        if it:
            for s in range(2):
                pair_term(it, s)
            for s in range(2):
                forcing_term(it, s, middle)
        slot = 1 + lax.rem(chip, 2)

        def send(chunks, out, into, sems):
            lines = [
                jnp.concatenate([injs[s, q + r : q + r + n] for q in (0, 128) for s in range(2)], axis=1) for r, n in chunks
            ]
            message = dot3(split(jnp.concatenate(lines, axis=0) if len(lines) > 1 else lines[0]), (msg_hi[...], msg_lo[...]))
            out[0] = message[:, 0:128]
            out[1] = message[:, 128:256]
            to = [(1, slot, {"lev": across[0]}), (1, slot, {"lev": across[1]}), (0, 0, {"lev": sibling})]
            for i, (which, where, target) in enumerate(to):
                start(remote(out.at[which], into.at[where], msg_send.at[sems, i], msg_recv.at[sems, where], target))

        if it == 0:
            send([(0, 128)], outgo, incoming, 0)
        else:
            send([(16, 96)], out_most, in_most, 1)
            for halo in halos:
                halo.wait_recv()
            for s in range(2):
                forcing_term(it, s, edges)
            send([(0, 16), (112, 16)], out_edge, in_edge, 2)
        inj = jnp.concatenate([injs[0], injs[1]], axis=1)
        mine = dot3(split(inj), (own_hi[...], own_lo[...]))
        if it == 0:
            give_full.wait_recv()
            for s in range(2):
                g_hi[s], g_lo[s] = split(full[s])
                hc_hi[s], hc_lo[s] = split(row[s].T)
        for s in range(2):
            product(it, s)
        for i, into in [(0, incoming)] if it == 0 else [(1, in_most), (2, in_edge)]:
            for where in range(3):
                pltpu.make_async_copy(into.at[where], into.at[where], msg_recv.at[i, where]).wait()
        join = lambda x: jnp.concatenate([x[0], x[1] + x[2]], axis=1)
        if it == 0:
            heard = join(incoming)
        else:
            heard = jnp.concatenate([join(in_edge[:, 0:16]), join(in_most), join(in_edge[:, 16:32])], axis=0)
        heard = split(heard)
        total = mine + jnp.concatenate(
            [dot3(heard, (rlo_hi[...], rlo_lo[...])), dot3(heard, (rhi_hi[...], rhi_lo[...]))], axis=0
        )
        total_of = [total[:, 128 * s : 128 * s + 128] for s in range(2)]
        if not final:
            def land(s, chunks):
                ends = [total_of[s][r : r + n] for r, n in chunks]
                ends = jnp.concatenate(ends, axis=0) if len(ends) > 1 else ends[0]
                add = dot3(split(ends), (hr_hi[s], hr_lo[s]))
                node = jnp.where(lax.broadcasted_iota(jnp.int32, ends.shape, 1) < S, ends, 0.0)
                at = 0
                for r, n in chunks:
                    state[it + 1, s, 8 + r : 8 + r + n, 0:512] += add[at : at + n]
                    state[it + 1, s, 8 + r : 8 + r + n, 512:640] = node[at : at + n]
                    at += n

            for s in range(2):
                land(s, edges)
            inner_from, inner_to = 8 + 248 * away, 264 * core
            outer_from, outer_to = 8 + 248 * core, 264 * away
            halos = [
                start(remote(state.at[it + 1, :, rows_at(a, 8), :], state.at[it + 1, :, rows_at(b, 8), :],
                             halo_send.at[it + 1, i], halo_recv.at[it + 1, i], where))
                for i, (a, b, where) in enumerate([
                    (outer_from, outer_to, {"lev": partner, "lon": west + (east - west) * core}),
                    (inner_from, inner_to, {"lev": partner}),
                ])
            ]
            for s in range(2):
                land(s, middle)
            continue
    ones = jnp.ones((8, 256), BF16)
    dot1 = lambda x: lax.dot_general(ones, x, NT, preferred_element_type=F32)
    line = lax.broadcasted_iota(jnp.int32, (8, 128), 0)

    ends_ref[0], ends_ref[1] = total_of

    def last_values(s):
        pieces = split(ends_ref[s])
        for b in range(4):
            rows = slice(128 * b, 128 * b + 128)
            value = dot3((hc_hi[s, rows, :], hc_lo[s, rows, :]), pieces, NT)
            for h in range(2):
                outs[s, ORDER[2 * b + h]] += value[64 * h : 64 * h + 64]
        outs[s, 0] = ends_ref[s].T[0:64]

    def squares_of(s):
        packed = jnp.zeros((8, 128), F32)
        for j in range(5):
            values = [outs[s, level] for level in ((ORDER + (0,))[2 * j : 2 * j + 2])]
            values = jnp.concatenate(values if j < 4 else values + [jnp.zeros_like(values[0])], axis=0)
            high, low = split(values * values)
            packed = jnp.where(line == j, dot1(high) + dot1(low), packed)
        part[s] = packed

    last_values(away)
    squares_of(away)
    give = start(remote(part.at[away], part_in, out_send.at[0], out_recv.at[0], {"lev": partner}))
    back = start(remote(outs.at[away], out_any.at[core], out_send.at[1], out_recv.at[1], {"lev": partner}))
    last_values(core)
    keep = pltpu.make_async_copy(outs.at[core], out_any.at[core], load_sem.at[0])
    keep.start()
    squares_of(core)
    give.wait_recv()
    mine = part[core] + part_in[...]
    mysum[...] = mine
    wide_z = count // deep
    y, z = lon // wide_z, lax.rem(lon, wide_z)
    steps = [(dy, dz) for dy in range(deep) for dz in range(wide_z) if dy or dz]
    steps.sort(key=lambda step: -min(step[0], deep - step[0]) - min(step[1], wide_z - step[1]))
    for i, (dy, dz) in enumerate(steps):
        target = lax.rem(y + dy, deep) * wide_z + lax.rem(z + dz, wide_z)
        slot = lax.rem(count + lon - target - 1, count)
        remote(mysum.at[0:5], sumbuf.at[slot, 0:5], sum_send, sum_recv, {"lon": target}).start()
    keep.wait()
    back.wait_recv()
    for copy in pending:
        copy.wait_send()
    if steps:
        slots = sumbuf.at[0 : len(steps), 0:5]
        pltpu.make_async_copy(slots, slots, sum_send).wait()
        pltpu.make_async_copy(slots, slots, sum_recv).wait()
        mine = mine[0:5] + jnp.sum(sumbuf[:, 0:5], axis=0)
    total = mine * (1.0 / (512 * count))
    for j in range(9):
        level = (ORDER + (0,))[j]
        var_ref[level : level + 1, :] = total[j // 2 : j // 2 + 1, S * (j % 2) : S * (j % 2) + S]


def put_out(field_any, sums_any, out_ref, var_ref, sem):
    copies = [
        pltpu.make_async_copy(
            field_any.at[half, pl.ds(level, 3)], out_ref.at[pl.ds(level, 3), :, pl.ds(256 * half, 256)], sem.at[3 * half + level // 3]
        )
        for half in range(2)
        for level in (0, 3, 6)
    ]
    copies.append(pltpu.make_async_copy(sums_any, var_ref, sem.at[6]))
    for copy in copies:
        copy.start()
    for copy in copies:
        copy.wait()


def vmem(count):
    return [pl.BlockSpec(memory_space=pltpu.VMEM)] * count


def local(previous, loss_matrix, pair_matrix, diffusivity, mixing):
    count = lax.axis_size("lon")
    low = lambda *shape: [pltpu.VMEM(shape, BF16)] * 2
    full = lambda *shape: [pltpu.VMEM(shape, F32)]
    sems = lambda *shape: [pltpu.SemaphoreType.DMA(shape)] * 2
    scratch = [pltpu.SMEM((9,), F32)] * 2 + full(9, S, S) + full(2, 9, S, S) + full(9, S, 512) + [pltpu.SemaphoreType.DMA((5,))]
    scratch += full(2, 512, 512) + full(2, 128, 512) + low(2, 512, 512) + low(2, 128, 512) + low(2, 512, 128) + full(96, 128)
    scratch += low(2, 2, 256, 256) + low(2, S, S) + full(512, 640) + full(2, 8, 640)
    scratch += full(8, 96, 128) + low(256, 256) + low(512, 256) + low(256, 256) * 2
    scratch += full(256, S) * 2 + full(S, 256) * 2 + full(256, 256)
    scratch += full(2, 2, 272, 640) + low(2, 256, 512) + full(2, 256, 128) + full(2, 128, 128) + full(3, 128, 128)
    scratch += full(2, 96, 128) + full(3, 96, 128) + full(2, 32, 128) + full(3, 32, 128)
    scratch += full(2, 256, 640) + full(2, 9, S, 256) + full(2, 256, 128) + full(2, 8, 128) + full(8, 128) * 2 + full(max(count - 1, 1), 8, 128)
    scratch += sems(7) + sems(5) + sems(2, 2) + sems(3, 3) + sems(2) + [pltpu.SemaphoreType.DMA] * 2
    shapes = [jax.ShapeDtypeStruct((9, S, 512), F32), jax.ShapeDtypeStruct((9, S), F32)]
    halves = jax.ShapeDtypeStruct((2, 9, S, 256), F32)
    anywhere = [pl.BlockSpec(memory_space=pl.ANY)] * 2
    done = pl.pallas_call(
        functools.partial(kernel, count, 4 if count % 4 == 0 else 1),
        out_shape=[halves, shapes[1]],
        in_specs=[pl.BlockSpec(memory_space=pltpu.HBM)] * 5,
        out_specs=(anywhere[0], vmem(1)[0]),
        scratch_shapes=scratch,
        compiler_params=pltpu.CompilerParams(vmem_limit_bytes=32 * 2**20, collective_id=0, has_side_effects=True),
    )(*[pltpu.with_memory_space_constraint(x, pltpu.HBM) for x in (diffusivity, mixing, loss_matrix, pair_matrix, previous)])
    return tuple(pl.pallas_call(
        put_out,
        out_shape=shapes,
        in_specs=anywhere,
        out_specs=tuple(anywhere),
        scratch_shapes=[pltpu.SemaphoreType.DMA((7,))],
        compiler_params=pltpu.CompilerParams(vmem_limit_bytes=8 * 2**20),
    )(*done))


def solution(mesh):
    placed = (P("lev", None, "lon"), P("lev", None, None), P("lev", None, None), P("lev"), P("lev"))
    return jax.shard_map(
        local,
        mesh=mesh,
        in_specs=placed,
        out_specs=(P("lev", None, "lon"), P("lev", None)),
        check_vma=False,
    )
```

```python
import functools

import jax
import jax.numpy as jnp
from jax import lax
from jax.experimental import pallas as pl
from jax.experimental.pallas import tpu as pltpu
from jax.sharding import PartitionSpec as P

ITERS = 2
F32 = jnp.float32
BF16 = jnp.bfloat16
MESH = pl.DeviceIdType.MESH

S = 64
ORDER = (1, 2, 4, 5, 7, 8, 3, 6)
NN = (((1,), (0,)), ((), ()))
NT = (((1,), (1,)), ((), ()))
TN = (((0,), (0,)), ((), ()))


def split(x):
    high = x.astype(BF16)
    return high, (x - high.astype(F32)).astype(BF16)


def dot3(a, b, dims=NN):
    one = lambda x, y: lax.dot_general(x, y, dims, preferred_element_type=F32)
    return one(a[0], b[0]) + (one(a[0], b[1]) + one(a[1], b[0]))


def mm(a, b, dims=NN):
    return dot3(split(a), split(b), dims)


def eye(n):
    rows = lax.broadcasted_iota(jnp.int32, (n, n), 0)
    return (rows == lax.broadcasted_iota(jnp.int32, (n, n), 1)).astype(F32)


def spd_inverses(blocks, lows, high, doublings):
    centres = [0.5 * (high + low) for low in lows]
    units = [eye(block.shape[0]) for block in blocks]
    inverses = [unit * (1.0 / centre) for unit, centre in zip(units, centres)]
    residuals = [unit - block * (1.0 / centre) for unit, block, centre in zip(units, blocks, centres)]
    terms = [(high + low) / (high - low) for low in lows]
    for step in range(doublings):
        last = step == doublings - 1
        for i, unit in enumerate(units):
            twice = 2.0 * terms[i] * terms[i] - 1.0
            gain, shift = (twice + 1.0) / twice, 1.0 / twice
            terms[i] = twice
            centre = centres[i]
            n = unit.shape[0]
            late = step >= doublings - 3
            parts = (lambda x: (x.astype(BF16),)) if late else split
            product = (lambda x, y: lax.dot_general(x[0], y[0], NN, preferred_element_type=F32)) if late else dot3
            rest = parts(residuals[i])
            if step == 0:
                inverses[i] = (inverses[i] + residuals[i] * (1.0 / centre)) * gain
                if not last:
                    residuals[i] = gain * product(rest, rest) - shift * unit
                continue
            known = parts(inverses[i])
            if last:
                inverses[i] = gain * (inverses[i] + product(known, rest))
                continue
            both = product(tuple(jnp.concatenate(p, axis=0) for p in zip(known, rest)), rest)
            inverses[i] = gain * (inverses[i] + both[:n])
            residuals[i] = gain * both[n:] - shift * unit
    exact = [unit - mm(block, inverse) for unit, block, inverse in zip(units, blocks, inverses)]
    step = lambda x, y: lax.dot_general(x.astype(BF16), y.astype(BF16), NN, preferred_element_type=F32)
    return [inverse + step(inverse, rest) for inverse, rest in zip(inverses, exact)]


def wide(grid):
    return jnp.concatenate([jnp.concatenate(row, axis=1) if len(row) > 1 else row[0] for row in grid], axis=0)


def interior(link_ref, loss_ref, pack_ref):
    one = eye(S)
    zero = jnp.zeros((S, S), F32)
    links = [link_ref[i] for i in range(9)]
    shunt = [loss_ref[i] + one for i in range(9)]
    blocks = []
    for top in (1, 4, 7):
        diag = [shunt[level] + (links[level - 1] + links[level]) * one for level in (top, top + 1)]
        tie = -links[top] * one
        blocks.append(wide([[diag[0], tie], [tie, diag[1]]]))
    pairs = spd_inverses(blocks, [199.0] * 3, 6700.0, 5)
    none = jnp.zeros((S, 128), F32)
    spread = wide([
        [links[2] * pairs[0][S:], links[3] * pairs[1][:S], none],
        [none, links[5] * pairs[1][S:], links[6] * pairs[2][:S]],
    ])
    ground = jnp.concatenate(
        [shunt[1] + links[0] * one, shunt[2], shunt[4], shunt[5], shunt[7], shunt[8] + links[8] * one], axis=0
    )
    own = jnp.concatenate([shunt[3], shunt[6]], axis=0) + mm(spread, ground)
    down = links[5] * spread[0:S, 192:256]
    up = links[3] * spread[S:, 128:192]
    lane = lax.broadcasted_iota(jnp.int32, (128, 128), 1)
    ends = jnp.where(lane < S, spread[:, 0:128], spread[:, 256:384])
    stack = jnp.concatenate([shunt[level] for level in ORDER], axis=0)
    through = mm(spread, stack[0:384]) + stack[384:512]
    direct = [mm(pairs[0][:S], stack[0:128]), mm(pairs[2][S:], stack[256:384])]
    middle, = spd_inverses([wide([[own[:S] + down, -down], [-up, own[S:] + up]])], [68.6], 3010.0, 5)
    seen = mm(ends, middle, TN)
    loads = mm(seen, through)
    across = (links[0] * links[8]) * mm(seen[0:S], spread)[:, 320:384]
    pack_ref[0:64, :] = jnp.concatenate(
        [shunt[0] + links[0] * (loads[0:S] + direct[0]), links[8] * (loads[S:] + direct[1])], axis=1
    )
    pack_ref[64:96, :] = jnp.concatenate([across[0:32], across[32:64]], axis=1)
    return pairs, jnp.concatenate([spread, eye(128)], axis=1), middle, seen


def end_rows(link_ref, row_ref, pairs, spread, middle, seen):
    ends = mm(seen, spread)
    first = jnp.concatenate([ends[0:S, 0:128] + pairs[0][:S], ends[0:S, 128:512]], axis=1)
    last = jnp.concatenate([ends[S:, 0:256], ends[S:, 256:384] + pairs[2][S:], ends[S:, 384:512]], axis=1)
    row_ref[...] = jnp.concatenate([link_ref[0] * first, link_ref[8] * last], axis=0)


def finish_interior(full, pairs, spread, middle, seen):
    full[...] = mm(spread, mm(middle, spread), TN)
    for i in range(3):
        at = slice(128 * i, 128 * i + 128)
        full[at, at] += pairs[i]


def pair_weights(pair_ref, pw_hi, pw_lo, pn_hi, pn_lo):
    for half in range(2):
        row = lax.broadcasted_iota(jnp.int32, (256, 256), 0) // S
        column = lax.broadcasted_iota(jnp.int32, (256, 256), 1) // S
        tall = jnp.concatenate([pair_ref[level] for level in ORDER[4 * half : 4 * half + 4]], axis=0)
        tall = jnp.concatenate([tall, tall], axis=1)
        tall = jnp.where(row == column, jnp.concatenate([tall, tall], axis=1), 0.0)
        pw_hi[half], pw_lo[half] = split(tall)
    pn_hi[...], pn_lo[...] = split(pair_ref[0])


def field_of(prev_ref, field_ref):
    for j in range(4):
        both = jnp.concatenate([prev_ref[ORDER[2 * j]], prev_ref[ORDER[2 * j + 1]]], axis=0)
        field_ref[:, 128 * j : 128 * j + 128] = both.T
    last = jnp.concatenate([prev_ref[0], jnp.zeros_like(prev_ref[0])], axis=0)
    field_ref[:, 512:640] = last.T


def mix_row_of(mix_ref, mixrow_ref):
    lane = lax.broadcasted_iota(jnp.int32, (8, 640), 1) // S
    row = jnp.zeros((8, 640), F32)
    for j, level in enumerate(ORDER + (0,)):
        row = jnp.where(lane == j, mix_ref[level], row)
    mixrow_ref[...] = row


def unpack(packs, q):
    both, folded = packs(q)
    across = jnp.concatenate([folded[:, 0:S], folded[:, S:]], axis=0)
    return both[:, 0:S], both[:, S:], across


def interface(pack_ref, own_hi, own_lo, msg_hi, msg_lo, rlo_hi, rlo_lo, rhi_hi, rhi_lo, wp, wc, rs, rc, own):
    chip = lax.axis_index("lev") // 2
    one = eye(S)
    zero = jnp.zeros((S, S), F32)
    here, below, across = zip(*[
        unpack(lambda q: (pack_ref[q, 0:64, :], pack_ref[q, 64:96, :]), q) for q in range(8)
    ])
    back = [a.T for a in across]
    ground = [here[q] + (below[q - 1] if q else 0.0) for q in range(8)]
    diag = [ground[q] + across[q] + (back[q - 1] if q else 0.0) for q in range(8)]
    upper = wide([
        [diag[0], -across[0], zero, zero],
        [-back[0], diag[1], -across[1], zero],
        [zero, -back[1], diag[2], -across[2]],
        [zero, zero, -back[2], diag[3]],
    ])
    lower = wide([
        [diag[5], -across[5], zero],
        [-back[5], diag[6], -across[6]],
        [zero, -back[6], diag[7]],
    ])
    first = chip < 2
    small = jnp.where(
        first, upper[0:128, 0:128], wide([[500.0 * one, zero], [zero, diag[7]]])
    )
    upper_inverse, lower_inverse, small_inverse = spd_inverses(
        [upper, lower, small], [9.6, 21.0, 13.9], 2400.0, 6
    )
    upper_t = mm(back[3], upper_inverse[192:256, :])
    lower_t = mm(across[4], lower_inverse[0:64, :])
    middle = (
        ground[4]
        + mm(upper_t, jnp.concatenate(ground[0:4], axis=0))
        + mm(lower_t, jnp.concatenate([ground[5], ground[6], ground[7] + across[7]], axis=0))
    )
    middle_inverse, = spd_inverses([middle], [28.7], 2400.0, 5)
    spread = jnp.concatenate([upper_t, lower_t, one], axis=1)
    lifted = mm(middle_inverse, spread)
    place = {0: 0, 1: 1, 2: 2, 3: 3, 4: 7, 5: 4, 6: 5, 7: 6}
    link = jnp.where(first, back[1], across[6])
    away = mm(link, small_inverse[64:128, :])

    for c in range(4):
        nodes = (2 * c, 2 * c + 1, 2 * c + 1, 2 * c + 2)

        @pl.when(chip == c)
        def _(c=c, nodes=nodes):
            real = [n for n in range(2 * c, 2 * c + 3) if n < 8]
            against = real if 4 in real else real + [4]
            part = lambda x, n: x[:, S * place[n] : S * place[n] + S]
            both = [jnp.concatenate([part(x, n) for n in which], axis=1) for x, which in ((spread, real), (lifted, against))]
            product = mm(both[0], both[1], TN)

            def block(r, k):
                if r not in real or k not in against:
                    return zero
                i, j = real.index(r), against.index(k)
                value = product[S * i : S * i + S, S * j : S * j + S]
                i, j = place[r], place[k]
                if i < 4 and j < 4:
                    value += upper_inverse[S * i : S * i + S, S * j : S * j + S]
                elif 4 <= i < 7 and 4 <= j < 7:
                    value += lower_inverse[S * (i - 4) : S * (i - 3), S * (j - 4) : S * (j - 3)]
                return value

            def blocks(rows, columns):
                return wide([[block(r, k) for k in columns] for r in rows])

            own[...] = blocks(nodes, nodes)
            wc[...] = blocks(nodes, (4,))
            if c in (0, 3):
                far = [away[:, 0:64], away[:, 64:128]]
                if c == 0:
                    rs[...] = jnp.concatenate([far[0], far[1], far[1], one], axis=1)
                    wp[...] = jnp.concatenate([far[0].T, far[1].T, far[1].T, one], axis=0)
                else:
                    rs[...] = jnp.concatenate([one, far[1], far[1], zero], axis=1)
                    wp[...] = jnp.concatenate([one, far[1].T, far[1].T, zero], axis=0)
            else:
                gate = 2 if c == 1 else 6
                rs[...] = blocks((gate,), nodes)
                wp[...] = blocks(nodes, (gate,))

            def seen(n):
                if n > 7:
                    return zero
                n = place[n]
                return spread[:, S * n : S * n + S]

            rc[...] = jnp.concatenate([seen(n) for n in nodes], axis=1)

    own_hi[...], own_lo[...] = split(own[...])
    none = jnp.zeros((256, S), F32)
    msg = wide([[wp[...], none, wc[...], none], [none, wp[...], none, wc[...]]])
    msg_hi[...], msg_lo[...] = split(msg)
    none = jnp.zeros((S, 256), F32)
    rlo_hi[...], rlo_lo[...] = split(jnp.concatenate([rs[...], none, rc[...], none], axis=0))
    rhi_hi[...], rhi_lo[...] = split(jnp.concatenate([none, rs[...], none, rc[...]], axis=0))


def kernel(count, deep, link_hbm, mix_hbm, loss_hbm, pair_hbm, prev_hbm, out_any, var_ref,
           link_ref, mix_ref, loss_ref, pair_ref, prev_ref, load_sem,
           full, row, g_hi, g_lo, hr_hi, hr_lo, hc_hi, hc_lo, pack, pw_hi, pw_lo, pn_hi, pn_lo, field, mixrow,
           packs, own_hi, own_lo, msg_hi, msg_lo, rlo_hi, rlo_lo, rhi_hi, rhi_lo, wp, wc, rs, rc, own,
           state, gs_hi, gs_lo, injs, out_first, in_first, out_then, in_then, out_most, in_most, out_edge, in_edge, sums, outs, ends_ref, part, part_in, mysum, sumbuf,
           pack_send, pack_recv, give_send, give_recv, halo_send, halo_recv, msg_send, msg_recv, out_send, out_recv,
           sum_send, sum_recv):
    lev = lax.axis_index("lev")
    lon = lax.axis_index("lon")
    core = lax.rem(lev, 2)
    chip = lev // 2
    partner = lev + 1 - 2 * core
    base = lev - core
    sibling = 2 * (chip + 1 - 2 * lax.rem(chip, 2)) + core
    across_base = 2 - 2 * (chip // 2)
    far = lax.rem(chip + 2, 4)
    across = [2 * far + core, 2 * (2 * across_base + 1 - far) + core]
    west, east = lax.rem(lon + count - 1, count), lax.rem(lon + 1, count)
    loads = [
        pltpu.make_async_copy(src, dst, load_sem.at[i])
        for i, (src, dst) in enumerate([
            (link_hbm, link_ref), (loss_hbm, loss_ref), (prev_hbm, prev_ref), (pair_hbm, pair_ref.at[core]), (mix_hbm, mix_ref),
        ])
    ]
    for load in loads:
        load.start()
    barrier = pltpu.get_barrier_semaphore()
    others = [lax.rem(lev + d, 8) for d in range(1, 8)]
    for other in others:
        pl.semaphore_signal(barrier, inc=1, device_id={"lev": other}, device_id_type=MESH)
    for side in (west, east):
        pl.semaphore_signal(barrier, inc=1, device_id={"lev": partner, "lon": side}, device_id_type=MESH)

    def greet(d, carry):
        pl.semaphore_signal(barrier, inc=1, device_id={"lon": lax.rem(lon + d, count)}, device_id_type=MESH)
        return carry

    lax.fori_loop(1, count, greet, 0)

    def remote(src, dst, send, recv, where):
        return pltpu.make_async_remote_copy(
            src_ref=src, dst_ref=dst, send_sem=send, recv_sem=recv, device_id=where, device_id_type=MESH
        )

    def rows_at(start, size):
        return pl.ds(pl.multiple_of(start, 8), size)

    pending = []

    def start(copy):
        copy.start()
        pending.append(copy)
        return copy

    loads[0].wait()
    loads[1].wait()
    parts = interior(link_ref, loss_ref, pack)
    loads[3].wait()
    loads[4].wait()
    mix_row_of(mix_ref, mixrow.at[core])
    pl.semaphore_wait(barrier, 8 + count)
    packs[lev] = pack[...]
    spread = [
        start(remote(pack, packs.at[lev], pack_send.at[i], pack_recv.at[i], {"lev": target}))
        for i, target in enumerate([2 * lax.rem(chip + d, 4) + core for d in (2, 1, 3)] + [partner])
    ]
    end_rows(link_ref, row.at[core], *parts)
    loads[2].wait()
    field_of(prev_ref, field)

    def hand_on(i, d):
        spread[i].wait_recv()
        source = 2 * lax.rem(chip + 4 - d, 4) + core
        return start(remote(packs.at[source], packs.at[source], pack_send.at[4 + i], pack_recv.at[4 + i], {"lev": partner}))

    away = 1 - core
    gives = [
        start(remote(src, dst, give_send.at[i], give_recv.at[i], {"lev": partner}))
        for i, (src, dst) in enumerate([
            (field.at[rows_at(248 * away, 264)], state.at[0, core, rows_at(8 * core, 264)]),
            (pair_ref.at[core], pair_ref.at[core]),
            (mixrow.at[core], mixrow.at[core]),
            (row.at[core], row.at[core]),
        ])
    ]
    outer = [
        start(remote(field.at[0:8], state.at[0, core, 264:272], halo_send.at[0, 0], halo_recv.at[0, core],
                     {"lev": base + 1, "lon": west})),
        start(remote(field.at[504:512], state.at[0, core, 0:8], halo_send.at[0, 1], halo_recv.at[0, core],
                     {"lev": base, "lon": east})),
    ]
    state[0, core, rows_at(8 * away, 264), :] = field[rows_at(248 * core, 264), :]
    finish_interior(full.at[core], *parts)

    def pair_term(it, s, chunks=((0, 256),)):
        here = [state[it, s, 8 + r : 8 + r + n, :] for r, n in chunks]
        here = jnp.concatenate(here, axis=0) if len(here) > 1 else here[0]
        squares = split(here * here)
        out = []
        for half in range(2):
            piece = tuple(x[:, 256 * half : 256 * half + 256] for x in squares)
            out.append((256 * half, 256, dot3(piece, (pw_hi[s, half], pw_lo[s, half]), NT)))
        piece = tuple(x[:, 512:576] for x in squares)
        out.append((512, 64, dot3(piece, (pn_hi[s], pn_lo[s]), NT)))
        at = 0
        for r, n in chunks:
            for lane, width, value in out:
                sums[s, r : r + n, lane : lane + width] = value[at : at + n]
            at += n

    def forcing_term(it, s, chunks):
        forcing = []
        for r, n in chunks:
            here = state[it, s, 8 + r : 8 + r + n, 0:576]
            around = state[it, s, 7 + r : 7 + r + n, 0:576] + state[it, s, 9 + r : 9 + r + n, 0:576]
            value = state[0, s, 8 + r : 8 + r + n, 0:576] - sums[s, r : r + n, 0:576]
            forcing.append(value + mixrow[s, 0:1, 0:576] * (around - 2.0 * here))
        forcing = jnp.concatenate(forcing, axis=0) if len(forcing) > 1 else forcing[0]
        pieces = split(forcing[:, 0:512])
        node = forcing[:, 512:576]
        push = dot3(pieces, (hr_hi[s], hr_lo[s]), NT) + jnp.concatenate([node, jnp.zeros_like(node)], axis=1)
        at = 0
        for r, n in chunks:
            gs_hi[s, r : r + n, :], gs_lo[s, r : r + n, :] = (x[at : at + n] for x in pieces)
            injs[s, r : r + n, :] = push[at : at + n]
            at += n

    def weights(s):
        pair_weights(pair_ref.at[s], pw_hi.at[s], pw_lo.at[s], pn_hi.at[s], pn_lo.at[s])
        hr_hi[s], hr_lo[s] = split(row[s])

    def product(it, s):
        if it == ITERS - 1:
            for b in range(4):
                rows = slice(128 * b, 128 * b + 128)
                value = dot3((g_hi[s, rows, :], g_lo[s, rows, :]), (gs_hi[s], gs_lo[s]), NT)
                for h in range(2):
                    outs[s, ORDER[2 * b + h]] = value[64 * h : 64 * h + 64]
        else:
            state[it + 1, s, 8:264, 0:512] = dot3((gs_hi[s], gs_lo[s]), (g_hi[s], g_lo[s]))

    middle, edges = ((16, 224),), ((0, 16), (240, 16))
    weights(core)
    pair_term(0, core)
    forcing_term(0, core, middle)
    for give in gives:
        give.wait_recv()
    weights(away)
    handed = [hand_on(1, 1), hand_on(2, 3)]
    pair_term(0, away)
    handed.append(hand_on(0, 2))
    forcing_term(0, away, middle)
    give_full = start(remote(full.at[core], full.at[core], give_send.at[4], give_recv.at[4], {"lev": partner}))
    for slot in range(2):
        pltpu.make_async_copy(field.at[0:8], state.at[0, 0, 0:8], halo_recv.at[0, slot]).wait()
    for s in range(2):
        forcing_term(0, s, edges)
    for copy in [spread[3]] + handed:
        copy.wait_recv()
    interface(packs, own_hi, own_lo, msg_hi, msg_lo, rlo_hi, rlo_lo, rhi_hi, rhi_lo, wp, wc, rs, rc, own)
    for it in range(ITERS):
        final = it == ITERS - 1
        if it:
            for s in range(2):
                forcing_term(it, s, middle)
        slot = 1 + lax.rem(chip, 2)

        def send(chunks, parts):
            lines = [
                jnp.concatenate([injs[s, q + r : q + r + n] for q in (0, 128) for s in range(2)], axis=1) for r, n in chunks
            ]
            message = dot3(split(jnp.concatenate(lines, axis=0) if len(lines) > 1 else lines[0]), (msg_hi[...], msg_lo[...]))
            at = 0
            for out, into, sems in parts:
                size = out.shape[1]
                out[0] = message[at : at + size, 0:128]
                out[1] = message[at : at + size, 128:256]
                at += size
                to = [(1, slot, {"lev": across[0]}), (1, slot, {"lev": across[1]}), (0, 0, {"lev": sibling})]
                for i, (which, where, target) in enumerate(to):
                    start(remote(out.at[which], into.at[where], msg_send.at[sems, i], msg_recv.at[sems, where], target))

        if it == 0:
            send([(0, 32), (96, 32), (32, 64)], [(out_first, in_first, 0), (out_then, in_then, 3)])
        else:
            send([(16, 96)], [(out_most, in_most, 1)])
            for halo in halos:
                halo.wait_recv()
            for s in range(2):
                forcing_term(it, s, edges)
            send([(0, 16), (112, 16)], [(out_edge, in_edge, 2)])
        inj = jnp.concatenate([injs[0], injs[1]], axis=1)
        mine = dot3(split(inj), (own_hi[...], own_lo[...]))
        if it == 0:
            give_full.wait_recv()
            for s in range(2):
                g_hi[s], g_lo[s] = split(full[s])
                hc_hi[s], hc_lo[s] = split(row[s].T)
        for s in range(2):
            product(it, s)
        join = lambda x: jnp.concatenate([x[0], x[1] + x[2]], axis=1)

        def arrived(into, sems):
            for where in range(3):
                pltpu.make_async_copy(into.at[where], into.at[where], msg_recv.at[sems, where]).wait()

        def reached(heard, chunks):
            here = [mine[r : r + n] for r, n in chunks]
            heard = split(heard)
            return (jnp.concatenate(here, axis=0) if len(here) > 1 else here[0]) + jnp.concatenate(
                [dot3(heard, (rlo_hi[...], rlo_lo[...])), dot3(heard, (rhi_hi[...], rhi_lo[...]))], axis=0
            )

        def land(s, ends, chunks):
            ends = ends[:, 128 * s : 128 * s + 128]
            add = dot3(split(ends), (hr_hi[s], hr_lo[s]))
            node = jnp.where(lax.broadcasted_iota(jnp.int32, ends.shape, 1) < S, ends, 0.0)
            at = 0
            for r, n in chunks:
                state[it + 1, s, 8 + r : 8 + r + n, 0:512] += add[at : at + n]
                state[it + 1, s, 8 + r : 8 + r + n, 512:640] = node[at : at + n]
                at += n

        if not final:
            arrived(in_first, 0)
            columns = ((0, 32), (96, 32), (128, 32), (224, 32))
            ends = reached(join(in_first), columns)
            for s in range(2):
                land(s, ends, columns)
            inner_from, inner_to = 8 + 248 * away, 264 * core
            outer_from, outer_to = 8 + 248 * core, 264 * away
            halos = [
                start(remote(state.at[it + 1, :, rows_at(a, 8), :], state.at[it + 1, :, rows_at(b, 8), :],
                             halo_send.at[it + 1, i], halo_recv.at[it + 1, i], where))
                for i, (a, b, where) in enumerate([
                    (outer_from, outer_to, {"lev": partner, "lon": west + (east - west) * core}),
                    (inner_from, inner_to, {"lev": partner}),
                ])
            ]
            for s in range(2):
                pair_term(it + 1, s, columns)
            arrived(in_then, 3)
            columns = ((32, 64), (160, 64))
            ends = reached(join(in_then), columns)
            for s in range(2):
                land(s, ends, columns)
            for s in range(2):
                pair_term(it + 1, s, columns)
            continue
        arrived(in_most, 1)
        arrived(in_edge, 2)
        heard = jnp.concatenate([join(in_edge[:, 0:16]), join(in_most), join(in_edge[:, 16:32])], axis=0)
        total = reached(heard, ((0, 256),))
        total_of = [total[:, 128 * s : 128 * s + 128] for s in range(2)]
    ones = jnp.ones((8, 128), BF16)
    dot1 = lambda x: lax.dot_general(ones, x, NT, preferred_element_type=F32)
    line = lax.broadcasted_iota(jnp.int32, (8, 128), 0)

    ends_ref[0], ends_ref[1] = total_of

    def last_values(s):
        pieces = split(ends_ref[s])
        for b in range(4):
            rows = slice(128 * b, 128 * b + 128)
            value = dot3((hc_hi[s, rows, :], hc_lo[s, rows, :]), pieces, NT)
            for h in range(2):
                outs[s, ORDER[2 * b + h]] += value[64 * h : 64 * h + 64]
        outs[s, 0] = ends_ref[s].T[0:64]

    def squares_of(s):
        packed = jnp.zeros((8, 128), F32)
        for j in range(5):
            values = [outs[s, level] for level in ((ORDER + (0,))[2 * j : 2 * j + 2])]
            values = jnp.concatenate(values if j < 4 else values + [jnp.zeros_like(values[0])], axis=0)
            values = values * values
            high, low = split(values[:, 0:128] + values[:, 128:256])
            packed = jnp.where(line == j, dot1(high) + dot1(low), packed)
        part[s] = packed

    last_values(away)
    squares_of(away)
    give = start(remote(part.at[away], part_in, out_send.at[0], out_recv.at[0], {"lev": partner}))
    back = start(remote(outs.at[away], out_any.at[core], out_send.at[1], out_recv.at[1], {"lev": partner}))
    last_values(core)
    keep = pltpu.make_async_copy(outs.at[core], out_any.at[core], load_sem.at[0])
    keep.start()
    squares_of(core)
    give.wait_recv()
    mine = part[core] + part_in[...]
    mysum[...] = mine
    wide_z = count // deep
    y, z = lon // wide_z, lax.rem(lon, wide_z)
    steps = [(dy, dz) for dy in range(deep) for dz in range(wide_z) if dy or dz]
    steps.sort(key=lambda step: -min(step[0], deep - step[0]) - min(step[1], wide_z - step[1]))
    for i, (dy, dz) in enumerate(steps):
        target = lax.rem(y + dy, deep) * wide_z + lax.rem(z + dz, wide_z)
        slot = lax.rem(count + lon - target - 1, count)
        remote(mysum.at[0:5], sumbuf.at[slot, 0:5], sum_send, sum_recv, {"lon": target}).start()
    keep.wait()
    back.wait_recv()
    for copy in pending:
        copy.wait_send()
    if steps:
        slots = sumbuf.at[0 : len(steps), 0:5]
        pltpu.make_async_copy(slots, slots, sum_send).wait()
        pltpu.make_async_copy(slots, slots, sum_recv).wait()
        mine = mine[0:5] + jnp.sum(sumbuf[:, 0:5], axis=0)
    total = mine * (1.0 / (512 * count))
    for j in range(9):
        level = (ORDER + (0,))[j]
        var_ref[level : level + 1, :] = total[j // 2 : j // 2 + 1, S * (j % 2) : S * (j % 2) + S]


def put_out(field_any, sums_any, out_ref, var_ref, sem):
    copies = [
        pltpu.make_async_copy(
            field_any.at[half, pl.ds(level, 3)], out_ref.at[pl.ds(level, 3), :, pl.ds(256 * half, 256)], sem.at[3 * half + level // 3]
        )
        for half in range(2)
        for level in (0, 3, 6)
    ]
    copies.append(pltpu.make_async_copy(sums_any, var_ref, sem.at[6]))
    for copy in copies:
        copy.start()
    for copy in copies:
        copy.wait()


def vmem(count):
    return [pl.BlockSpec(memory_space=pltpu.VMEM)] * count


def local(previous, loss_matrix, pair_matrix, diffusivity, mixing):
    count = lax.axis_size("lon")
    low = lambda *shape: [pltpu.VMEM(shape, BF16)] * 2
    full = lambda *shape: [pltpu.VMEM(shape, F32)]
    sems = lambda *shape: [pltpu.SemaphoreType.DMA(shape)] * 2
    scratch = [pltpu.SMEM((9,), F32)] * 2 + full(9, S, S) + full(2, 9, S, S) + full(9, S, 512) + [pltpu.SemaphoreType.DMA((5,))]
    scratch += full(2, 512, 512) + full(2, 128, 512) + low(2, 512, 512) + low(2, 128, 512) + low(2, 512, 128) + full(96, 128)
    scratch += low(2, 2, 256, 256) + low(2, S, S) + full(512, 640) + full(2, 8, 640)
    scratch += full(8, 96, 128) + low(256, 256) + low(512, 256) + low(256, 256) * 2
    scratch += full(256, S) * 2 + full(S, 256) * 2 + full(256, 256)
    scratch += full(2, 2, 272, 640) + low(2, 256, 512) + full(2, 256, 128) + full(2, 64, 128) + full(3, 64, 128) + full(2, 64, 128) + full(3, 64, 128)
    scratch += full(2, 96, 128) + full(3, 96, 128) + full(2, 32, 128) + full(3, 32, 128)
    scratch += full(2, 256, 640) + full(2, 9, S, 256) + full(2, 256, 128) + full(2, 8, 128) + full(8, 128) * 2 + full(max(count - 1, 1), 8, 128)
    scratch += sems(7) + sems(5) + sems(2, 2) + sems(4, 3) + sems(2) + [pltpu.SemaphoreType.DMA] * 2
    shapes = [jax.ShapeDtypeStruct((9, S, 512), F32), jax.ShapeDtypeStruct((9, S), F32)]
    halves = jax.ShapeDtypeStruct((2, 9, S, 256), F32)
    anywhere = [pl.BlockSpec(memory_space=pl.ANY)] * 2
    done = pl.pallas_call(
        functools.partial(kernel, count, 4 if count % 4 == 0 else 1),
        out_shape=[halves, shapes[1]],
        in_specs=[pl.BlockSpec(memory_space=pltpu.HBM)] * 5,
        out_specs=(anywhere[0], vmem(1)[0]),
        scratch_shapes=scratch,
        compiler_params=pltpu.CompilerParams(vmem_limit_bytes=32 * 2**20, collective_id=0, has_side_effects=True),
    )(*[pltpu.with_memory_space_constraint(x, pltpu.HBM) for x in (diffusivity, mixing, loss_matrix, pair_matrix, previous)])
    return tuple(pl.pallas_call(
        put_out,
        out_shape=shapes,
        in_specs=anywhere,
        out_specs=tuple(anywhere),
        scratch_shapes=[pltpu.SemaphoreType.DMA((7,))],
        compiler_params=pltpu.CompilerParams(vmem_limit_bytes=8 * 2**20),
    )(*done))


def solution(mesh):
    placed = (P("lev", None, "lon"), P("lev", None, None), P("lev", None, None), P("lev"), P("lev"))
    return jax.shard_map(
        local,
        mesh=mesh,
        in_specs=placed,
        out_specs=(P("lev", None, "lon"), P("lev", None)),
        check_vma=False,
    )
```

```python
import functools

import jax
import jax.numpy as jnp
from jax import lax
from jax.experimental import pallas as pl
from jax.experimental.pallas import tpu as pltpu
from jax.sharding import PartitionSpec as P

ITERS = 2
F32 = jnp.float32
BF16 = jnp.bfloat16
MESH = pl.DeviceIdType.MESH

S = 64
ORDER = (1, 2, 4, 5, 7, 8, 3, 6)
NN = (((1,), (0,)), ((), ()))
NT = (((1,), (1,)), ((), ()))
TN = (((0,), (0,)), ((), ()))


def split(x):
    high = x.astype(BF16)
    return high, (x - high.astype(F32)).astype(BF16)


def dot3(a, b, dims=NN):
    one = lambda x, y: lax.dot_general(x, y, dims, preferred_element_type=F32)
    return one(a[0], b[0]) + (one(a[0], b[1]) + one(a[1], b[0]))


def mm(a, b, dims=NN):
    return dot3(split(a), split(b), dims)


def eye(n):
    rows = lax.broadcasted_iota(jnp.int32, (n, n), 0)
    return (rows == lax.broadcasted_iota(jnp.int32, (n, n), 1)).astype(F32)


def spd_inverses(blocks, lows, high, doublings):
    centres = [0.5 * (high + low) for low in lows]
    units = [eye(block.shape[0]) for block in blocks]
    inverses = [unit * (1.0 / centre) for unit, centre in zip(units, centres)]
    residuals = [unit - block * (1.0 / centre) for unit, block, centre in zip(units, blocks, centres)]
    terms = [(high + low) / (high - low) for low in lows]
    for step in range(doublings):
        last = step == doublings - 1
        for i, unit in enumerate(units):
            twice = 2.0 * terms[i] * terms[i] - 1.0
            gain, shift = (twice + 1.0) / twice, 1.0 / twice
            terms[i] = twice
            centre = centres[i]
            n = unit.shape[0]
            late = step >= doublings - 3
            parts = (lambda x: (x.astype(BF16),)) if late else split
            product = (lambda x, y: lax.dot_general(x[0], y[0], NN, preferred_element_type=F32)) if late else dot3
            rest = parts(residuals[i])
            if step == 0:
                inverses[i] = (inverses[i] + residuals[i] * (1.0 / centre)) * gain
                if not last:
                    residuals[i] = gain * product(rest, rest) - shift * unit
                continue
            known = parts(inverses[i])
            if last:
                inverses[i] = gain * (inverses[i] + product(known, rest))
                continue
            both = product(tuple(jnp.concatenate(p, axis=0) for p in zip(known, rest)), rest)
            inverses[i] = gain * (inverses[i] + both[:n])
            residuals[i] = gain * both[n:] - shift * unit
    exact = [unit - mm(block, inverse) for unit, block, inverse in zip(units, blocks, inverses)]
    step = lambda x, y: lax.dot_general(x.astype(BF16), y.astype(BF16), NN, preferred_element_type=F32)
    return [inverse + step(inverse, rest) for inverse, rest in zip(inverses, exact)]


def wide(grid):
    return jnp.concatenate([jnp.concatenate(row, axis=1) if len(row) > 1 else row[0] for row in grid], axis=0)


def interior(link_ref, loss_ref, pack_ref):
    one = eye(S)
    zero = jnp.zeros((S, S), F32)
    links = [link_ref[i] for i in range(9)]
    shunt = [loss_ref[i] + one for i in range(9)]
    blocks = []
    for top in (1, 4, 7):
        diag = [shunt[level] + (links[level - 1] + links[level]) * one for level in (top, top + 1)]
        tie = -links[top] * one
        blocks.append(wide([[diag[0], tie], [tie, diag[1]]]))
    pairs = spd_inverses(blocks, [199.0] * 3, 6700.0, 5)
    none = jnp.zeros((S, 128), F32)
    spread = wide([
        [links[2] * pairs[0][S:], links[3] * pairs[1][:S], none],
        [none, links[5] * pairs[1][S:], links[6] * pairs[2][:S]],
    ])
    ground = jnp.concatenate(
        [shunt[1] + links[0] * one, shunt[2], shunt[4], shunt[5], shunt[7], shunt[8] + links[8] * one], axis=0
    )
    own = jnp.concatenate([shunt[3], shunt[6]], axis=0) + mm(spread, ground)
    down = links[5] * spread[0:S, 192:256]
    up = links[3] * spread[S:, 128:192]
    lane = lax.broadcasted_iota(jnp.int32, (128, 128), 1)
    ends = jnp.where(lane < S, spread[:, 0:128], spread[:, 256:384])
    stack = jnp.concatenate([shunt[level] for level in ORDER], axis=0)
    through = mm(spread, stack[0:384]) + stack[384:512]
    direct = [mm(pairs[0][:S], stack[0:128]), mm(pairs[2][S:], stack[256:384])]
    middle, = spd_inverses([wide([[own[:S] + down, -down], [-up, own[S:] + up]])], [68.6], 3010.0, 5)
    seen = mm(ends, middle, TN)
    loads = mm(seen, through)
    across = (links[0] * links[8]) * mm(seen[0:S], spread)[:, 320:384]
    pack_ref[0:64, :] = jnp.concatenate(
        [shunt[0] + links[0] * (loads[0:S] + direct[0]), links[8] * (loads[S:] + direct[1])], axis=1
    )
    pack_ref[64:96, :] = jnp.concatenate([across[0:32], across[32:64]], axis=1)
    return pairs, jnp.concatenate([spread, eye(128)], axis=1), middle, seen


def end_rows(link_ref, row_ref, pairs, spread, middle, seen):
    ends = mm(seen, spread)
    first = jnp.concatenate([ends[0:S, 0:128] + pairs[0][:S], ends[0:S, 128:512]], axis=1)
    last = jnp.concatenate([ends[S:, 0:256], ends[S:, 256:384] + pairs[2][S:], ends[S:, 384:512]], axis=1)
    row_ref[...] = jnp.concatenate([link_ref[0] * first, link_ref[8] * last], axis=0)


def finish_interior(full, pairs, spread, middle, seen):
    full[...] = mm(spread, mm(middle, spread), TN)
    for i in range(3):
        at = slice(128 * i, 128 * i + 128)
        full[at, at] += pairs[i]


def pair_weights(pair_ref, pw_hi, pw_lo, pn_hi, pn_lo):
    for half in range(2):
        row = lax.broadcasted_iota(jnp.int32, (256, 256), 0) // S
        column = lax.broadcasted_iota(jnp.int32, (256, 256), 1) // S
        tall = jnp.concatenate([pair_ref[level] for level in ORDER[4 * half : 4 * half + 4]], axis=0)
        tall = jnp.concatenate([tall, tall], axis=1)
        tall = jnp.where(row == column, jnp.concatenate([tall, tall], axis=1), 0.0)
        pw_hi[half], pw_lo[half] = split(tall)
    pn_hi[...], pn_lo[...] = split(pair_ref[0])


def field_of(prev_ref, field_ref):
    for j in range(4):
        both = jnp.concatenate([prev_ref[ORDER[2 * j]], prev_ref[ORDER[2 * j + 1]]], axis=0)
        field_ref[:, 128 * j : 128 * j + 128] = both.T
    last = jnp.concatenate([prev_ref[0], jnp.zeros_like(prev_ref[0])], axis=0)
    field_ref[:, 512:640] = last.T


def mix_row_of(mix_ref, mixrow_ref):
    lane = lax.broadcasted_iota(jnp.int32, (8, 640), 1) // S
    row = jnp.zeros((8, 640), F32)
    for j, level in enumerate(ORDER + (0,)):
        row = jnp.where(lane == j, mix_ref[level], row)
    mixrow_ref[...] = row


def unpack(packs, q):
    both, folded = packs(q)
    across = jnp.concatenate([folded[:, 0:S], folded[:, S:]], axis=0)
    return both[:, 0:S], both[:, S:], across


def interface(pack_ref, own_hi, own_lo, msg_hi, msg_lo, rlo_hi, rlo_lo, rhi_hi, rhi_lo, wp, wc, rs, rc, own):
    chip = lax.axis_index("lev") // 2
    one = eye(S)
    zero = jnp.zeros((S, S), F32)
    here, below, across = zip(*[
        unpack(lambda q: (pack_ref[q, 0:64, :], pack_ref[q, 64:96, :]), q) for q in range(8)
    ])
    back = [a.T for a in across]
    ground = [here[q] + (below[q - 1] if q else 0.0) for q in range(8)]
    diag = [ground[q] + across[q] + (back[q - 1] if q else 0.0) for q in range(8)]
    upper = wide([
        [diag[0], -across[0], zero, zero],
        [-back[0], diag[1], -across[1], zero],
        [zero, -back[1], diag[2], -across[2]],
        [zero, zero, -back[2], diag[3]],
    ])
    lower = wide([
        [diag[5], -across[5], zero],
        [-back[5], diag[6], -across[6]],
        [zero, -back[6], diag[7]],
    ])
    first = chip < 2
    small = jnp.where(
        first, upper[0:128, 0:128], wide([[500.0 * one, zero], [zero, diag[7]]])
    )
    upper_inverse, lower_inverse, small_inverse = spd_inverses(
        [upper, lower, small], [9.6, 21.0, 13.9], 2400.0, 6
    )
    upper_t = mm(back[3], upper_inverse[192:256, :])
    lower_t = mm(across[4], lower_inverse[0:64, :])
    middle = (
        ground[4]
        + mm(upper_t, jnp.concatenate(ground[0:4], axis=0))
        + mm(lower_t, jnp.concatenate([ground[5], ground[6], ground[7] + across[7]], axis=0))
    )
    middle_inverse, = spd_inverses([middle], [28.7], 2400.0, 5)
    spread = jnp.concatenate([upper_t, lower_t, one], axis=1)
    lifted = mm(middle_inverse, spread)
    place = {0: 0, 1: 1, 2: 2, 3: 3, 4: 7, 5: 4, 6: 5, 7: 6}
    link = jnp.where(first, back[1], across[6])
    away = mm(link, small_inverse[64:128, :])

    for c in range(4):
        nodes = (2 * c, 2 * c + 1, 2 * c + 1, 2 * c + 2)

        @pl.when(chip == c)
        def _(c=c, nodes=nodes):
            real = [n for n in range(2 * c, 2 * c + 3) if n < 8]
            against = real if 4 in real else real + [4]
            part = lambda x, n: x[:, S * place[n] : S * place[n] + S]
            both = [jnp.concatenate([part(x, n) for n in which], axis=1) for x, which in ((spread, real), (lifted, against))]
            product = mm(both[0], both[1], TN)

            def block(r, k):
                if r not in real or k not in against:
                    return zero
                i, j = real.index(r), against.index(k)
                value = product[S * i : S * i + S, S * j : S * j + S]
                i, j = place[r], place[k]
                if i < 4 and j < 4:
                    value += upper_inverse[S * i : S * i + S, S * j : S * j + S]
                elif 4 <= i < 7 and 4 <= j < 7:
                    value += lower_inverse[S * (i - 4) : S * (i - 3), S * (j - 4) : S * (j - 3)]
                return value

            def blocks(rows, columns):
                return wide([[block(r, k) for k in columns] for r in rows])

            own[...] = blocks(nodes, nodes)
            wc[...] = blocks(nodes, (4,))
            if c in (0, 3):
                far = [away[:, 0:64], away[:, 64:128]]
                if c == 0:
                    rs[...] = jnp.concatenate([far[0], far[1], far[1], one], axis=1)
                    wp[...] = jnp.concatenate([far[0].T, far[1].T, far[1].T, one], axis=0)
                else:
                    rs[...] = jnp.concatenate([one, far[1], far[1], zero], axis=1)
                    wp[...] = jnp.concatenate([one, far[1].T, far[1].T, zero], axis=0)
            else:
                gate = 2 if c == 1 else 6
                rs[...] = blocks((gate,), nodes)
                wp[...] = blocks(nodes, (gate,))

            def seen(n):
                if n > 7:
                    return zero
                n = place[n]
                return spread[:, S * n : S * n + S]

            rc[...] = jnp.concatenate([seen(n) for n in nodes], axis=1)

    own_hi[...], own_lo[...] = split(own[...])
    none = jnp.zeros((256, S), F32)
    msg = wide([[wp[...], none, wc[...], none], [none, wp[...], none, wc[...]]])
    msg_hi[...], msg_lo[...] = split(msg)
    none = jnp.zeros((S, 256), F32)
    rlo_hi[...], rlo_lo[...] = split(jnp.concatenate([rs[...], none, rc[...], none], axis=0))
    rhi_hi[...], rhi_lo[...] = split(jnp.concatenate([none, rs[...], none, rc[...]], axis=0))


def kernel(count, deep, link_hbm, mix_hbm, loss_hbm, pair_hbm, prev_hbm, out_any, var_ref,
           link_ref, mix_ref, loss_ref, pair_ref, prev_ref, load_sem,
           full, row, g_hi, g_lo, hr_hi, hr_lo, hc_hi, hc_lo, pack, pw_hi, pw_lo, pn_hi, pn_lo, field, mixrow,
           packs, own_hi, own_lo, msg_hi, msg_lo, rlo_hi, rlo_lo, rhi_hi, rhi_lo, wp, wc, rs, rc, own,
           state, gs_hi, gs_lo, injs, out_first, in_first, out_then, in_then, out_most, in_most, out_edge, in_edge, sums, outs, ends_ref, part, part_in, mysum, sumbuf,
           pack_send, pack_recv, give_send, give_recv, halo_send, halo_recv, msg_send, msg_recv, out_send, out_recv,
           sum_send, sum_recv):
    lev = lax.axis_index("lev")
    lon = lax.axis_index("lon")
    core = lax.rem(lev, 2)
    chip = lev // 2
    partner = lev + 1 - 2 * core
    base = lev - core
    sibling = 2 * (chip + 1 - 2 * lax.rem(chip, 2)) + core
    across_base = 2 - 2 * (chip // 2)
    far = lax.rem(chip + 2, 4)
    across = [2 * far + core, 2 * (2 * across_base + 1 - far) + core]
    west, east = lax.rem(lon + count - 1, count), lax.rem(lon + 1, count)
    loads = [
        pltpu.make_async_copy(src, dst, load_sem.at[i])
        for i, (src, dst) in enumerate([
            (link_hbm, link_ref), (loss_hbm, loss_ref), (prev_hbm, prev_ref), (pair_hbm, pair_ref.at[core]), (mix_hbm, mix_ref),
        ])
    ]
    for load in loads:
        load.start()
    barrier = pltpu.get_barrier_semaphore()
    others = [lax.rem(lev + d, 8) for d in range(1, 8)]
    for other in others:
        pl.semaphore_signal(barrier, inc=1, device_id={"lev": other}, device_id_type=MESH)
    for side in (west, east):
        pl.semaphore_signal(barrier, inc=1, device_id={"lev": partner, "lon": side}, device_id_type=MESH)

    def greet(d, carry):
        pl.semaphore_signal(barrier, inc=1, device_id={"lon": lax.rem(lon + d, count)}, device_id_type=MESH)
        return carry

    lax.fori_loop(1, count, greet, 0)

    def remote(src, dst, send, recv, where):
        return pltpu.make_async_remote_copy(
            src_ref=src, dst_ref=dst, send_sem=send, recv_sem=recv, device_id=where, device_id_type=MESH
        )

    def rows_at(start, size):
        return pl.ds(pl.multiple_of(start, 8), size)

    pending = []

    def start(copy):
        copy.start()
        pending.append(copy)
        return copy

    loads[0].wait()
    loads[1].wait()
    parts = interior(link_ref, loss_ref, pack)
    loads[3].wait()
    loads[4].wait()
    mix_row_of(mix_ref, mixrow.at[core])
    pl.semaphore_wait(barrier, 8 + count)
    packs[lev] = pack[...]
    spread = [
        start(remote(pack, packs.at[lev], pack_send.at[i], pack_recv.at[i], {"lev": target}))
        for i, target in enumerate([2 * lax.rem(chip + d, 4) + core for d in (2, 1, 3)] + [partner])
    ]
    away = 1 - core

    def give(i, src, dst):
        return start(remote(src, dst, give_send.at[i], give_recv.at[i], {"lev": partner}))

    gives = [give(i, x.at[core], x.at[core]) for i, x in ((1, pair_ref), (2, mixrow))]
    end_rows(link_ref, row.at[core], *parts)
    gives.append(give(3, row.at[core], row.at[core]))
    loads[2].wait()
    field_of(prev_ref, field)
    gives.append(give(0, field.at[rows_at(248 * away, 264)], state.at[0, core, rows_at(8 * core, 264)]))

    def hand_on(i, d):
        spread[i].wait_recv()
        source = 2 * lax.rem(chip + 4 - d, 4) + core
        return start(remote(packs.at[source], packs.at[source], pack_send.at[4 + i], pack_recv.at[4 + i], {"lev": partner}))

    outer = [
        start(remote(field.at[0:8], state.at[0, core, 264:272], halo_send.at[0, 0], halo_recv.at[0, core],
                     {"lev": base + 1, "lon": west})),
        start(remote(field.at[504:512], state.at[0, core, 0:8], halo_send.at[0, 1], halo_recv.at[0, core],
                     {"lev": base, "lon": east})),
    ]
    state[0, core, rows_at(8 * away, 264), :] = field[rows_at(248 * core, 264), :]
    finish_interior(full.at[core], *parts)

    def pair_term(it, s, chunks=((0, 256),)):
        here = [state[it, s, 8 + r : 8 + r + n, :] for r, n in chunks]
        here = jnp.concatenate(here, axis=0) if len(here) > 1 else here[0]
        squares = split(here * here)
        out = []
        for half in range(2):
            piece = tuple(x[:, 256 * half : 256 * half + 256] for x in squares)
            out.append((256 * half, 256, dot3(piece, (pw_hi[s, half], pw_lo[s, half]), NT)))
        piece = tuple(x[:, 512:576] for x in squares)
        out.append((512, 64, dot3(piece, (pn_hi[s], pn_lo[s]), NT)))
        at = 0
        for r, n in chunks:
            for lane, width, value in out:
                sums[s, r : r + n, lane : lane + width] = value[at : at + n]
            at += n

    def forcing_term(it, s, chunks):
        forcing = []
        for r, n in chunks:
            here = state[it, s, 8 + r : 8 + r + n, 0:576]
            around = state[it, s, 7 + r : 7 + r + n, 0:576] + state[it, s, 9 + r : 9 + r + n, 0:576]
            value = state[0, s, 8 + r : 8 + r + n, 0:576] - sums[s, r : r + n, 0:576]
            forcing.append(value + mixrow[s, 0:1, 0:576] * (around - 2.0 * here))
        forcing = jnp.concatenate(forcing, axis=0) if len(forcing) > 1 else forcing[0]
        pieces = split(forcing[:, 0:512])
        node = forcing[:, 512:576]
        push = dot3(pieces, (hr_hi[s], hr_lo[s]), NT) + jnp.concatenate([node, jnp.zeros_like(node)], axis=1)
        at = 0
        for r, n in chunks:
            gs_hi[s, r : r + n, :], gs_lo[s, r : r + n, :] = (x[at : at + n] for x in pieces)
            injs[s, r : r + n, :] = push[at : at + n]
            at += n

    def weights(s):
        pair_weights(pair_ref.at[s], pw_hi.at[s], pw_lo.at[s], pn_hi.at[s], pn_lo.at[s])
        hr_hi[s], hr_lo[s] = split(row[s])

    def product(it, s):
        if it == ITERS - 1:
            for b in range(4):
                rows = slice(128 * b, 128 * b + 128)
                value = dot3((g_hi[s, rows, :], g_lo[s, rows, :]), (gs_hi[s], gs_lo[s]), NT)
                for h in range(2):
                    outs[s, ORDER[2 * b + h]] = value[64 * h : 64 * h + 64]
        else:
            state[it + 1, s, 8:264, 0:512] = dot3((gs_hi[s], gs_lo[s]), (g_hi[s], g_lo[s]))

    middle, edges = ((16, 224),), ((0, 16), (240, 16))
    weights(core)
    pair_term(0, core)
    forcing_term(0, core, middle)
    for gift in gives:
        gift.wait_recv()
    weights(away)
    pair_term(0, away)
    handed = [hand_on(1, 1), hand_on(2, 3), hand_on(0, 2)]
    for slot in range(2):
        pltpu.make_async_copy(field.at[0:8], state.at[0, 0, 0:8], halo_recv.at[0, slot]).wait()
    forcing_term(0, core, edges)
    forcing_term(0, away, ((0, 256),))
    give_full = start(remote(full.at[core], full.at[core], give_send.at[4], give_recv.at[4], {"lev": partner}))
    for copy in [spread[3]] + handed:
        copy.wait_recv()
    interface(packs, own_hi, own_lo, msg_hi, msg_lo, rlo_hi, rlo_lo, rhi_hi, rhi_lo, wp, wc, rs, rc, own)
    for it in range(ITERS):
        final = it == ITERS - 1
        if it:
            for s in range(2):
                forcing_term(it, s, middle)
        slot = 1 + lax.rem(chip, 2)

        def send(chunks, parts):
            lines = [
                jnp.concatenate([injs[s, q + r : q + r + n] for q in (0, 128) for s in range(2)], axis=1) for r, n in chunks
            ]
            message = dot3(split(jnp.concatenate(lines, axis=0) if len(lines) > 1 else lines[0]), (msg_hi[...], msg_lo[...]))
            at = 0
            for out, into, sems in parts:
                size = out.shape[1]
                out[0] = message[at : at + size, 0:128]
                out[1] = message[at : at + size, 128:256]
                at += size
                to = [(1, slot, {"lev": across[0]}), (1, slot, {"lev": across[1]}), (0, 0, {"lev": sibling})]
                for i, (which, where, target) in enumerate(to):
                    start(remote(out.at[which], into.at[where], msg_send.at[sems, i], msg_recv.at[sems, where], target))

        if it == 0:
            send([(0, 32), (96, 32), (32, 64)], [(out_first, in_first, 0), (out_then, in_then, 3)])
        else:
            send([(16, 96)], [(out_most, in_most, 1)])
            for halo in halos:
                halo.wait_recv()
            for s in range(2):
                forcing_term(it, s, edges)
            send([(0, 16), (112, 16)], [(out_edge, in_edge, 2)])
        inj = jnp.concatenate([injs[0], injs[1]], axis=1)
        mine = dot3(split(inj), (own_hi[...], own_lo[...]))
        if it == 0:
            give_full.wait_recv()
            for s in range(2):
                g_hi[s], g_lo[s] = split(full[s])
                hc_hi[s], hc_lo[s] = split(row[s].T)
        for s in range(2):
            product(it, s)
        join = lambda x: jnp.concatenate([x[0], x[1] + x[2]], axis=1)

        def arrived(into, sems):
            for where in range(3):
                pltpu.make_async_copy(into.at[where], into.at[where], msg_recv.at[sems, where]).wait()

        def reached(heard, chunks):
            here = [mine[r : r + n] for r, n in chunks]
            heard = split(heard)
            return (jnp.concatenate(here, axis=0) if len(here) > 1 else here[0]) + jnp.concatenate(
                [dot3(heard, (rlo_hi[...], rlo_lo[...])), dot3(heard, (rhi_hi[...], rhi_lo[...]))], axis=0
            )

        def land(s, ends, chunks):
            ends = ends[:, 128 * s : 128 * s + 128]
            add = dot3(split(ends), (hr_hi[s], hr_lo[s]))
            node = jnp.where(lax.broadcasted_iota(jnp.int32, ends.shape, 1) < S, ends, 0.0)
            at = 0
            for r, n in chunks:
                state[it + 1, s, 8 + r : 8 + r + n, 0:512] += add[at : at + n]
                state[it + 1, s, 8 + r : 8 + r + n, 512:640] = node[at : at + n]
                at += n

        if not final:
            arrived(in_first, 0)
            columns = ((0, 32), (96, 32), (128, 32), (224, 32))
            ends = reached(join(in_first), columns)
            for s in range(2):
                land(s, ends, columns)
            inner_from, inner_to = 8 + 248 * away, 264 * core
            outer_from, outer_to = 8 + 248 * core, 264 * away
            halos = [
                start(remote(state.at[it + 1, :, rows_at(a, 8), :], state.at[it + 1, :, rows_at(b, 8), :],
                             halo_send.at[it + 1, i], halo_recv.at[it + 1, i], where))
                for i, (a, b, where) in enumerate([
                    (outer_from, outer_to, {"lev": partner, "lon": west + (east - west) * core}),
                    (inner_from, inner_to, {"lev": partner}),
                ])
            ]
            for s in range(2):
                pair_term(it + 1, s, columns)
            arrived(in_then, 3)
            columns = ((32, 64), (160, 64))
            ends = reached(join(in_then), columns)
            for s in range(2):
                land(s, ends, columns)
            for s in range(2):
                pair_term(it + 1, s, columns)
            continue
        arrived(in_most, 1)
        arrived(in_edge, 2)
        heard = jnp.concatenate([join(in_edge[:, 0:16]), join(in_most), join(in_edge[:, 16:32])], axis=0)
        total = reached(heard, ((0, 256),))
        total_of = [total[:, 128 * s : 128 * s + 128] for s in range(2)]
    ones = jnp.ones((8, 128), BF16)
    dot1 = lambda x: lax.dot_general(ones, x, NT, preferred_element_type=F32)
    line = lax.broadcasted_iota(jnp.int32, (8, 128), 0)

    ends_ref[0], ends_ref[1] = total_of

    def last_values(s):
        pieces = split(ends_ref[s])
        for b in range(4):
            rows = slice(128 * b, 128 * b + 128)
            value = dot3((hc_hi[s, rows, :], hc_lo[s, rows, :]), pieces, NT)
            for h in range(2):
                outs[s, ORDER[2 * b + h]] += value[64 * h : 64 * h + 64]
        outs[s, 0] = ends_ref[s].T[0:64]

    def squares_of(s):
        packed = jnp.zeros((8, 128), F32)
        for j in range(5):
            values = [outs[s, level] for level in ((ORDER + (0,))[2 * j : 2 * j + 2])]
            values = jnp.concatenate(values if j < 4 else values + [jnp.zeros_like(values[0])], axis=0)
            values = values * values
            high, low = split(values[:, 0:128] + values[:, 128:256])
            packed = jnp.where(line == j, dot1(high) + dot1(low), packed)
        part[s] = packed

    last_values(away)
    squares_of(away)
    give = start(remote(part.at[away], part_in, out_send.at[0], out_recv.at[0], {"lev": partner}))
    back = start(remote(outs.at[away], out_any.at[core], out_send.at[1], out_recv.at[1], {"lev": partner}))
    last_values(core)
    keep = pltpu.make_async_copy(outs.at[core], out_any.at[core], load_sem.at[0])
    keep.start()
    squares_of(core)
    give.wait_recv()
    mine = part[core] + part_in[...]
    mysum[...] = mine
    wide_z = count // deep
    y, z = lon // wide_z, lax.rem(lon, wide_z)
    steps = [(dy, dz) for dy in range(deep) for dz in range(wide_z) if dy or dz]
    steps.sort(key=lambda step: -min(step[0], deep - step[0]) - min(step[1], wide_z - step[1]))
    for i, (dy, dz) in enumerate(steps):
        target = lax.rem(y + dy, deep) * wide_z + lax.rem(z + dz, wide_z)
        slot = lax.rem(count + lon - target - 1, count)
        remote(mysum.at[0:5], sumbuf.at[slot, 0:5], sum_send, sum_recv, {"lon": target}).start()
    keep.wait()
    back.wait_recv()
    for copy in pending:
        copy.wait_send()
    if steps:
        slots = sumbuf.at[0 : len(steps), 0:5]
        pltpu.make_async_copy(slots, slots, sum_send).wait()
        pltpu.make_async_copy(slots, slots, sum_recv).wait()
        mine = mine[0:5] + jnp.sum(sumbuf[:, 0:5], axis=0)
    total = mine * (1.0 / (512 * count))
    for j in range(9):
        level = (ORDER + (0,))[j]
        var_ref[level : level + 1, :] = total[j // 2 : j // 2 + 1, S * (j % 2) : S * (j % 2) + S]


def put_out(field_any, sums_any, out_ref, var_ref, sem):
    copies = [
        pltpu.make_async_copy(
            field_any.at[half, pl.ds(level, 3)], out_ref.at[pl.ds(level, 3), :, pl.ds(256 * half, 256)], sem.at[3 * half + level // 3]
        )
        for half in range(2)
        for level in (0, 3, 6)
    ]
    copies.append(pltpu.make_async_copy(sums_any, var_ref, sem.at[6]))
    for copy in copies:
        copy.start()
    for copy in copies:
        copy.wait()


def vmem(count):
    return [pl.BlockSpec(memory_space=pltpu.VMEM)] * count


def local(previous, loss_matrix, pair_matrix, diffusivity, mixing):
    count = lax.axis_size("lon")
    low = lambda *shape: [pltpu.VMEM(shape, BF16)] * 2
    full = lambda *shape: [pltpu.VMEM(shape, F32)]
    sems = lambda *shape: [pltpu.SemaphoreType.DMA(shape)] * 2
    scratch = [pltpu.SMEM((9,), F32)] * 2 + full(9, S, S) + full(2, 9, S, S) + full(9, S, 512) + [pltpu.SemaphoreType.DMA((5,))]
    scratch += full(2, 512, 512) + full(2, 128, 512) + low(2, 512, 512) + low(2, 128, 512) + low(2, 512, 128) + full(96, 128)
    scratch += low(2, 2, 256, 256) + low(2, S, S) + full(512, 640) + full(2, 8, 640)
    scratch += full(8, 96, 128) + low(256, 256) + low(512, 256) + low(256, 256) * 2
    scratch += full(256, S) * 2 + full(S, 256) * 2 + full(256, 256)
    scratch += full(2, 2, 272, 640) + low(2, 256, 512) + full(2, 256, 128) + full(2, 64, 128) + full(3, 64, 128) + full(2, 64, 128) + full(3, 64, 128)
    scratch += full(2, 96, 128) + full(3, 96, 128) + full(2, 32, 128) + full(3, 32, 128)
    scratch += full(2, 256, 640) + full(2, 9, S, 256) + full(2, 256, 128) + full(2, 8, 128) + full(8, 128) * 2 + full(max(count - 1, 1), 8, 128)
    scratch += sems(7) + sems(5) + sems(2, 2) + sems(4, 3) + sems(2) + [pltpu.SemaphoreType.DMA] * 2
    shapes = [jax.ShapeDtypeStruct((9, S, 512), F32), jax.ShapeDtypeStruct((9, S), F32)]
    halves = jax.ShapeDtypeStruct((2, 9, S, 256), F32)
    anywhere = [pl.BlockSpec(memory_space=pl.ANY)] * 2
    done = pl.pallas_call(
        functools.partial(kernel, count, 4 if count % 4 == 0 else 1),
        out_shape=[halves, shapes[1]],
        in_specs=[pl.BlockSpec(memory_space=pltpu.HBM)] * 5,
        out_specs=(anywhere[0], vmem(1)[0]),
        scratch_shapes=scratch,
        compiler_params=pltpu.CompilerParams(vmem_limit_bytes=32 * 2**20, collective_id=0, has_side_effects=True),
    )(*[pltpu.with_memory_space_constraint(x, pltpu.HBM) for x in (diffusivity, mixing, loss_matrix, pair_matrix, previous)])
    return tuple(pl.pallas_call(
        put_out,
        out_shape=shapes,
        in_specs=anywhere,
        out_specs=tuple(anywhere),
        scratch_shapes=[pltpu.SemaphoreType.DMA((7,))],
        compiler_params=pltpu.CompilerParams(vmem_limit_bytes=8 * 2**20),
    )(*done))


def solution(mesh):
    placed = (P("lev", None, "lon"), P("lev", None, None), P("lev", None, None), P("lev"), P("lev"))
    return jax.shard_map(
        local,
        mesh=mesh,
        in_specs=placed,
        out_specs=(P("lev", None, "lon"), P("lev", None)),
        check_vma=False,
    )
```

```python
import functools

import jax
import jax.numpy as jnp
from jax import lax
from jax.experimental import pallas as pl
from jax.experimental.pallas import tpu as pltpu
from jax.sharding import PartitionSpec as P

ITERS = 2
F32 = jnp.float32
BF16 = jnp.bfloat16
MESH = pl.DeviceIdType.MESH

S = 64
ORDER = (1, 2, 4, 5, 7, 8, 3, 6)
NN = (((1,), (0,)), ((), ()))
NT = (((1,), (1,)), ((), ()))
TN = (((0,), (0,)), ((), ()))


def split(x):
    high = x.astype(BF16)
    return high, (x - high.astype(F32)).astype(BF16)


def dot3(a, b, dims=NN):
    one = lambda x, y: lax.dot_general(x, y, dims, preferred_element_type=F32)
    return one(a[0], b[0]) + (one(a[0], b[1]) + one(a[1], b[0]))


def mm(a, b, dims=NN):
    return dot3(split(a), split(b), dims)


def eye(n):
    rows = lax.broadcasted_iota(jnp.int32, (n, n), 0)
    return (rows == lax.broadcasted_iota(jnp.int32, (n, n), 1)).astype(F32)


def spd_inverses(blocks, lows, high, doublings):
    centres = [0.5 * (high + low) for low in lows]
    units = [eye(block.shape[0]) for block in blocks]
    inverses = [unit * (1.0 / centre) for unit, centre in zip(units, centres)]
    residuals = [unit - block * (1.0 / centre) for unit, block, centre in zip(units, blocks, centres)]
    terms = [(high + low) / (high - low) for low in lows]
    for step in range(doublings):
        last = step == doublings - 1
        for i, unit in enumerate(units):
            twice = 2.0 * terms[i] * terms[i] - 1.0
            gain, shift = (twice + 1.0) / twice, 1.0 / twice
            terms[i] = twice
            centre = centres[i]
            n = unit.shape[0]
            late = step >= doublings - 3
            parts = (lambda x: (x.astype(BF16),)) if late else split
            product = (lambda x, y: lax.dot_general(x[0], y[0], NN, preferred_element_type=F32)) if late else dot3
            rest = parts(residuals[i])
            if step == 0:
                inverses[i] = (inverses[i] + residuals[i] * (1.0 / centre)) * gain
                if not last:
                    residuals[i] = gain * product(rest, rest) - shift * unit
                continue
            known = parts(inverses[i])
            if last:
                inverses[i] = gain * (inverses[i] + product(known, rest))
                continue
            both = product(tuple(jnp.concatenate(p, axis=0) for p in zip(known, rest)), rest)
            inverses[i] = gain * (inverses[i] + both[:n])
            residuals[i] = gain * both[n:] - shift * unit
    exact = [unit - mm(block, inverse) for unit, block, inverse in zip(units, blocks, inverses)]
    step = lambda x, y: lax.dot_general(x.astype(BF16), y.astype(BF16), NN, preferred_element_type=F32)
    return [inverse + step(inverse, rest) for inverse, rest in zip(inverses, exact)]


def wide(grid):
    return jnp.concatenate([jnp.concatenate(row, axis=1) if len(row) > 1 else row[0] for row in grid], axis=0)


def interior(link_ref, loss_ref, pack_ref):
    one = eye(S)
    zero = jnp.zeros((S, S), F32)
    links = [link_ref[i] for i in range(9)]
    shunt = [loss_ref[i] + one for i in range(9)]
    blocks = []
    for top in (1, 4, 7):
        diag = [shunt[level] + (links[level - 1] + links[level]) * one for level in (top, top + 1)]
        tie = -links[top] * one
        blocks.append(wide([[diag[0], tie], [tie, diag[1]]]))
    pairs = spd_inverses(blocks, [199.0] * 3, 6700.0, 5)
    none = jnp.zeros((S, 128), F32)
    spread = wide([
        [links[2] * pairs[0][S:], links[3] * pairs[1][:S], none],
        [none, links[5] * pairs[1][S:], links[6] * pairs[2][:S]],
    ])
    ground = jnp.concatenate(
        [shunt[1] + links[0] * one, shunt[2], shunt[4], shunt[5], shunt[7], shunt[8] + links[8] * one], axis=0
    )
    own = jnp.concatenate([shunt[3], shunt[6]], axis=0) + mm(spread, ground)
    down = links[5] * spread[0:S, 192:256]
    up = links[3] * spread[S:, 128:192]
    lane = lax.broadcasted_iota(jnp.int32, (128, 128), 1)
    ends = jnp.where(lane < S, spread[:, 0:128], spread[:, 256:384])
    stack = jnp.concatenate([shunt[level] for level in ORDER], axis=0)
    through = mm(spread, stack[0:384]) + stack[384:512]
    direct = [mm(pairs[0][:S], stack[0:128]), mm(pairs[2][S:], stack[256:384])]
    middle, = spd_inverses([wide([[own[:S] + down, -down], [-up, own[S:] + up]])], [68.6], 3010.0, 5)
    seen = mm(ends, middle, TN)
    loads = mm(seen, through)
    across = (links[0] * links[8]) * mm(seen[0:S], spread)[:, 320:384]
    pack_ref[0:64, :] = jnp.concatenate(
        [shunt[0] + links[0] * (loads[0:S] + direct[0]), links[8] * (loads[S:] + direct[1])], axis=1
    )
    pack_ref[64:96, :] = jnp.concatenate([across[0:32], across[32:64]], axis=1)
    return pairs, jnp.concatenate([spread, eye(128)], axis=1), middle, seen


def end_rows(link_ref, row_ref, pairs, spread, middle, seen):
    ends = mm(seen, spread)
    first = jnp.concatenate([ends[0:S, 0:128] + pairs[0][:S], ends[0:S, 128:512]], axis=1)
    last = jnp.concatenate([ends[S:, 0:256], ends[S:, 256:384] + pairs[2][S:], ends[S:, 384:512]], axis=1)
    row_ref[...] = jnp.concatenate([link_ref[0] * first, link_ref[8] * last], axis=0)


def finish_interior(full, pairs, spread, middle, seen):
    full[...] = mm(spread, mm(middle, spread), TN)
    for i in range(3):
        at = slice(128 * i, 128 * i + 128)
        full[at, at] += pairs[i]


def pair_weights(pair_ref, pw_hi, pw_lo, pn_hi, pn_lo):
    for half in range(2):
        row = lax.broadcasted_iota(jnp.int32, (256, 256), 0) // S
        column = lax.broadcasted_iota(jnp.int32, (256, 256), 1) // S
        tall = jnp.concatenate([pair_ref[level] for level in ORDER[4 * half : 4 * half + 4]], axis=0)
        tall = jnp.concatenate([tall, tall], axis=1)
        tall = jnp.where(row == column, jnp.concatenate([tall, tall], axis=1), 0.0)
        pw_hi[half], pw_lo[half] = split(tall)
    pn_hi[...], pn_lo[...] = split(pair_ref[0])


def field_of(prev_ref, field_ref):
    for j in range(4):
        both = jnp.concatenate([prev_ref[ORDER[2 * j]], prev_ref[ORDER[2 * j + 1]]], axis=0)
        field_ref[:, 128 * j : 128 * j + 128] = both.T
    last = jnp.concatenate([prev_ref[0], jnp.zeros_like(prev_ref[0])], axis=0)
    field_ref[:, 512:640] = last.T


def mix_row_of(mix_ref, mixrow_ref):
    lane = lax.broadcasted_iota(jnp.int32, (8, 640), 1) // S
    row = jnp.zeros((8, 640), F32)
    for j, level in enumerate(ORDER + (0,)):
        row = jnp.where(lane == j, mix_ref[level], row)
    mixrow_ref[...] = row


def unpack(packs, q):
    both, folded = packs(q)
    across = jnp.concatenate([folded[:, 0:S], folded[:, S:]], axis=0)
    return both[:, 0:S], both[:, S:], across


def interface(pack_ref, own_hi, own_lo, msg_hi, msg_lo, rlo_hi, rlo_lo, rhi_hi, rhi_lo, wp, wc, rs, rc, own):
    chip = lax.axis_index("lev") // 2
    one = eye(S)
    zero = jnp.zeros((S, S), F32)
    here, below, across = zip(*[
        unpack(lambda q: (pack_ref[q, 0:64, :], pack_ref[q, 64:96, :]), q) for q in range(8)
    ])
    back = [a.T for a in across]
    ground = [here[q] + (below[q - 1] if q else 0.0) for q in range(8)]
    diag = [ground[q] + across[q] + (back[q - 1] if q else 0.0) for q in range(8)]
    upper = wide([
        [diag[0], -across[0], zero, zero],
        [-back[0], diag[1], -across[1], zero],
        [zero, -back[1], diag[2], -across[2]],
        [zero, zero, -back[2], diag[3]],
    ])
    lower = wide([
        [diag[5], -across[5], zero],
        [-back[5], diag[6], -across[6]],
        [zero, -back[6], diag[7]],
    ])
    first = chip < 2
    small = jnp.where(
        first, upper[0:128, 0:128], wide([[500.0 * one, zero], [zero, diag[7]]])
    )
    upper_inverse, lower_inverse, small_inverse = spd_inverses(
        [upper, lower, small], [9.6, 21.0, 13.9], 2400.0, 6
    )
    upper_t = mm(back[3], upper_inverse[192:256, :])
    lower_t = mm(across[4], lower_inverse[0:64, :])
    middle = (
        ground[4]
        + mm(upper_t, jnp.concatenate(ground[0:4], axis=0))
        + mm(lower_t, jnp.concatenate([ground[5], ground[6], ground[7] + across[7]], axis=0))
    )
    middle_inverse, = spd_inverses([middle], [28.7], 2400.0, 5)
    spread = jnp.concatenate([upper_t, lower_t, one], axis=1)
    lifted = mm(middle_inverse, spread)
    place = {0: 0, 1: 1, 2: 2, 3: 3, 4: 7, 5: 4, 6: 5, 7: 6}
    link = jnp.where(first, back[1], across[6])
    away = mm(link, small_inverse[64:128, :])

    for c in range(4):
        nodes = (2 * c, 2 * c + 1, 2 * c + 1, 2 * c + 2)

        @pl.when(chip == c)
        def _(c=c, nodes=nodes):
            real = [n for n in range(2 * c, 2 * c + 3) if n < 8]
            against = real if 4 in real else real + [4]
            part = lambda x, n: x[:, S * place[n] : S * place[n] + S]
            both = [jnp.concatenate([part(x, n) for n in which], axis=1) for x, which in ((spread, real), (lifted, against))]
            product = mm(both[0], both[1], TN)

            def block(r, k):
                if r not in real or k not in against:
                    return zero
                i, j = real.index(r), against.index(k)
                value = product[S * i : S * i + S, S * j : S * j + S]
                i, j = place[r], place[k]
                if i < 4 and j < 4:
                    value += upper_inverse[S * i : S * i + S, S * j : S * j + S]
                elif 4 <= i < 7 and 4 <= j < 7:
                    value += lower_inverse[S * (i - 4) : S * (i - 3), S * (j - 4) : S * (j - 3)]
                return value

            def blocks(rows, columns):
                return wide([[block(r, k) for k in columns] for r in rows])

            own[...] = blocks(nodes, nodes)
            wc[...] = blocks(nodes, (4,))
            if c in (0, 3):
                far = [away[:, 0:64], away[:, 64:128]]
                if c == 0:
                    rs[...] = jnp.concatenate([far[0], far[1], far[1], one], axis=1)
                    wp[...] = jnp.concatenate([far[0].T, far[1].T, far[1].T, one], axis=0)
                else:
                    rs[...] = jnp.concatenate([one, far[1], far[1], zero], axis=1)
                    wp[...] = jnp.concatenate([one, far[1].T, far[1].T, zero], axis=0)
            else:
                gate = 2 if c == 1 else 6
                rs[...] = blocks((gate,), nodes)
                wp[...] = blocks(nodes, (gate,))

            def seen(n):
                if n > 7:
                    return zero
                n = place[n]
                return spread[:, S * n : S * n + S]

            rc[...] = jnp.concatenate([seen(n) for n in nodes], axis=1)

    own_hi[...], own_lo[...] = split(own[...])
    none = jnp.zeros((256, S), F32)
    msg = wide([[wp[...], none, wc[...], none], [none, wp[...], none, wc[...]]])
    msg_hi[...], msg_lo[...] = split(msg)
    none = jnp.zeros((S, 256), F32)
    rlo_hi[...], rlo_lo[...] = split(jnp.concatenate([rs[...], none, rc[...], none], axis=0))
    rhi_hi[...], rhi_lo[...] = split(jnp.concatenate([none, rs[...], none, rc[...]], axis=0))


def kernel(count, deep, link_hbm, mix_hbm, loss_hbm, pair_hbm, prev_hbm, out_any, var_ref,
           link_ref, mix_ref, loss_ref, pair_ref, prev_ref, load_sem,
           full, row, g_hi, g_lo, hr_hi, hr_lo, hc_hi, hc_lo, pack, pw_hi, pw_lo, pn_hi, pn_lo, field, mixrow,
           packs, own_hi, own_lo, msg_hi, msg_lo, rlo_hi, rlo_lo, rhi_hi, rhi_lo, wp, wc, rs, rc, own,
           state, gs_hi, gs_lo, injs, out_first, in_first, out_then, in_then, out_most, in_most, out_edge, in_edge, sums, outs, ends_ref, part, part_in, mysum, sumbuf,
           pack_send, pack_recv, give_send, give_recv, halo_send, halo_recv, msg_send, msg_recv, out_send, out_recv,
           sum_send, sum_recv):
    lev = lax.axis_index("lev")
    lon = lax.axis_index("lon")
    core = lax.rem(lev, 2)
    chip = lev // 2
    partner = lev + 1 - 2 * core
    base = lev - core
    sibling = 2 * (chip + 1 - 2 * lax.rem(chip, 2)) + core
    across_base = 2 - 2 * (chip // 2)
    far = lax.rem(chip + 2, 4)
    across = [2 * far + core, 2 * (2 * across_base + 1 - far) + core]
    west, east = lax.rem(lon + count - 1, count), lax.rem(lon + 1, count)
    loads = [
        pltpu.make_async_copy(src, dst, load_sem.at[i])
        for i, (src, dst) in enumerate([
            (link_hbm, link_ref), (loss_hbm, loss_ref), (prev_hbm, prev_ref), (pair_hbm, pair_ref.at[core]), (mix_hbm, mix_ref),
        ])
    ]
    for load in loads:
        load.start()
    barrier = pltpu.get_barrier_semaphore()
    others = [lax.rem(lev + d, 8) for d in range(1, 8)]
    for other in others:
        pl.semaphore_signal(barrier, inc=1, device_id={"lev": other}, device_id_type=MESH)
    for side in (west, east):
        pl.semaphore_signal(barrier, inc=1, device_id={"lev": partner, "lon": side}, device_id_type=MESH)

    def greet(d, carry):
        pl.semaphore_signal(barrier, inc=1, device_id={"lon": lax.rem(lon + d, count)}, device_id_type=MESH)
        return carry

    lax.fori_loop(1, count, greet, 0)

    def remote(src, dst, send, recv, where):
        return pltpu.make_async_remote_copy(
            src_ref=src, dst_ref=dst, send_sem=send, recv_sem=recv, device_id=where, device_id_type=MESH
        )

    def rows_at(start, size):
        return pl.ds(pl.multiple_of(start, 8), size)

    pending = []

    def start(copy):
        copy.start()
        pending.append(copy)
        return copy

    loads[0].wait()
    loads[1].wait()
    parts = interior(link_ref, loss_ref, pack)
    loads[3].wait()
    loads[4].wait()
    mix_row_of(mix_ref, mixrow.at[core])
    pl.semaphore_wait(barrier, 8 + count)
    packs[lev] = pack[...]
    spread = [
        start(remote(pack, packs.at[lev], pack_send.at[i], pack_recv.at[i], {"lev": target}))
        for i, target in enumerate([2 * lax.rem(chip + d, 4) + core for d in (2, 1, 3)] + [partner])
    ]
    away = 1 - core

    def give(i, src, dst):
        return start(remote(src, dst, give_send.at[i], give_recv.at[i], {"lev": partner}))

    gives = [give(i, x.at[core], x.at[core]) for i, x in ((1, pair_ref), (2, mixrow))]
    end_rows(link_ref, row.at[core], *parts)
    gives.append(give(3, row.at[core], row.at[core]))
    loads[2].wait()
    field_of(prev_ref, field)
    gives.append(give(0, field.at[rows_at(248 * away, 264)], state.at[0, core, rows_at(8 * core, 264)]))

    def hand_on(i, d):
        spread[i].wait_recv()
        source = 2 * lax.rem(chip + 4 - d, 4) + core
        return start(remote(packs.at[source], packs.at[source], pack_send.at[4 + i], pack_recv.at[4 + i], {"lev": partner}))

    outer = [
        start(remote(field.at[0:8], state.at[0, core, 264:272], halo_send.at[0, 0], halo_recv.at[0, core],
                     {"lev": base + 1, "lon": west})),
        start(remote(field.at[504:512], state.at[0, core, 0:8], halo_send.at[0, 1], halo_recv.at[0, core],
                     {"lev": base, "lon": east})),
    ]
    state[0, core, rows_at(8 * away, 264), :] = field[rows_at(248 * core, 264), :]
    finish_interior(full.at[core], *parts)

    def pair_term(it, s, chunks=((0, 256),)):
        here = [state[it, s, 8 + r : 8 + r + n, :] for r, n in chunks]
        here = jnp.concatenate(here, axis=0) if len(here) > 1 else here[0]
        squares = split(here * here)
        out = []
        for half in range(2):
            piece = tuple(x[:, 256 * half : 256 * half + 256] for x in squares)
            out.append((256 * half, 256, dot3(piece, (pw_hi[s, half], pw_lo[s, half]), NT)))
        piece = tuple(x[:, 512:576] for x in squares)
        out.append((512, 64, dot3(piece, (pn_hi[s], pn_lo[s]), NT)))
        at = 0
        for r, n in chunks:
            for lane, width, value in out:
                sums[s, r : r + n, lane : lane + width] = value[at : at + n]
            at += n

    def forcing_term(it, s, chunks):
        forcing = []
        for r, n in chunks:
            here = state[it, s, 8 + r : 8 + r + n, 0:576]
            around = state[it, s, 7 + r : 7 + r + n, 0:576] + state[it, s, 9 + r : 9 + r + n, 0:576]
            value = state[0, s, 8 + r : 8 + r + n, 0:576] - sums[s, r : r + n, 0:576]
            forcing.append(value + mixrow[s, 0:1, 0:576] * (around - 2.0 * here))
        forcing = jnp.concatenate(forcing, axis=0) if len(forcing) > 1 else forcing[0]
        pieces = split(forcing[:, 0:512])
        node = forcing[:, 512:576]
        push = dot3(pieces, (hr_hi[s], hr_lo[s]), NT) + jnp.concatenate([node, jnp.zeros_like(node)], axis=1)
        at = 0
        for r, n in chunks:
            gs_hi[s, r : r + n, :], gs_lo[s, r : r + n, :] = (x[at : at + n] for x in pieces)
            injs[s, r : r + n, :] = push[at : at + n]
            at += n

    def weights(s):
        pair_weights(pair_ref.at[s], pw_hi.at[s], pw_lo.at[s], pn_hi.at[s], pn_lo.at[s])
        hr_hi[s], hr_lo[s] = split(row[s])

    def product(it, s):
        if it == ITERS - 1:
            for b in range(4):
                rows = slice(128 * b, 128 * b + 128)
                value = dot3((g_hi[s, rows, :], g_lo[s, rows, :]), (gs_hi[s], gs_lo[s]), NT)
                for h in range(2):
                    outs[s, ORDER[2 * b + h]] = value[64 * h : 64 * h + 64]
        else:
            state[it + 1, s, 8:264, 0:512] = dot3((gs_hi[s], gs_lo[s]), (g_hi[s], g_lo[s]))

    middle, edges = ((16, 224),), ((0, 16), (240, 16))
    weights(core)
    pair_term(0, core)
    forcing_term(0, core, middle)
    for gift in gives:
        gift.wait_recv()
    weights(away)
    pair_term(0, away)
    handed = [hand_on(1, 1), hand_on(2, 3), hand_on(0, 2)]
    for slot in range(2):
        pltpu.make_async_copy(field.at[0:8], state.at[0, 0, 0:8], halo_recv.at[0, slot]).wait()
    forcing_term(0, core, edges)
    forcing_term(0, away, ((0, 256),))
    give_full = start(remote(full.at[core], full.at[core], give_send.at[4], give_recv.at[4], {"lev": partner}))
    for copy in [spread[3]] + handed:
        copy.wait_recv()
    interface(packs, own_hi, own_lo, msg_hi, msg_lo, rlo_hi, rlo_lo, rhi_hi, rhi_lo, wp, wc, rs, rc, own)
    for it in range(ITERS):
        final = it == ITERS - 1
        if it:
            for s in range(2):
                forcing_term(it, s, middle)
        slot = 1 + lax.rem(chip, 2)

        def send(chunks, parts):
            lines = [
                jnp.concatenate([injs[s, q + r : q + r + n] for q in (0, 128) for s in range(2)], axis=1) for r, n in chunks
            ]
            message = dot3(split(jnp.concatenate(lines, axis=0) if len(lines) > 1 else lines[0]), (msg_hi[...], msg_lo[...]))
            at = 0
            for out, into, sems in parts:
                size = out.shape[1]
                out[0] = message[at : at + size, 0:128]
                out[1] = message[at : at + size, 128:256]
                at += size
                to = [(1, slot, {"lev": across[0]}), (1, slot, {"lev": across[1]}), (0, 0, {"lev": sibling})]
                for i, (which, where, target) in enumerate(to):
                    start(remote(out.at[which], into.at[where], msg_send.at[sems, i], msg_recv.at[sems, where], target))

        if it == 0:
            send([(0, 32), (96, 32), (32, 64)], [(out_first, in_first, 0), (out_then, in_then, 3)])
        else:
            send([(16, 96)], [(out_most, in_most, 1)])
            for halo in halos:
                halo.wait_recv()
            for s in range(2):
                forcing_term(it, s, edges)
            send([(0, 16), (112, 16)], [(out_edge, in_edge, 2)])
        inj = jnp.concatenate([injs[0], injs[1]], axis=1)
        mine = dot3(split(inj), (own_hi[...], own_lo[...]))
        if it == 0:
            give_full.wait_recv()
            for s in range(2):
                g_hi[s], g_lo[s] = split(full[s])
                hc_hi[s], hc_lo[s] = split(row[s].T)
        for s in range(2):
            product(it, s)
        join = lambda x: jnp.concatenate([x[0], x[1] + x[2]], axis=1)

        def arrived(into, sems):
            for where in range(3):
                pltpu.make_async_copy(into.at[where], into.at[where], msg_recv.at[sems, where]).wait()

        def reached(heard, chunks):
            here = [mine[r : r + n] for r, n in chunks]
            heard = split(heard)
            return (jnp.concatenate(here, axis=0) if len(here) > 1 else here[0]) + jnp.concatenate(
                [dot3(heard, (rlo_hi[...], rlo_lo[...])), dot3(heard, (rhi_hi[...], rhi_lo[...]))], axis=0
            )

        def land(s, ends, chunks):
            ends = ends[:, 128 * s : 128 * s + 128]
            add = dot3(split(ends), (hr_hi[s], hr_lo[s]))
            node = jnp.where(lax.broadcasted_iota(jnp.int32, ends.shape, 1) < S, ends, 0.0)
            at = 0
            for r, n in chunks:
                state[it + 1, s, 8 + r : 8 + r + n, 0:512] += add[at : at + n]
                state[it + 1, s, 8 + r : 8 + r + n, 512:640] = node[at : at + n]
                at += n

        if not final:
            arrived(in_first, 0)
            columns = ((0, 32), (96, 32), (128, 32), (224, 32))
            ends = reached(join(in_first), columns)
            for s in range(2):
                land(s, ends, columns)
            inner_from, inner_to = 8 + 248 * away, 264 * core
            outer_from, outer_to = 8 + 248 * core, 264 * away
            halos = [
                start(remote(state.at[it + 1, :, rows_at(a, 8), :], state.at[it + 1, :, rows_at(b, 8), :],
                             halo_send.at[it + 1, i], halo_recv.at[it + 1, i], where))
                for i, (a, b, where) in enumerate([
                    (outer_from, outer_to, {"lev": partner, "lon": west + (east - west) * core}),
                    (inner_from, inner_to, {"lev": partner}),
                ])
            ]
            for s in range(2):
                pair_term(it + 1, s, columns)
            arrived(in_then, 3)
            columns = ((32, 64), (160, 64))
            ends = reached(join(in_then), columns)
            for s in range(2):
                land(s, ends, columns)
            for s in range(2):
                pair_term(it + 1, s, columns)
            continue
        arrived(in_most, 1)
        arrived(in_edge, 2)
        heard = jnp.concatenate([join(in_edge[:, 0:16]), join(in_most), join(in_edge[:, 16:32])], axis=0)
        total = reached(heard, ((0, 256),))
        total_of = [total[:, 128 * s : 128 * s + 128] for s in range(2)]
    ones = jnp.ones((8, 128), BF16)
    dot1 = lambda x: lax.dot_general(ones, x, NT, preferred_element_type=F32)
    line = lax.broadcasted_iota(jnp.int32, (8, 128), 0)

    ends_ref[0], ends_ref[1] = total_of

    def last_values(s):
        pieces = split(ends_ref[s])
        for b in range(4):
            rows = slice(128 * b, 128 * b + 128)
            value = dot3((hc_hi[s, rows, :], hc_lo[s, rows, :]), pieces, NT)
            for h in range(2):
                outs[s, ORDER[2 * b + h]] += value[64 * h : 64 * h + 64]
        outs[s, 0] = ends_ref[s].T[0:64]

    def squares_of(s):
        packed = jnp.zeros((8, 128), F32)
        for j in range(5):
            values = [outs[s, level] for level in ((ORDER + (0,))[2 * j : 2 * j + 2])]
            values = jnp.concatenate(values if j < 4 else values + [jnp.zeros_like(values[0])], axis=0)
            values = values * values
            high, low = split(values[:, 0:128] + values[:, 128:256])
            packed = jnp.where(line == j, dot1(high) + dot1(low), packed)
        part[s] = packed

    last_values(away)
    squares_of(away)
    give = start(remote(part.at[away], part_in, out_send.at[0], out_recv.at[0], {"lev": partner}))
    last_values(core)
    keep = pltpu.make_async_copy(outs.at[core], out_any.at[core], load_sem.at[0])
    keep.start()
    squares_of(core)
    give.wait_recv()
    mine = part[core] + part_in[...]
    mysum[...] = mine
    wide_z = count // deep
    y, z = lon // wide_z, lax.rem(lon, wide_z)
    steps = [(dy, dz) for dy in range(deep) for dz in range(wide_z) if dy or dz]
    steps.sort(key=lambda step: -min(step[0], deep - step[0]) - min(step[1], wide_z - step[1]))
    for i, (dy, dz) in enumerate(steps):
        target = lax.rem(y + dy, deep) * wide_z + lax.rem(z + dz, wide_z)
        slot = lax.rem(count + lon - target - 1, count)
        remote(mysum.at[0:5], sumbuf.at[slot, 0:5], sum_send, sum_recv, {"lon": target}).start()
    back = start(remote(outs.at[away], out_any.at[core], out_send.at[1], out_recv.at[1], {"lev": partner}))
    keep.wait()
    back.wait_recv()
    for copy in pending:
        copy.wait_send()
    if steps:
        slots = sumbuf.at[0 : len(steps), 0:5]
        pltpu.make_async_copy(slots, slots, sum_send).wait()
        pltpu.make_async_copy(slots, slots, sum_recv).wait()
        mine = mine[0:5] + jnp.sum(sumbuf[:, 0:5], axis=0)
    total = mine * (1.0 / (512 * count))
    for j in range(9):
        level = (ORDER + (0,))[j]
        var_ref[level : level + 1, :] = total[j // 2 : j // 2 + 1, S * (j % 2) : S * (j % 2) + S]


def put_out(field_any, sums_any, out_ref, var_ref, sem):
    copies = [
        pltpu.make_async_copy(
            field_any.at[half, pl.ds(level, 3)], out_ref.at[pl.ds(level, 3), :, pl.ds(256 * half, 256)], sem.at[3 * half + level // 3]
        )
        for half in range(2)
        for level in (0, 3, 6)
    ]
    copies.append(pltpu.make_async_copy(sums_any, var_ref, sem.at[6]))
    for copy in copies:
        copy.start()
    for copy in copies:
        copy.wait()


def vmem(count):
    return [pl.BlockSpec(memory_space=pltpu.VMEM)] * count


def local(previous, loss_matrix, pair_matrix, diffusivity, mixing):
    count = lax.axis_size("lon")
    low = lambda *shape: [pltpu.VMEM(shape, BF16)] * 2
    full = lambda *shape: [pltpu.VMEM(shape, F32)]
    sems = lambda *shape: [pltpu.SemaphoreType.DMA(shape)] * 2
    scratch = [pltpu.SMEM((9,), F32)] * 2 + full(9, S, S) + full(2, 9, S, S) + full(9, S, 512) + [pltpu.SemaphoreType.DMA((5,))]
    scratch += full(2, 512, 512) + full(2, 128, 512) + low(2, 512, 512) + low(2, 128, 512) + low(2, 512, 128) + full(96, 128)
    scratch += low(2, 2, 256, 256) + low(2, S, S) + full(512, 640) + full(2, 8, 640)
    scratch += full(8, 96, 128) + low(256, 256) + low(512, 256) + low(256, 256) * 2
    scratch += full(256, S) * 2 + full(S, 256) * 2 + full(256, 256)
    scratch += full(2, 2, 272, 640) + low(2, 256, 512) + full(2, 256, 128) + full(2, 64, 128) + full(3, 64, 128) + full(2, 64, 128) + full(3, 64, 128)
    scratch += full(2, 96, 128) + full(3, 96, 128) + full(2, 32, 128) + full(3, 32, 128)
    scratch += full(2, 256, 640) + full(2, 9, S, 256) + full(2, 256, 128) + full(2, 8, 128) + full(8, 128) * 2 + full(max(count - 1, 1), 8, 128)
    scratch += sems(7) + sems(5) + sems(2, 2) + sems(4, 3) + sems(2) + [pltpu.SemaphoreType.DMA] * 2
    shapes = [jax.ShapeDtypeStruct((9, S, 512), F32), jax.ShapeDtypeStruct((9, S), F32)]
    halves = jax.ShapeDtypeStruct((2, 9, S, 256), F32)
    anywhere = [pl.BlockSpec(memory_space=pl.ANY)] * 2
    done = pl.pallas_call(
        functools.partial(kernel, count, 4 if count % 4 == 0 else 1),
        out_shape=[halves, shapes[1]],
        in_specs=[pl.BlockSpec(memory_space=pltpu.HBM)] * 5,
        out_specs=(anywhere[0], vmem(1)[0]),
        scratch_shapes=scratch,
        compiler_params=pltpu.CompilerParams(vmem_limit_bytes=32 * 2**20, collective_id=0, has_side_effects=True),
    )(*[pltpu.with_memory_space_constraint(x, pltpu.HBM) for x in (diffusivity, mixing, loss_matrix, pair_matrix, previous)])
    return tuple(pl.pallas_call(
        put_out,
        out_shape=shapes,
        in_specs=anywhere,
        out_specs=tuple(anywhere),
        scratch_shapes=[pltpu.SemaphoreType.DMA((7,))],
        compiler_params=pltpu.CompilerParams(vmem_limit_bytes=8 * 2**20),
    )(*done))


def solution(mesh):
    placed = (P("lev", None, "lon"), P("lev", None, None), P("lev", None, None), P("lev"), P("lev"))
    return jax.shard_map(
        local,
        mesh=mesh,
        in_specs=placed,
        out_specs=(P("lev", None, "lon"), P("lev", None)),
        check_vma=False,
    )
```
